256 devices in a mesh: gx: 8 (over x_lo, y), gy: 4 (over x_hi, core), gz: 8 (over z).
Axes of the slice: x: 4 (x_hi: 2, x_lo: 2; x = x_hi * 2 + x_lo), y: 4, z: 8, core: 2. Of those that a mesh axis runs over, the one named last changes fastest.
Arguments:
- offsets: float32 [16, 8, 64, 16, 3], P('gx', 'gy', 'gz'), may hold values from 0.2649 to 2.3351, as said below
- velocities: float32 [16, 8, 64, 16, 3], P('gx', 'gy', 'gz'), may hold values from -6 to 6
- occupied: int32 [16, 8, 64, 16], P('gx', 'gy', 'gz'), may hold values 0 or 1
Outputs:
- positions: float32 [16, 8, 64, 16, 3], P('gx', 'gy', 'gz')
- new_velocities: float32 [16, 8, 64, 16, 3], P('gx', 'gy', 'gz')
- forces: float32 [16, 8, 64, 16, 3], P('gx', 'gy', 'gz')
- capacity_history: float32 [4, 2], replicated
The draws below stay inside these ranges and needn't reach their ends.
Inputs may be any that keep to these rules, and one draw needn't show every extreme that they name: `offsets`: each offset lies within the cell, a jittered body-centred lattice of 16 sites with spacing 1.3 per cell, jitter at most 0.06 in each coordinate.
All inputs are finite; a program needn't handle non-finite values.
Results may differ from the reference program's by a relative error of at most 0.0003.
Values sent between devices are 32-bit elements.
A program may use at most 128 MiB of HBM per device.

```python
import jax
import jax.numpy as jnp
from jax import lax

SLOTS = 16
STEPS = 4
NX = 16
NY = 8
NZ = 64


LATTICE_STEP = 1.3


JITTER = 0.06


def draw_offsets(key, part):
    slot_ids = jnp.arange(SLOTS) % 16
    corner = slot_ids % 8
    corner_bits = jnp.stack([corner // 4, corner // 2 % 2, corner % 2], axis=-1).astype(jnp.float32)
    centred = (slot_ids // 8).astype(jnp.float32)[:, None]
    lattice = LATTICE_STEP * (corner_bits + 0.5 * centred) + 0.325
    shape_all = (NX, NY, NZ, SLOTS, 3)
    jitter = jax.random.uniform(key, shape_all, jnp.float32, -JITTER, JITTER)
    return (lattice + jitter).astype(jnp.float32)


def plant(result, key, smallest, largest):
    longest = result.shape.index(max(result.shape))
    spots = []
    for shift in (0, 1):
        where = [jax.random.randint(jax.random.fold_in(key, axis), (), 0, length) for axis, length in enumerate(result.shape)]
        where[longest] = (where[longest] + shift) % result.shape[longest]
        spots.append(tuple(where))
    return result.at[spots[0]].set(smallest).at[spots[1]].set(largest)


def block_levels(stream_key, dims, pieces, least, largest):
    def one(dim, shards_of):
        heights = jax.random.uniform(jax.random.fold_in(jax.random.fold_in(stream_key, 6), dim), (shards_of,), jnp.float32, least / len(pieces), largest / len(pieces))
        return jnp.repeat(jnp.exp(heights), dims[dim] // shards_of).reshape((-1,) + (1,) * (len(dims) - dim - 1))

    loudness = one(*pieces[0])
    for cut in pieces[1:]:
        loudness = loudness * one(*cut)
    return loudness


def bell_draw(own_key, shape, spread, bound, shards=(), kind=jnp.bfloat16):
    level = block_levels(own_key, shape, shards, -0.22, 0.18) if shards else 1.0
    entries = jax.random.normal(own_key, shape, jnp.float32) * spread * level
    return jnp.minimum(jnp.maximum(entries, -bound), bound).astype(kind)


def setup_inputs(seed: int = 0) -> dict:
    keys = jax.random.split(jax.random.key(seed), 4)
    offsets = draw_offsets(jax.random.fold_in(keys[3], 71), 0)
    velocities = bell_draw(keys[1], (NX, NY, NZ, SLOTS, 3), 1.0, 6.0, ((0, 8), (1, 4), (2, 8)), jnp.float32)
    occupied = plant((jax.random.randint(keys[2], (NX, NY, NZ, SLOTS), 0, 16) < 13).astype(jnp.int32), jax.random.fold_in(keys[2], 1), 0, 1)
    return dict(offsets=offsets, velocities=velocities, occupied=occupied)


CUTOFF = 2.5
CELL_SIDE = 2.6
TIME_STEP = 0.005
BATH_STRENGTH = 0.25
GOAL_WARMTH = 0.8
FORCE_EDGE = 24.0 * (2.0 * CUTOFF ** (-13) - CUTOFF ** (-7))
ENERGY_EDGE = 4.0 * (CUTOFF ** (-12) - CUTOFF ** (-6))
STENCILS = [(along_x, along_y, along_z) for along_x in (-1, 0, 1) for along_y in (-1, 0, 1) for along_z in (-1, 0, 1)]

def pair_terms(own_cells, neighbour, stencil):
    cell_shift = jnp.array(stencil, jnp.float32) * CELL_SIDE
    separation = neighbour[..., None, :, :3] + cell_shift - own_cells[..., :, None, :3]
    squared = lax.optimization_barrier(jnp.sum(separation * separation, axis=-1))
    occupied_pair = own_cells[..., :, None, 3] * neighbour[..., None, :, 3]
    inside = (occupied_pair > 0.5) & (squared < CUTOFF * CUTOFF)
    if stencil == (0, 0, 0):
        slots_count = own_cells.shape[-2]
        inside = inside & jnp.logical_not(jnp.eye(slots_count, dtype=bool))
    guarded = jnp.where(inside, squared, 1.0)
    inverse = 1.0 / guarded
    inverse_six = inverse * inverse * inverse
    radius = jnp.sqrt(guarded)
    strength = 24.0 * (2.0 * inverse_six * inverse_six - inverse_six) * inverse - FORCE_EDGE / radius
    strength = jnp.where(inside, strength, 0.0)
    energy = 4.0 * (inverse_six * inverse_six - inverse_six) - ENERGY_EDGE + (radius - CUTOFF) * FORCE_EDGE
    energy = jnp.where(inside, energy, 0.0)
    pushes = -strength[..., None] * separation
    return (pushes, energy)

def window(padded, stencil, extent):
    return padded[1 + stencil[0]:1 + stencil[0] + extent[0], 1 + stencil[1]:1 + stencil[1] + extent[1], 1 + stencil[2]:1 + stencil[2] + extent[2]]

def full_forces(padded):
    extent = (padded.shape[0] - 2, padded.shape[1] - 2, padded.shape[2] - 2)
    own_cells = window(padded, (0, 0, 0), extent)
    forces = jnp.zeros(own_cells.shape[:-1] + (3,), jnp.float32)
    energy = jnp.zeros((), jnp.float32)
    for stencil in STENCILS:
        pushes, pair_energy = pair_terms(own_cells, window(padded, stencil, extent), stencil)
        forces = forces + lax.optimization_barrier(jnp.sum(pushes, axis=-2))
        energy = energy + jnp.sum(pair_energy)
    return (forces, 0.5 * energy)

def evaluate(position, weight):
    packed = jnp.concatenate([position, weight[..., None]], axis=-1)
    padded = jnp.pad(packed, ((1, 1), (1, 1), (1, 1), (0, 0), (0, 0)), mode='wrap')

    def one_plane(plane_index):
        block = lax.dynamic_slice_in_dim(padded, plane_index, 3, 0)
        return full_forces(block)
    forces, capacity_history = lax.map(one_plane, jnp.arange(NX, dtype=jnp.int32))
    return (forces.reshape(position.shape), jnp.sum(capacity_history))

def reference(offsets, velocities, occupied):
    weight = occupied.astype(jnp.float32)
    velocity = velocities * weight[..., None]
    position = offsets
    slot_total = float(NX * NY * NZ * SLOTS)
    forces, initial_energy = evaluate(position, weight)
    body_tally = jnp.sum(weight)
    records = []
    for step_index in range(STEPS):
        velocity = velocity + 0.5 * TIME_STEP * forces
        position = position + TIME_STEP * velocity
        forces, potential = evaluate(position, weight)
        velocity = velocity + 0.5 * TIME_STEP * forces
        moving_vigor = 0.5 * jnp.sum(velocity * velocity)
        warmth_gauge = 2.0 * moving_vigor / (3.0 * body_tally)
        speed_stretch = jnp.sqrt(1.0 + BATH_STRENGTH * (GOAL_WARMTH / warmth_gauge - 1.0))
        velocity = speed_stretch * velocity
        records.append(jnp.stack([potential, speed_stretch * speed_stretch * moving_vigor]) / slot_total)
    return (position, velocity, forces, jnp.stack(records))
```

```python
import functools
import itertools

import jax
import jax.numpy as jnp
from jax import lax
from jax.experimental import pallas as pl
from jax.experimental.pallas import tpu as pltpu
from jax.sharding import PartitionSpec as P

MESH = pl.DeviceIdType.MESH
STEPS = 4
CUTOFF = 2.5
CELL_SIDE = 2.6
TIME_STEP = 0.005
BATH_STRENGTH = 0.25
GOAL_WARMTH = 0.8
FORCE_EDGE = 24.0 * (2.0 * CUTOFF ** (-13) - CUTOFF ** (-7))
ENERGY_EDGE = 4.0 * (CUTOFF ** (-12) - CUTOFF ** (-6))
FAR = 1.0e15


GROUPS = (("z", "core"), ("xl", "xh", "y"))


def parts_of(axes):
    gx, gy, gz = axes
    return {"xl": gx // 4, "y": 4, "xh": gy // 2, "core": 2, "z": gz}


def members(axes, group):
    sizes = parts_of(axes)
    every = itertools.product(*[range(sizes[a]) for a in group])
    return [dict(zip(group, d)) for d in every if any(d)]


def offsets_of(size):
    return [0] if size == 1 else [0, 1] if size == 2 else [0, 1, -1]


def kernel(
    axes, shape, o_in, v_in, occ_in, result,
    ostate, vstate, near, osend, orecv, oedge, oedges, fsend, frecv, fedge, fedges, held, tally, count, history,
    sums, gathered, o_send_sem, o_recv_sem, f_send_sem, f_recv_sem, s_send_sems, s_recv_sems,
):
    gx, gy, gz = axes
    nx, ny, nz, slots = shape
    lanes = nz * slots
    tile = fsend.shape[2]
    devices = gx * gy * gz
    slot_total = float(devices * nx * ny * lanes)
    me = [lax.axis_index(a) for a in ("gx", "gy", "gz")]
    sizes = parts_of(axes)
    place = {"xl": me[0] // 4, "y": lax.rem(me[0], 4), "xh": me[1] // 2, "core": lax.rem(me[1], 2), "z": me[2]}
    peers = [members(axes, group) for group in GROUPS]

    def member(d, sign):
        at = dict(place)
        for a, o in d.items():
            if o:
                at[a] = lax.rem(at[a] + (o if sign > 0 else sizes[a] - o), sizes[a])
        return (at["xl"] * 4 + at["y"], at["xh"] * 2 + at["core"], at["z"])

    turned = [[lax.rem(me[i] + j, n) for j in range(n)] for i, n in enumerate(axes)]

    def device(d):
        return tuple(turned[i][d[i] % axes[i]] for i in range(3))

    def canonical(size, off):
        return 0 if size == 1 else off % 2 if size == 2 else off

    def padded(size, n):
        return (
            [(canonical(size, -1), n - 1)]
            + [(0, i) for i in range(n)]
            + [(canonical(size, 1), 0)]
        )

    px_of, py_of = padded(gx, nx), padded(gy, ny)
    xs = offsets_of(gx)
    partners = [
        (a, b, c) for a in xs for b in offsets_of(gy) for c in offsets_of(gz) if (a, b, c) != (0, 0, 0)
    ]
    slot_of = {d: i for i, d in enumerate(partners)}
    level_of = [i for i, d in enumerate(partners) if d[2] == 0]
    level_slot = {partners[i]: j for j, i in enumerate(level_of)}

    def layers_of(b):
        return sorted({yl for off, yl in py_of if off == b})

    def copies_of(send, recv, edge, edges, send_sem, recv_sem):
        copies = []
        for i, d in reversed([*enumerate(partners)]):
            need = layers_of(d[1])
            where = pl.ds(need[0], len(need))
            if d[2] == 0:
                src, dst = send.at[where], recv.at[level_slot[d], where]
            else:
                src, dst = edge.at[0 if d[2] == 1 else 1, where], edges.at[i, pl.ds(0, len(need))]
            copies.append(pltpu.make_async_remote_copy(
                src_ref=src, dst_ref=dst, send_sem=send_sem.at[i], recv_sem=recv_sem.at[i],
                device_id=device(tuple(-x for x in d)), device_id_type=MESH,
            ))
        return copies

    def spread_of(stage, p):
        at = 0
        for a in GROUPS[stage]:
            at = at * sizes[a] + place[a]
        return at, [
            pltpu.make_async_remote_copy(
                src_ref=sums.at[stage], dst_ref=gathered[stage].at[p, at],
                send_sem=s_send_sems[stage].at[i], recv_sem=s_recv_sems[stage].at[p, i],
                device_id=member(d, -1), device_id_type=MESH,
            )
            for i, d in enumerate(peers[stage])
        ]

    barrier = pltpu.get_barrier_semaphore()

    for d in partners:
        pl.semaphore_signal(barrier, inc=1, device_id=device(d), device_id_type=MESH)
    for group in peers:
        for d in group:
            pl.semaphore_signal(barrier, inc=1, device_id=member(d, 1), device_id_type=MESH)

    lane = lax.broadcasted_iota(jnp.int32, (nz, lanes), 1)
    level = lax.broadcasted_iota(jnp.int32, (nz, lanes), 0)
    spread = (
        lax.rem(lax.broadcasted_iota(jnp.int32, (slots, lanes), 1), slots)
        == lax.broadcasted_iota(jnp.int32, (slots, lanes), 0)
    ).astype(jnp.float32)

    def rows_of(planes):
        flat = planes.reshape(-1, slots)
        wide = jnp.dot(flat, spread, precision=lax.Precision.HIGHEST, preferred_element_type=jnp.float32)
        wide = wide.reshape(-1, nz, lanes)
        return jnp.sum(jnp.where((lane // slots == level)[None], wide, 0.0), axis=1)

    o_rows = rows_of(o_in[...])
    v_rows = rows_of(v_in[...])
    w_rows = rows_of(occ_in[...].astype(jnp.float32))
    osend[...] = jnp.zeros_like(osend)
    fsend[...] = jnp.zeros_like(fsend)
    for x in range(nx):
        for y in range(ny):
            w = w_rows[x * ny + y : x * ny + y + 1]
            for c in range(3):
                i = (x * ny + y) * 3 + c
                r = c * nx + x
                osend[y, 0, r : r + 1] = jnp.where(w > 0.5, o_rows[i : i + 1], FAR)
                osend[y, 1, r : r + 1] = v_rows[i : i + 1] * w
    tally[...] = jnp.sum(w_rows, axis=0, keepdims=True)

    tile_lane = lax.broadcasted_iota(jnp.int32, (tile, lanes), 1)
    tile_row = lax.broadcasted_iota(jnp.int32, (tile, lanes), 0)
    ends = [lax.rem(tile_lane, slots), lax.rem(tile_lane, slots) + (lanes - slots)]
    back = tile_row * slots + lax.rem(tile_lane, slots)

    def packed(block, side):
        taken = jnp.take_along_axis(block, ends[side], axis=1, mode="promise_in_bounds")
        return jnp.sum(jnp.where(tile_lane // slots == tile_row, taken, 0.0), axis=0, keepdims=True)

    def unpacked(row):
        wide = jnp.broadcast_to(row, (tile, lanes))
        return jnp.take_along_axis(wide, back, axis=1, mode="promise_in_bounds")

    for side in range(2):
        for y in range(ny):
            for q in range(2):
                oedge[side, y, q] = packed(osend[y, q], side)

    pl.semaphore_wait(barrier, len(partners) + sum(len(group) for group in peers))
    first = copies_of(osend, orecv, oedge, oedges, o_send_sem, o_recv_sem)
    for copy in first:
        copy.start()
    for copy in first:
        copy.wait()

    edge_lane = tile_lane

    def columns(own, level_block, edge_row):
        found = {}
        for xi, a in enumerate(xs):
            for py, (b, yl) in enumerate(py_of):
                mid = own(yl) if (a, b) == (0, 0) else level_block(level_slot[a, b, 0], yl)
                found[xi, py, 1] = mid
                at = layers_of(b).index(yl)
                below, above = (unpacked(edge_row((a, b, c), at)) for c in (-1, 1))
                low = jnp.where(edge_lane >= lanes - slots, below, mid)
                found[xi, py, 0] = pltpu.roll(low, slots, 1)
                high = jnp.where(edge_lane < slots, above, mid)
                found[xi, py, 2] = pltpu.roll(high, lanes - slots, 1)
        return found

    for q, state in enumerate((ostate, vstate)):
        found = columns(
            lambda yl: osend[yl, q], lambda s, yl: orecv[s, yl, q], lambda d, at: oedges[slot_of[d], at, q]
        )
        for (xi, py, dz), value in found.items():
            state[xi, py, dz] = value

    lane_id = lax.broadcasted_iota(jnp.int32, (slots, lanes), 1)
    slot_id = lax.broadcasted_iota(jnp.int32, (slots, lanes), 0)
    pick = (lane_id // slots) * slots + slot_id
    itself = lax.rem(lane_id, slots) == slot_id

    def nearby(py, _):
        for px, (a, xl) in enumerate(px_of):
            for dz in range(3):
                for c in range(3):
                    r = c * nx + xl
                    row = jnp.broadcast_to(ostate[xs.index(a), py, dz, r : r + 1], (slots, lanes))
                    near[px, py, dz, c] = jnp.take_along_axis(row, pick, axis=1, mode="promise_in_bounds")
        return 0

    half = 0.5 * TIME_STEP

    def step(k, _):
        p = lax.rem(k, 2)
        for py in range(ny + 2):
            nearby(py, 0)

        energy_rows = jnp.zeros((1, lanes), jnp.float32)
        for x in range(nx):
            def one_row(y, carried):
                block = ostate[0, y + 1, 1]
                mine = [block[c * nx + x : c * nx + x + 1] for c in range(3)]
                occupied = mine[0] < 0.5 * FAR
                force = [jnp.zeros((slots, lanes), jnp.float32) for _ in range(3)]
                bonds, reach, pairs = (jnp.zeros((slots, lanes), jnp.float32) for _ in range(3))
                for dx in (-1, 0, 1):
                    for dy in (-1, 0, 1):
                        for dz in (-1, 0, 1):
                            shift = (dx, dy, dz)
                            apart = [
                                near[x + 1 + dx, y + 1 + dy, dz + 1, c] - (mine[c] - shift[c] * CELL_SIDE)
                                for c in range(3)
                            ]
                            squared = apart[0] * apart[0] + apart[1] * apart[1] + apart[2] * apart[2]
                            if shift == (0, 0, 0):
                                squared = jnp.where(itself, FAR, squared)
                            inside = squared < CUTOFF * CUTOFF
                            inv = jnp.where(inside, lax.rsqrt(squared), 0.0)
                            inv2 = inv * inv
                            inv6 = inv2 * inv2 * inv2
                            less = inv6 - 1.0
                            pull = inv * (FORCE_EDGE / 24.0 - inv * inv6 * (inv6 + less))
                            for c in range(3):
                                force[c] = force[c] + pull * apart[c]
                            bonds = bonds + inv6 * less
                            reach = reach + squared * inv
                            pairs = pairs + jnp.where(inside, 1.0, 0.0)
                for c in range(3):
                    total = 24.0 * jnp.sum(force[c], axis=0, keepdims=True)
                    fsend[p, y, c * nx + x : c * nx + x + 1] = jnp.where(occupied, total, 0.0)
                energy = 4.0 * bonds + FORCE_EDGE * reach - (ENERGY_EDGE + CUTOFF * FORCE_EDGE) * pairs
                total = jnp.sum(energy, axis=0, keepdims=True)
                return carried + jnp.where(occupied, total, 0.0)

            for y in range(ny):
                energy_rows = one_row(y, energy_rows)

        kinetic = jnp.zeros((tile, lanes), jnp.float32)
        for y in range(ny):
            v = vstate[0, y + 1, 1] + half * jnp.where(tile_row < 3 * nx, fsend[p, y], 0.0)
            kinetic = kinetic + v * v
        kinetic = jnp.sum(kinetic, axis=0, keepdims=True)
        kinetic = jnp.where(k == 0, tally[...], 0.5 * kinetic)
        potential = 0.5 * energy_rows
        first_half = lane[:1] < lanes // 2
        row = jnp.where(first_half, kinetic, potential) + pltpu.roll(
            jnp.where(first_half, potential, kinetic), lanes // 2, 1
        )
        sums[0] = row
        at, spread = spread_of(0, p)
        for copy in spread:
            copy.start()
        gathered[0][p, at] = row

        for side in range(2):
            for y in range(ny):
                fedge[p, side, y] = packed(fsend[p, y], side)
        halo = copies_of(fsend.at[p], frecv.at[p], fedge.at[p], fedges.at[p], f_send_sem, f_recv_sem.at[p])
        for copy in halo:
            copy.start()

        def total_of(stage):
            parts = [gathered[stage][p, i] for i in range(len(peers[stage]) + 1)]
            while len(parts) > 1:
                parts = [sum(parts[i + 1 : i + 2], parts[i]) for i in range(0, len(parts), 2)]
            return parts[0]

        for stage in range(1, len(GROUPS)):
            for copy in spread:
                copy.wait()
            row = total_of(stage - 1)
            sums[stage] = row
            at, spread = spread_of(stage, p)
            for copy in spread:
                copy.start()
            gathered[stage][p, at] = row

        for copy in halo:
            copy.wait()
        found = columns(
            lambda yl: fsend[p, yl], lambda s, yl: frecv[p, s, yl], lambda d, at: fedges[p, slot_of[d], at]
        )
        before = jnp.where(k > 0, half, 0.0)
        for (xi, py, dz), f in found.items():
            f = jnp.where(tile_row < 3 * nx, f, 0.0)
            held[xi, py, dz] = half * f
            vstate[xi, py, dz] = vstate[xi, py, dz] + before * f

        for copy in spread:
            copy.wait()
        row = total_of(len(GROUPS) - 1)
        vigor = jnp.sum(jnp.where(first_half, row, 0.0), axis=1, keepdims=True)
        potential = jnp.sum(jnp.where(first_half, 0.0, row), axis=1, keepdims=True)

        @pl.when(k == 0)
        def _():
            count[...] = jnp.broadcast_to(vigor, (1, lanes))

        vigor, potential = (jnp.broadcast_to(t, (1, lanes)) for t in (vigor, potential))
        warmth = 2.0 * vigor / (3.0 * count[...])
        lam = jnp.where(k == 0, 1.0, jnp.sqrt(1.0 + BATH_STRENGTH * (GOAL_WARMTH / warmth - 1.0)))
        which = lax.broadcasted_iota(jnp.int32, (2, lanes), 1)
        record = jnp.concatenate([potential, lam * lam * vigor], axis=0) / slot_total
        history[...] = jnp.where(which == k - 1, record, history[...])

        @pl.when(k < STEPS)
        def _():
            for xi, py, dz in found:
                v = vstate[xi, py, dz] * lam + held[xi, py, dz]
                vstate[xi, py, dz] = v
                ostate[xi, py, dz] = ostate[xi, py, dz] + TIME_STEP * v

        @pl.when(k == STEPS)
        def _():
            for y in range(ny):
                result[y] = ostate[0, y + 1, 1]
                result[ny + y] = vstate[0, y + 1, 1] * lam
                result[2 * ny + y] = fsend[p, y]
            result[3 * ny, 0:2] = history[...]

        return 0

    history[...] = jnp.zeros_like(history)
    lax.fori_loop(0, STEPS + 1, step, 0)


def unpack(shape, result, o_in, occ_in, o_out, v_out, f_out, h_out):
    nx, ny, nz, slots = shape
    lanes = nz * slots
    at = lax.broadcasted_iota(jnp.int32, (nz, lanes), 0) * slots + lax.rem(
        lax.broadcasted_iota(jnp.int32, (nz, lanes), 1), slots
    )
    for i, ref in enumerate((o_out, v_out, f_out)):
        for y in range(ny):
            for x in range(nx):
                for c in range(3):
                    r = c * nx + x
                    row = jnp.broadcast_to(result[i * ny + y, r : r + 1], (nz, lanes))
                    plane = jnp.take_along_axis(row, at, axis=1, mode="promise_in_bounds")[:, :slots]
                    if i == 0:
                        plane = jnp.where(occ_in[x, y] > 0, plane, o_in[x, y, c])
                    ref[x, y, c] = plane
    h_out[...] = result[3 * ny, 0:2, :STEPS]


def shards(axes, offsets, velocities, occupied):
    gx, gy, gz = axes
    nx, ny, nz, slots = occupied.shape
    lanes = nz * slots
    tile = lanes // slots
    assert gz > 2 and tile >= 3 * nx + 2
    nxo, nyo, nzo = (len(offsets_of(s)) for s in axes)
    halo = nxo * nyo * nzo - 1
    level = nxo * nyo - 1
    others = [len(members(axes, group)) for group in GROUPS]
    f32 = jnp.float32
    plane = jax.ShapeDtypeStruct((nx, ny, 3, nz, slots), f32)
    vmem = pl.BlockSpec(memory_space=pltpu.VMEM)
    dma = pltpu.SemaphoreType.DMA
    o_planes = jnp.transpose(offsets, (0, 1, 4, 2, 3))
    result = pl.pallas_call(
        functools.partial(kernel, axes, (nx, ny, nz, slots)),
        name="verlet",
        out_shape=jax.ShapeDtypeStruct((3 * ny + 1, tile, lanes), f32),
        in_specs=[vmem] * 3,
        out_specs=vmem,
        scratch_shapes=[
            pltpu.VMEM((nxo, ny + 2, 3, tile, lanes), f32),
            pltpu.VMEM((nxo, ny + 2, 3, tile, lanes), f32),
            pltpu.VMEM((nx + 2, ny + 2, 3, 3, slots, lanes), f32),
            pltpu.VMEM((ny, 2, tile, lanes), f32),
            pltpu.VMEM((max(level, 1), ny, 2, tile, lanes), f32),
            pltpu.VMEM((2, ny, 2, 1, lanes), f32),
            pltpu.VMEM((halo, ny, 2, 1, lanes), f32),
            pltpu.VMEM((2, ny, tile, lanes), f32),
            pltpu.VMEM((2, max(level, 1), ny, tile, lanes), f32),
            pltpu.VMEM((2, 2, ny, 1, lanes), f32),
            pltpu.VMEM((2, halo, ny, 1, lanes), f32),
            pltpu.VMEM((nxo, ny + 2, 3, tile, lanes), f32),
            pltpu.VMEM((1, lanes), f32),
            pltpu.VMEM((1, lanes), f32),
            pltpu.VMEM((2, lanes), f32),
            pltpu.VMEM((len(GROUPS), 1, lanes), f32),
            [pltpu.VMEM((2, n + 1, 1, lanes), f32) for n in others],
            dma((halo,)),
            dma((halo,)),
            dma((halo,)),
            dma((2, halo)),
            [dma((n,)) for n in others],
            [dma((2, n)) for n in others],
        ],
        compiler_params=pltpu.CompilerParams(collective_id=0, has_side_effects=True),
    )(
        o_planes,
        jnp.transpose(velocities, (0, 1, 4, 2, 3)),
        occupied,
    )
    o, v, f, h = pl.pallas_call(
        functools.partial(unpack, (nx, ny, nz, slots)),
        name="unpack",
        out_shape=[plane, plane, plane, jax.ShapeDtypeStruct((2, STEPS), f32)],
        in_specs=[vmem] * 3,
        out_specs=[vmem] * 4,
    )(result, o_planes, occupied)
    back = (0, 1, 3, 4, 2)
    return (jnp.transpose(o, back), jnp.transpose(v, back), jnp.transpose(f, back), h.T)


def solution(mesh):
    axes = tuple(mesh.shape[a] for a in ("gx", "gy", "gz"))
    in_specs = (
        P("gx", "gy", "gz", None, None),
        P("gx", "gy", "gz", None, None),
        P("gx", "gy", "gz", None),
    )
    out_specs = (
        P("gx", "gy", "gz", None, None),
        P("gx", "gy", "gz", None, None),
        P("gx", "gy", "gz", None, None),
        P(),
    )
    return jax.shard_map(
        functools.partial(shards, axes), mesh=mesh, in_specs=in_specs, out_specs=out_specs, check_vma=False
    )
```

```python
import functools
import itertools

import jax
import jax.numpy as jnp
from jax import lax
from jax.experimental import pallas as pl
from jax.experimental.pallas import tpu as pltpu
from jax.sharding import PartitionSpec as P

MESH = pl.DeviceIdType.MESH
STEPS = 4
CUTOFF = 2.5
CELL_SIDE = 2.6
TIME_STEP = 0.005
BATH_STRENGTH = 0.25
GOAL_WARMTH = 0.8
FORCE_EDGE = 24.0 * (2.0 * CUTOFF ** (-13) - CUTOFF ** (-7))
ENERGY_EDGE = 4.0 * (CUTOFF ** (-12) - CUTOFF ** (-6))
FAR = 32.0


NEAR = ("z",)
WIDE = ("xl", "xh", "y")


def parts_of(axes):
    gx, gy, gz = axes
    return {"xl": gx // 4, "y": 4, "xh": gy // 2, "z": gz}


def chips_of(axes, group):
    sizes = parts_of(axes)

    def hops(d):
        return sum(min(o, sizes[a] - o) for a, o in d.items())

    every = itertools.product(*[range(sizes[a]) for a in group])
    return sorted((dict(zip(group, d)) for d in every), key=lambda d: -hops(d))


def offsets_of(size):
    return [0] if size == 1 else [0, 1] if size == 2 else [0, 1, -1]


def canonical(size, off):
    return 0 if size == 1 else off % 2 if size == 2 else off


def padded(size, n):
    return [(canonical(size, -1), n - 1)] + [(0, i) for i in range(n)] + [(canonical(size, 1), 0)]


def partners_of(axes, ny):
    every = itertools.product(*[offsets_of(n) for n in axes])
    flat, rows, found = 0, 0, {}
    for d in every:
        if d == (0, 0, 0):
            continue
        need = sorted({yl for off, yl in padded(axes[1], ny) if off == d[1]})
        if d[2] == 0:
            found[d] = need, flat
            flat += len(need)
        else:
            found[d] = need, rows
            rows += len(need)
    return found, flat, rows


def kernel(
    axes, shape, o_in, v_in, occ_in, result,
    ostate, vstate, held, near, osend, orecv, oedge, oedges, vsend, vrecv, vedge, vedges,
    fsend, frecv, fedge, fedges, tally, history, scale, row_sum, near_sums, chip_sum, wide_sums, wide_out,
    o_sem, v_sem, f_send_sem, f_recv_sem, near_send, near_recv, wide_send, wide_recv,
):
    gx, gy, gz = axes
    nx, ny, nz, slots = shape
    lanes = nz * slots
    tile = fsend.shape[2]
    slot_total = float(gx * gy * gz * nx * ny * lanes)
    me = [lax.axis_index(a) for a in ("gx", "gy", "gz")]
    sizes = parts_of(axes)
    place = {"xl": me[0] // 4, "y": lax.rem(me[0], 4), "xh": me[1] // 2, "z": me[2]}
    core = lax.rem(me[1], 2)
    leads = core == 1
    follows = core == 0
    near_chips, wide_chips = chips_of(axes, NEAR), chips_of(axes, WIDE)

    turned = [[lax.rem(me[i] + j, n) for j in range(n)] for i, n in enumerate(axes)]

    def device(d):
        return tuple(turned[i][d[i] % axes[i]] for i in range(3))

    def member(d, sign, which):
        at = dict(place)
        for a, o in d.items():
            if o:
                at[a] = lax.rem(at[a] + (o if sign > 0 else sizes[a] - o), sizes[a])
        return (at["xl"] * 4 + at["y"], at["xh"] * 2 + which, at["z"])

    def index_in(group):
        at = 0
        for a in group:
            at = at * sizes[a] + place[a]
        return at

    px_of, py_of = padded(gx, nx), padded(gy, ny)
    xs = offsets_of(gx)
    partners, flats, rows = partners_of(axes, ny)

    def remote(src, dst, send_sem, recv_sem, to):
        return pltpu.make_async_remote_copy(
            src_ref=src, dst_ref=dst, send_sem=send_sem, recv_sem=recv_sem, device_id=to, device_id_type=MESH
        )

    def copies_of(send, recv, edge, edges, send_sem, recv_sem):
        copies = []
        for d, (need, at) in reversed([*partners.items()]):
            where = pl.ds(need[0], len(need))
            to = device(tuple(-x for x in d))
            if d[2] == 0:
                copies.append(remote(send.at[where], recv.at[pl.ds(at, len(need))], send_sem.at[0], recv_sem.at[0], to))
            else:
                src = edge.at[0 if d[2] == 1 else 1, where]
                copies.append(remote(src, edges.at[pl.ds(at, len(need))], send_sem.at[1], recv_sem.at[1], to))
        return copies

    def await_all(ref, sem):
        pltpu.make_async_copy(ref, ref, sem).wait()

    def await_halo(recv, edges, sem):
        await_all(recv, sem.at[0])
        await_all(edges, sem.at[1])

    barrier = pltpu.get_barrier_semaphore()

    greeted = [device(d) for d in partners]
    greeted += [member(d, 1, which) for group in (near_chips, wide_chips) for d in group if any(d.values()) for which in (0, 1)]
    greeted.append(member({}, 1, 1 - core))
    for to in greeted:
        pl.semaphore_signal(barrier, inc=1, device_id=to, device_id_type=MESH)

    lane = lax.broadcasted_iota(jnp.int32, (nz, lanes), 1)
    level = lax.broadcasted_iota(jnp.int32, (nz, lanes), 0)
    spread = (
        lax.rem(lax.broadcasted_iota(jnp.int32, (slots, lanes), 1), slots)
        == lax.broadcasted_iota(jnp.int32, (slots, lanes), 0)
    ).astype(jnp.float32)

    def rows_of(planes):
        flat = planes.reshape(-1, slots)
        wide = jnp.dot(flat, spread, precision=lax.Precision.HIGHEST, preferred_element_type=jnp.float32)
        wide = wide.reshape(-1, nz, lanes)
        return jnp.sum(jnp.where((lane // slots == level)[None], wide, 0.0), axis=1)

    o_rows = rows_of(o_in[...])
    v_rows = rows_of(v_in[...])
    w_rows = rows_of(occ_in[...].astype(jnp.float32))
    osend[...] = jnp.zeros_like(osend)
    vsend[...] = jnp.zeros_like(vsend)
    fsend[...] = jnp.zeros_like(fsend)
    for x in range(nx):
        for y in range(ny):
            w = w_rows[x * ny + y : x * ny + y + 1]
            for c in range(3):
                i = (x * ny + y) * 3 + c
                r = c * nx + x
                osend[y, r : r + 1] = jnp.where(w > 0.5, o_rows[i : i + 1], FAR)
                vsend[y, r : r + 1] = v_rows[i : i + 1] * w

    quarter = lanes // 4
    row_lane = lane[:1]

    def folded(row, times):
        for i in range(times):
            row = row + pltpu.roll(row, lanes >> (i + 1), 1)
        return row

    tally[...] = folded(jnp.sum(w_rows, axis=0, keepdims=True), 2)

    tile_lane = lax.broadcasted_iota(jnp.int32, (tile, lanes), 1)
    tile_row = lax.broadcasted_iota(jnp.int32, (tile, lanes), 0)
    ends = [lax.rem(tile_lane, slots), lax.rem(tile_lane, slots) + (lanes - slots)]
    back = tile_row * slots + lax.rem(tile_lane, slots)

    def packed(block, side):
        taken = jnp.take_along_axis(block, ends[side], axis=1, mode="promise_in_bounds")
        return jnp.sum(jnp.where(tile_lane // slots == tile_row, taken, 0.0), axis=0, keepdims=True)

    def unpacked(row):
        wide = jnp.broadcast_to(row, (tile, lanes))
        return jnp.take_along_axis(wide, back, axis=1, mode="promise_in_bounds")

    for side in range(2):
        for y in range(ny):
            oedge[side, y] = packed(osend[y], side)
            vedge[side, y] = packed(vsend[y], side)

    pl.semaphore_wait(barrier, len(greeted))
    for copy in copies_of(osend, orecv, oedge, oedges, o_sem.at[0], o_sem.at[1]):
        copy.start()
    for copy in copies_of(vsend, vrecv, vedge, vedges, v_sem.at[0], v_sem.at[1]):
        copy.start()

    def columns(send, recv, edges):
        found = {}
        for xi, a in enumerate(xs):
            for py, (b, yl) in enumerate(py_of):
                if (a, b) == (0, 0):
                    mid = send[yl]
                else:
                    need, at = partners[a, b, 0]
                    mid = recv[at + need.index(yl)]
                ends_of = []
                for c in (-1, 1):
                    need, at = partners[a, b, c]
                    ends_of.append(unpacked(edges[at + need.index(yl)]))
                below, above = ends_of
                found[xi, py, 1] = mid
                low = jnp.where(tile_lane >= lanes - slots, below, mid)
                found[xi, py, 0] = pltpu.roll(low, slots, 1)
                high = jnp.where(tile_lane < slots, above, mid)
                found[xi, py, 2] = pltpu.roll(high, lanes - slots, 1)
        return found

    await_halo(orecv, oedges, o_sem.at[1])
    for (xi, py, dz), value in columns(osend, orecv, oedges).items():
        ostate[xi, py, dz] = value

    lane_id = lax.broadcasted_iota(jnp.int32, (slots, lanes), 1)
    slot_id = lax.broadcasted_iota(jnp.int32, (slots, lanes), 0)
    pick = (lane_id // slots) * slots + slot_id
    itself = lax.rem(lane_id, slots) == slot_id

    def nearby(py):
        for px, (a, xl) in enumerate(px_of):
            for dz in range(3):
                for c in range(3):
                    r = c * nx + xl
                    row = jnp.broadcast_to(ostate[xs.index(a), py, dz, r : r + 1], (slots, lanes))
                    near[px, py, dz, c] = jnp.take_along_axis(row, pick, axis=1, mode="promise_in_bounds")

    half = 0.5 * TIME_STEP
    reach2 = CUTOFF * CUTOFF

    def terms(squared):
        inv = lax.rsqrt(squared)
        inv2 = inv * inv
        inv6 = inv2 * inv2 * inv2
        inv12 = inv6 * inv6
        bond = inv12 - inv6
        return inv, bond, inv * (bond + inv12)

    _, _, edge = terms(jnp.full((slots, lanes), reach2, jnp.float32))
    pair_count = 27.0 * slots

    def step(k, _):
        p = lax.rem(k, 2)
        for py in range(ny + 2):
            nearby(py)

        energy_rows = jnp.zeros((1, lanes), jnp.float32)
        for x in range(nx):
            for y in range(ny):
                block = ostate[0, y + 1, 1]
                mine = [block[c * nx + x : c * nx + x + 1] for c in range(3)]
                occupied = mine[0] < 0.5 * FAR
                force = [jnp.zeros((slots, lanes), jnp.float32) for _ in range(3)]
                bonds, reach = (jnp.zeros((slots, lanes), jnp.float32) for _ in range(2))
                for shift in itertools.product((-1, 0, 1), repeat=3):
                    dx, dy, dz = shift
                    apart = [
                        near[x + 1 + dx, y + 1 + dy, dz + 1, c] - (mine[c] - shift[c] * CELL_SIDE)
                        for c in range(3)
                    ]
                    squared = apart[0] * apart[0] + apart[1] * apart[1] + apart[2] * apart[2]
                    if shift == (0, 0, 0):
                        squared = jnp.where(itself, reach2, squared)
                    squared = jnp.minimum(squared, reach2)
                    inv, bond, push = terms(squared)
                    pull = inv * (edge - push)
                    for c in range(3):
                        force[c] = force[c] + pull * apart[c]
                    bonds = bonds + bond
                    reach = reach + squared * inv
                for c in range(3):
                    total = 24.0 * jnp.sum(force[c], axis=0, keepdims=True)
                    fsend[p, y, c * nx + x : c * nx + x + 1] = jnp.where(occupied, total, 0.0)
                energy = 4.0 * bonds + FORCE_EDGE * reach
                total = jnp.sum(energy, axis=0, keepdims=True)
                total = total - pair_count * (ENERGY_EDGE + CUTOFF * FORCE_EDGE)
                energy_rows = energy_rows + jnp.where(occupied, total, 0.0)

        @pl.when(k > 0)
        def _():
            kinetic = jnp.zeros((tile, lanes), jnp.float32)
            for y in range(ny):
                v = vstate[0, y + 1, 1] + half * fsend[p, y]
                kinetic = kinetic + v * v
            kinetic = folded(jnp.sum(kinetic, axis=0, keepdims=True), 1)
            potential = folded(energy_rows, 2)
            row = jnp.where(
                row_lane < 2 * quarter, 0.5 * kinetic, jnp.where(row_lane < 3 * quarter, 0.5 * potential, tally[...])
            )
            row_sum[...] = row
            at = index_in(NEAR) * 2 + core
            for d in near_chips:
                if any(d.values()):
                    remote(row_sum, near_sums.at[p, at], near_send, near_recv.at[p], member(d, -1, 1)).start()

            @pl.when(follows)
            def _():
                remote(row_sum, near_sums.at[p, at], near_send, near_recv.at[p], member({}, 1, 1)).start()

            @pl.when(leads)
            def _():
                near_sums[p, at] = row

        @pl.when(k < STEPS)
        def _():
            for side in range(2):
                for y in range(ny):
                    fedge[p, side, y] = packed(fsend[p, y], side)
            for copy in copies_of(
                fsend.at[p], frecv.at[p], fedge.at[p], fedges.at[p], f_send_sem, f_recv_sem.at[p]
            ):
                copy.start()

        def total_of(ref, n):
            parts = [ref[p, i] for i in range(n)]
            while len(parts) > 1:
                parts = [sum(parts[i + 1 : i + 2], parts[i]) for i in range(0, len(parts), 2)]
            return parts[0]

        n_near, n_wide = len(near_chips), len(wide_chips)

        @pl.when((k > 0) & leads)
        def _():
            await_all(near_sums.at[p, pl.ds(0, 2 * n_near - 1)], near_recv.at[p])
            row = total_of(near_sums, 2 * n_near)
            chip_sum[...] = row
            at = index_in(WIDE)
            for d in wide_chips:
                for which in (0, 1):
                    if which == 0 or any(d.values()):
                        remote(
                            chip_sum, wide_sums.at[p, at], wide_send, wide_recv.at[p], member(d, -1, which)
                        ).start()
            wide_sums[p, at] = row

        @pl.when(k == 0)
        def _():
            await_halo(vrecv, vedges, v_sem.at[1])
            for (xi, py, dz), value in columns(vsend, vrecv, vedges).items():
                vstate[xi, py, dz] = value

        @pl.when(k < STEPS)
        def _():
            await_halo(frecv.at[p], fedges.at[p], f_recv_sem.at[p])
            await_halo(frecv.at[p], fedges.at[p], f_send_sem)
            before = jnp.where(k > 0, half, 0.0)
            for (xi, py, dz), f in columns(fsend.at[p], frecv.at[p], fedges.at[p]).items():
                vstate[xi, py, dz] = vstate[xi, py, dz] + before * f
                held[xi, py, dz] = half * f

        @pl.when(k > 0)
        def _():
            @pl.when(leads)
            def _():
                await_all(near_sums.at[p, pl.ds(0, n_near - 1)], near_send)
                await_all(wide_sums.at[p, pl.ds(0, n_wide - 1)], wide_recv.at[p])

            @pl.when(follows)
            def _():
                await_all(near_sums.at[p, pl.ds(0, n_near)], near_send)
                await_all(wide_sums.at[p], wide_recv.at[p])

            row = total_of(wide_sums, n_wide)

            def across(low, high):
                picked = jnp.where((row_lane >= low * quarter) & (row_lane < high * quarter), row, 0.0)
                return jnp.broadcast_to(jnp.sum(picked, axis=1, keepdims=True), (1, lanes))

            vigor, potential, count = across(0, 2), across(2, 3), across(3, 4)
            square = (1.0 - BATH_STRENGTH) + (BATH_STRENGTH * GOAL_WARMTH * 1.5) * count / vigor
            which = lax.broadcasted_iota(jnp.int32, (2, lanes), 1)
            record = jnp.concatenate([potential, square * vigor], axis=0) / slot_total
            history[...] = jnp.where(which == k - 1, record, history[...])
            scale[...] = jnp.sqrt(square)

            @pl.when(leads)
            def _():
                await_all(wide_out, wide_send)

        lam = scale[...]

        @pl.when(k < STEPS)
        def _():
            for xi in range(len(xs)):
                for py in range(ny + 2):
                    for dz in range(3):
                        v = vstate[xi, py, dz] * lam + held[xi, py, dz]
                        vstate[xi, py, dz] = v
                        ostate[xi, py, dz] = ostate[xi, py, dz] + TIME_STEP * v

        @pl.when(k == STEPS)
        def _():
            for y in range(ny):
                result[y] = ostate[0, y + 1, 1]
                result[ny + y] = (vstate[0, y + 1, 1] + half * fsend[p, y]) * lam
                result[2 * ny + y] = fsend[p, y]
            result[3 * ny, 0:2] = history[...]

        return 0

    history[...] = jnp.zeros_like(history)
    scale[...] = jnp.ones_like(scale)
    lax.fori_loop(0, STEPS + 1, step, 0)
    await_halo(orecv, oedges, o_sem.at[0])
    await_halo(vrecv, vedges, v_sem.at[0])


def unpack(shape, result, o_in, occ_in, o_out, v_out, f_out, h_out):
    nx, ny, nz, slots = shape
    lanes = nz * slots
    at = lax.broadcasted_iota(jnp.int32, (nz, lanes), 0) * slots + lax.rem(
        lax.broadcasted_iota(jnp.int32, (nz, lanes), 1), slots
    )
    for i, ref in enumerate((o_out, v_out, f_out)):
        for y in range(ny):
            for x in range(nx):
                for c in range(3):
                    r = c * nx + x
                    row = jnp.broadcast_to(result[i * ny + y, r : r + 1], (nz, lanes))
                    plane = jnp.take_along_axis(row, at, axis=1, mode="promise_in_bounds")[:, :slots]
                    if i == 0:
                        plane = jnp.where(occ_in[x, y] > 0, plane, o_in[x, y, c])
                    ref[x, y, c] = plane
    h_out[...] = result[3 * ny, 0:2, :STEPS]


def shards(axes, offsets, velocities, occupied):
    nx, ny, nz, slots = occupied.shape
    lanes = nz * slots
    tile = lanes // slots
    assert axes[2] > 2 and tile >= 3 * nx
    _, flats, rows = partners_of(axes, ny)
    nxo = len(offsets_of(axes[0]))
    n_near, n_wide = (len(chips_of(axes, group)) for group in (NEAR, WIDE))
    f32 = jnp.float32
    plane = jax.ShapeDtypeStruct((nx, ny, 3, nz, slots), f32)
    vmem = pl.BlockSpec(memory_space=pltpu.VMEM)
    dma = pltpu.SemaphoreType.DMA
    o_planes = jnp.transpose(offsets, (0, 1, 4, 2, 3))
    state = pltpu.VMEM((nxo, ny + 2, 3, tile, lanes), f32)
    halo = [
        pltpu.VMEM((ny, tile, lanes), f32),
        pltpu.VMEM((flats, tile, lanes), f32),
        pltpu.VMEM((2, ny, 1, lanes), f32),
        pltpu.VMEM((rows, 1, lanes), f32),
    ]
    result = pl.pallas_call(
        functools.partial(kernel, axes, (nx, ny, nz, slots)),
        name="verlet",
        out_shape=jax.ShapeDtypeStruct((3 * ny + 1, tile, lanes), f32),
        in_specs=[vmem] * 3,
        out_specs=vmem,
        scratch_shapes=[
            state,
            state,
            state,
            pltpu.VMEM((nx + 2, ny + 2, 3, 3, slots, lanes), f32),
            *halo,
            *halo,
            pltpu.VMEM((2, ny, tile, lanes), f32),
            pltpu.VMEM((2, flats, tile, lanes), f32),
            pltpu.VMEM((2, 2, ny, 1, lanes), f32),
            pltpu.VMEM((2, rows, 1, lanes), f32),
            pltpu.VMEM((1, lanes), f32),
            pltpu.VMEM((2, lanes), f32),
            pltpu.VMEM((1, lanes), f32),
            pltpu.VMEM((1, lanes), f32),
            pltpu.VMEM((2, 2 * n_near, 1, lanes), f32),
            pltpu.VMEM((1, lanes), f32),
            pltpu.VMEM((2, n_wide, 1, lanes), f32),
            pltpu.VMEM((2 * n_wide - 1, 1, lanes), f32),
            dma((2, 2)),
            dma((2, 2)),
            dma((2,)),
            dma((2, 2)),
            dma,
            dma((2,)),
            dma,
            dma((2,)),
        ],
        compiler_params=pltpu.CompilerParams(collective_id=0, has_side_effects=True),
    )(
        o_planes,
        jnp.transpose(velocities, (0, 1, 4, 2, 3)),
        occupied,
    )
    o, v, f, h = pl.pallas_call(
        functools.partial(unpack, (nx, ny, nz, slots)),
        name="unpack",
        out_shape=[plane, plane, plane, jax.ShapeDtypeStruct((2, STEPS), f32)],
        in_specs=[vmem] * 3,
        out_specs=[vmem] * 4,
    )(result, o_planes, occupied)
    back = (0, 1, 3, 4, 2)
    return (jnp.transpose(o, back), jnp.transpose(v, back), jnp.transpose(f, back), h.T)


def solution(mesh):
    axes = tuple(mesh.shape[a] for a in ("gx", "gy", "gz"))
    in_specs = (
        P("gx", "gy", "gz", None, None),
        P("gx", "gy", "gz", None, None),
        P("gx", "gy", "gz", None),
    )
    out_specs = (
        P("gx", "gy", "gz", None, None),
        P("gx", "gy", "gz", None, None),
        P("gx", "gy", "gz", None, None),
        P(),
    )
    return jax.shard_map(
        functools.partial(shards, axes), mesh=mesh, in_specs=in_specs, out_specs=out_specs, check_vma=False
    )
```

```python
import functools
import itertools

import jax
import jax.numpy as jnp
from jax import lax
from jax.experimental import pallas as pl
from jax.experimental.pallas import tpu as pltpu
from jax.sharding import PartitionSpec as P

MESH = pl.DeviceIdType.MESH
STEPS = 4
CUTOFF = 2.5
CELL_SIDE = 2.6
TIME_STEP = 0.005
BATH_STRENGTH = 0.25
GOAL_WARMTH = 0.8
FORCE_EDGE = 24.0 * (2.0 * CUTOFF ** (-13) - CUTOFF ** (-7))
ENERGY_EDGE = 4.0 * (CUTOFF ** (-12) - CUTOFF ** (-6))
FAR = 32.0
VERLET_VMEM = 60 * 1024 * 1024
UNPACK_VMEM = 4 * 1024 * 1024


NEAR = ("z",)
WIDE = ("xl", "xh", "y")


def parts_of(axes):
    gx, gy, gz = axes
    return {"xl": gx // 4, "y": 4, "xh": gy // 2, "z": gz}


def chips_of(axes, group):
    sizes = parts_of(axes)

    def hops(d):
        return sum(min(o, sizes[a] - o) for a, o in d.items())

    every = itertools.product(*[range(sizes[a]) for a in group])
    return sorted((dict(zip(group, d)) for d in every), key=lambda d: -hops(d))


def offsets_of(size):
    return [0] if size == 1 else [0, 1] if size == 2 else [0, 1, -1]


def canonical(size, off):
    return 0 if size == 1 else off % 2 if size == 2 else off


def padded(size, n):
    return [(canonical(size, -1), n - 1)] + [(0, i) for i in range(n)] + [(canonical(size, 1), 0)]


def partners_of(axes, ny):
    every = itertools.product(*[offsets_of(n) for n in axes])
    flat, rows, found = 0, 0, {}
    for d in every:
        if d == (0, 0, 0):
            continue
        need = sorted({yl for off, yl in padded(axes[1], ny) if off == d[1]})
        if d[2] == 0:
            found[d] = need, flat
            flat += len(need)
        else:
            found[d] = need, rows
            rows += len(need)
    return found, flat, rows


def kernel(
    axes, shape, o_in, v_in, occ_in, result,
    planes_in, kept, ostate, vstate, held, near, osend, orecv, oedge, oedges, vsend, vrecv, vedge, vedges,
    occ_planes, fsend, frecv, fedge, fedges, tally, history, scale, row_sum, near_sums, chip_sum, wide_sums, wide_out,
    in_sem, o_sem, v_sem, f_send_sem, f_recv_sem, near_send, near_recv, wide_send, wide_recv,
):
    gx, gy, gz = axes
    nx, ny, nz, slots = shape
    lanes = nz * slots
    tile = fsend.shape[2]
    slot_total = float(gx * gy * gz * nx * ny * lanes)
    me = [lax.axis_index(a) for a in ("gx", "gy", "gz")]
    sizes = parts_of(axes)
    place = {"xl": me[0] // 4, "y": lax.rem(me[0], 4), "xh": me[1] // 2, "z": me[2]}
    core = lax.rem(me[1], 2)
    leads = core == 1
    follows = core == 0
    near_chips, wide_chips = chips_of(axes, NEAR), chips_of(axes, WIDE)

    turned = [[lax.rem(me[i] + j, n) for j in range(n)] for i, n in enumerate(axes)]

    def device(d):
        return tuple(turned[i][d[i] % axes[i]] for i in range(3))

    def member(d, sign, which):
        at = dict(place)
        for a, o in d.items():
            if o:
                at[a] = lax.rem(at[a] + (o if sign > 0 else sizes[a] - o), sizes[a])
        return (at["xl"] * 4 + at["y"], at["xh"] * 2 + which, at["z"])

    def index_in(group):
        at = 0
        for a in group:
            at = at * sizes[a] + place[a]
        return at

    px_of, py_of = padded(gx, nx), padded(gy, ny)
    xs = offsets_of(gx)
    partners, flats, rows = partners_of(axes, ny)

    def remote(src, dst, send_sem, recv_sem, to):
        return pltpu.make_async_remote_copy(
            src_ref=src, dst_ref=dst, send_sem=send_sem, recv_sem=recv_sem, device_id=to, device_id_type=MESH
        )

    def copies_of(send, recv, edge, edges, send_sem, recv_sem):
        copies = []
        for d, (need, at) in reversed([*partners.items()]):
            where = pl.ds(need[0], len(need))
            to = device(tuple(-x for x in d))
            if d[2] == 0:
                copies.append(remote(send.at[where], recv.at[pl.ds(at, len(need))], send_sem.at[0], recv_sem.at[0], to))
            else:
                src = edge.at[0 if d[2] == 1 else 1, where]
                copies.append(remote(src, edges.at[pl.ds(at, len(need))], send_sem.at[1], recv_sem.at[1], to))
        return copies

    def await_all(ref, sem):
        pltpu.make_async_copy(ref, ref, sem).wait()

    def await_halo(recv, edges, sem):
        await_all(recv, sem.at[0])
        await_all(edges, sem.at[1])

    barrier = pltpu.get_barrier_semaphore()

    greeted = [device(d) for d in partners]
    greeted += [member(d, 1, which) for group in (near_chips, wide_chips) for d in group if any(d.values()) for which in (0, 1)]
    greeted.append(member({}, 1, 1 - core))
    for to in greeted:
        pl.semaphore_signal(barrier, inc=1, device_id=to, device_id_type=MESH)

    loads = [
        pltpu.make_async_copy(o_in, planes_in.at[0], in_sem.at[0]),
        pltpu.make_async_copy(occ_in, occ_planes, in_sem.at[1]),
        pltpu.make_async_copy(v_in, planes_in.at[1], in_sem.at[2]),
    ]
    for load in loads:
        load.start()

    lane = lax.broadcasted_iota(jnp.int32, (nz, lanes), 1)
    level = lax.broadcasted_iota(jnp.int32, (nz, lanes), 0)
    spread = (
        lax.rem(lax.broadcasted_iota(jnp.int32, (slots, lanes), 1), slots)
        == lax.broadcasted_iota(jnp.int32, (slots, lanes), 0)
    ).astype(jnp.float32)

    def rows_of(planes):
        flat = planes.reshape(-1, slots)
        wide = jnp.dot(flat, spread, precision=lax.Precision.HIGHEST, preferred_element_type=jnp.float32)
        wide = wide.reshape(-1, nz, lanes)
        return jnp.sum(jnp.where((lane // slots == level)[None], wide, 0.0), axis=1)

    for load in loads:
        load.wait()
    o_rows = rows_of(planes_in[0])
    v_rows = rows_of(planes_in[1])
    w_rows = rows_of(occ_planes[...].astype(jnp.float32))
    osend[...] = jnp.zeros_like(osend)
    kept[...] = jnp.zeros_like(kept)
    vsend[...] = jnp.zeros_like(vsend)
    fsend[...] = jnp.zeros_like(fsend)
    for x in range(nx):
        for y in range(ny):
            w = w_rows[x * ny + y : x * ny + y + 1]
            for c in range(3):
                i = (x * ny + y) * 3 + c
                r = c * nx + x
                kept[y, r : r + 1] = o_rows[i : i + 1]
                osend[y, r : r + 1] = jnp.where(w > 0.5, o_rows[i : i + 1], FAR)
                vsend[y, r : r + 1] = v_rows[i : i + 1] * w

    quarter = lanes // 4
    row_lane = lane[:1]

    def folded(row, times):
        for i in range(times):
            row = row + pltpu.roll(row, lanes >> (i + 1), 1)
        return row

    tally[...] = folded(jnp.sum(w_rows, axis=0, keepdims=True), 2)

    tile_lane = lax.broadcasted_iota(jnp.int32, (tile, lanes), 1)
    tile_row = lax.broadcasted_iota(jnp.int32, (tile, lanes), 0)
    ends = [lax.rem(tile_lane, slots), lax.rem(tile_lane, slots) + (lanes - slots)]
    back = tile_row * slots + lax.rem(tile_lane, slots)

    def packed(block, side):
        taken = jnp.take_along_axis(block, ends[side], axis=1, mode="promise_in_bounds")
        return jnp.sum(jnp.where(tile_lane // slots == tile_row, taken, 0.0), axis=0, keepdims=True)

    def unpacked(row):
        wide = jnp.broadcast_to(row, (tile, lanes))
        return jnp.take_along_axis(wide, back, axis=1, mode="promise_in_bounds")

    for side in range(2):
        for y in range(ny):
            oedge[side, y] = packed(osend[y], side)
            vedge[side, y] = packed(vsend[y], side)

    pl.semaphore_wait(barrier, len(greeted))
    for copy in copies_of(osend, orecv, oedge, oedges, o_sem.at[0], o_sem.at[1]):
        copy.start()
    for copy in copies_of(vsend, vrecv, vedge, vedges, v_sem.at[0], v_sem.at[1]):
        copy.start()

    def columns(send, recv, edges):
        found = {}
        for xi, a in enumerate(xs):
            for py, (b, yl) in enumerate(py_of):
                if (a, b) == (0, 0):
                    mid = send[yl]
                else:
                    need, at = partners[a, b, 0]
                    mid = recv[at + need.index(yl)]
                ends_of = []
                for c in (-1, 1):
                    need, at = partners[a, b, c]
                    ends_of.append(unpacked(edges[at + need.index(yl)]))
                below, above = ends_of
                found[xi, py, 1] = mid
                low = jnp.where(tile_lane >= lanes - slots, below, mid)
                found[xi, py, 0] = pltpu.roll(low, slots, 1)
                high = jnp.where(tile_lane < slots, above, mid)
                found[xi, py, 2] = pltpu.roll(high, lanes - slots, 1)
        return found

    await_halo(orecv, oedges, o_sem.at[1])
    for (xi, py, dz), value in columns(osend, orecv, oedges).items():
        ostate[xi, py, dz] = value

    lane_id = lax.broadcasted_iota(jnp.int32, (slots, lanes), 1)
    slot_id = lax.broadcasted_iota(jnp.int32, (slots, lanes), 0)
    pick = (lane_id // slots) * slots + slot_id
    itself = lax.rem(lane_id, slots) == slot_id

    def nearby(py):
        for px, (a, xl) in enumerate(px_of):
            for dz in range(3):
                for c in range(3):
                    r = c * nx + xl
                    row = jnp.broadcast_to(ostate[xs.index(a), py, dz, r : r + 1], (slots, lanes))
                    near[px, py, dz, c] = jnp.take_along_axis(row, pick, axis=1, mode="promise_in_bounds")

    half = 0.5 * TIME_STEP
    reach2 = CUTOFF * CUTOFF

    def terms(squared):
        inv = lax.rsqrt(squared)
        inv2 = inv * inv
        inv6 = inv2 * inv2 * inv2
        inv12 = inv6 * inv6
        bond = inv12 - inv6
        return inv, bond, inv * (bond + inv12)

    _, _, edge = terms(jnp.full((slots, lanes), reach2, jnp.float32))
    pair_count = 27.0 * slots

    def step(k, _):
        p = lax.rem(k, 2)
        for py in range(ny + 2):
            nearby(py)

        energy_rows = jnp.zeros((1, lanes), jnp.float32)
        for x in range(nx):
            for y in range(ny):
                block = ostate[0, y + 1, 1]
                mine = [block[c * nx + x : c * nx + x + 1] for c in range(3)]
                occupied = mine[0] < 0.5 * FAR
                force = [jnp.zeros((slots, lanes), jnp.float32) for _ in range(3)]
                bonds, reach = (jnp.zeros((slots, lanes), jnp.float32) for _ in range(2))
                for shift in itertools.product((-1, 0, 1), repeat=3):
                    dx, dy, dz = shift
                    apart = [
                        near[x + 1 + dx, y + 1 + dy, dz + 1, c] - (mine[c] - shift[c] * CELL_SIDE)
                        for c in range(3)
                    ]
                    squared = apart[0] * apart[0] + apart[1] * apart[1] + apart[2] * apart[2]
                    if shift == (0, 0, 0):
                        squared = jnp.where(itself, reach2, squared)
                    squared = jnp.minimum(squared, reach2)
                    inv, bond, push = terms(squared)
                    pull = inv * (edge - push)
                    for c in range(3):
                        force[c] = force[c] + pull * apart[c]
                    bonds = bonds + bond
                    reach = reach + squared * inv
                for c in range(3):
                    total = 24.0 * jnp.sum(force[c], axis=0, keepdims=True)
                    fsend[p, y, c * nx + x : c * nx + x + 1] = jnp.where(occupied, total, 0.0)
                energy = 4.0 * bonds + FORCE_EDGE * reach
                total = jnp.sum(energy, axis=0, keepdims=True)
                total = total - pair_count * (ENERGY_EDGE + CUTOFF * FORCE_EDGE)
                energy_rows = energy_rows + jnp.where(occupied, total, 0.0)

        @pl.when(k > 0)
        def _():
            kinetic = jnp.zeros((tile, lanes), jnp.float32)
            for y in range(ny):
                v = vstate[0, y + 1, 1] + half * fsend[p, y]
                kinetic = kinetic + v * v
            kinetic = folded(jnp.sum(kinetic, axis=0, keepdims=True), 1)
            potential = folded(energy_rows, 2)
            row = jnp.where(
                row_lane < 2 * quarter, 0.5 * kinetic, jnp.where(row_lane < 3 * quarter, 0.5 * potential, tally[...])
            )
            row_sum[...] = row
            at = index_in(NEAR) * 2 + core
            for d in near_chips:
                if any(d.values()):
                    remote(row_sum, near_sums.at[p, at], near_send, near_recv.at[p], member(d, -1, 1)).start()

            @pl.when(follows)
            def _():
                remote(row_sum, near_sums.at[p, at], near_send, near_recv.at[p], member({}, 1, 1)).start()

            @pl.when(leads)
            def _():
                near_sums[p, at] = row

        @pl.when(k < STEPS)
        def _():
            for side in range(2):
                for y in range(ny):
                    fedge[p, side, y] = packed(fsend[p, y], side)
            for copy in copies_of(
                fsend.at[p], frecv.at[p], fedge.at[p], fedges.at[p], f_send_sem, f_recv_sem.at[p]
            ):
                copy.start()

        def total_of(ref, n):
            parts = [ref[p, i] for i in range(n)]
            while len(parts) > 1:
                parts = [sum(parts[i + 1 : i + 2], parts[i]) for i in range(0, len(parts), 2)]
            return parts[0]

        n_near, n_wide = len(near_chips), len(wide_chips)

        @pl.when((k > 0) & leads)
        def _():
            await_all(near_sums.at[p, pl.ds(0, 2 * n_near - 1)], near_recv.at[p])
            row = total_of(near_sums, 2 * n_near)
            chip_sum[...] = row
            at = index_in(WIDE)
            for d in wide_chips:
                for which in (0, 1):
                    if which == 0 or any(d.values()):
                        remote(
                            chip_sum, wide_sums.at[p, at], wide_send, wide_recv.at[p], member(d, -1, which)
                        ).start()
            wide_sums[p, at] = row

        @pl.when(k == 0)
        def _():
            await_halo(vrecv, vedges, v_sem.at[1])
            for (xi, py, dz), value in columns(vsend, vrecv, vedges).items():
                vstate[xi, py, dz] = value

        @pl.when(k < STEPS)
        def _():
            await_halo(frecv.at[p], fedges.at[p], f_recv_sem.at[p])
            await_halo(frecv.at[p], fedges.at[p], f_send_sem)
            before = jnp.where(k > 0, half, 0.0)
            for (xi, py, dz), f in columns(fsend.at[p], frecv.at[p], fedges.at[p]).items():
                vstate[xi, py, dz] = vstate[xi, py, dz] + before * f
                held[xi, py, dz] = half * f

        @pl.when(k > 0)
        def _():
            @pl.when(leads)
            def _():
                await_all(near_sums.at[p, pl.ds(0, n_near - 1)], near_send)
                await_all(wide_sums.at[p, pl.ds(0, n_wide - 1)], wide_recv.at[p])

            @pl.when(follows)
            def _():
                await_all(near_sums.at[p, pl.ds(0, n_near)], near_send)
                await_all(wide_sums.at[p], wide_recv.at[p])

            row = total_of(wide_sums, n_wide)

            def across(low, high):
                picked = jnp.where((row_lane >= low * quarter) & (row_lane < high * quarter), row, 0.0)
                return jnp.broadcast_to(jnp.sum(picked, axis=1, keepdims=True), (1, lanes))

            vigor, potential, count = across(0, 2), across(2, 3), across(3, 4)
            square = (1.0 - BATH_STRENGTH) + (BATH_STRENGTH * GOAL_WARMTH * 1.5) * count / vigor
            which = lax.broadcasted_iota(jnp.int32, (2, lanes), 1)
            record = jnp.concatenate([potential, square * vigor], axis=0) / slot_total
            history[...] = jnp.where(which == k - 1, record, history[...])
            scale[...] = jnp.sqrt(square)

            @pl.when(leads)
            def _():
                await_all(wide_out, wide_send)

        lam = scale[...]

        @pl.when(k < STEPS)
        def _():
            for xi in range(len(xs)):
                for py in range(ny + 2):
                    for dz in range(3):
                        v = vstate[xi, py, dz] * lam + held[xi, py, dz]
                        vstate[xi, py, dz] = v
                        ostate[xi, py, dz] = ostate[xi, py, dz] + TIME_STEP * v

        @pl.when(k == STEPS)
        def _():
            for y in range(ny):
                here = ostate[0, y + 1, 1]
                result[y] = jnp.where(here < 0.5 * FAR, here, kept[y])
                result[ny + y] = (vstate[0, y + 1, 1] + half * fsend[p, y]) * lam
                result[2 * ny + y] = fsend[p, y]
            result[3 * ny, 0:2] = history[...]

        return 0

    history[...] = jnp.zeros_like(history)
    scale[...] = jnp.ones_like(scale)
    lax.fori_loop(0, STEPS + 1, step, 0)
    await_halo(orecv, oedges, o_sem.at[0])
    await_halo(vrecv, vedges, v_sem.at[0])


def unpack(shape, result, o_out, v_out, f_out, h_out):
    nx, ny, nz, slots = shape
    lanes = nz * slots
    at = lax.broadcasted_iota(jnp.int32, (nz, lanes), 0) * slots + lax.rem(
        lax.broadcasted_iota(jnp.int32, (nz, lanes), 1), slots
    )
    for i, ref in enumerate((o_out, v_out, f_out)):
        for y in range(ny):
            for x in range(nx):
                for c in range(3):
                    r = c * nx + x
                    row = jnp.broadcast_to(result[i * ny + y, r : r + 1], (nz, lanes))
                    ref[x, y, c] = jnp.take_along_axis(row, at, axis=1, mode="promise_in_bounds")[:, :slots]
    h_out[...] = result[3 * ny, 0:2, :STEPS]


def shards(axes, offsets, velocities, occupied):
    nx, ny, nz, slots = occupied.shape
    lanes = nz * slots
    tile = lanes // slots
    assert axes[2] > 2 and tile >= 3 * nx
    _, flats, rows = partners_of(axes, ny)
    nxo = len(offsets_of(axes[0]))
    n_near, n_wide = (len(chips_of(axes, group)) for group in (NEAR, WIDE))
    f32 = jnp.float32
    plane = jax.ShapeDtypeStruct((nx, ny, 3, nz, slots), f32)
    vmem = pl.BlockSpec(memory_space=pltpu.VMEM)
    dma = pltpu.SemaphoreType.DMA
    state = pltpu.VMEM((nxo, ny + 2, 3, tile, lanes), f32)
    halo = [
        pltpu.VMEM((ny, tile, lanes), f32),
        pltpu.VMEM((flats, tile, lanes), f32),
        pltpu.VMEM((2, ny, 1, lanes), f32),
        pltpu.VMEM((rows, 1, lanes), f32),
    ]
    result = pl.pallas_call(
        functools.partial(kernel, axes, (nx, ny, nz, slots)),
        name="verlet",
        out_shape=pltpu.VMEM((3 * ny + 1, tile, lanes), f32),
        in_specs=[pl.BlockSpec(memory_space=pltpu.HBM)] * 3,
        out_specs=vmem,
        scratch_shapes=[
            pltpu.VMEM((2, nx, ny, 3, nz, slots), f32),
            pltpu.VMEM((ny, tile, lanes), f32),
            state,
            state,
            state,
            pltpu.VMEM((nx + 2, ny + 2, 3, 3, slots, lanes), f32),
            *halo,
            *halo,
            pltpu.VMEM((nx, ny, nz, slots), jnp.int32),
            pltpu.VMEM((2, ny, tile, lanes), f32),
            pltpu.VMEM((2, flats, tile, lanes), f32),
            pltpu.VMEM((2, 2, ny, 1, lanes), f32),
            pltpu.VMEM((2, rows, 1, lanes), f32),
            pltpu.VMEM((1, lanes), f32),
            pltpu.VMEM((2, lanes), f32),
            pltpu.VMEM((1, lanes), f32),
            pltpu.VMEM((1, lanes), f32),
            pltpu.VMEM((2, 2 * n_near, 1, lanes), f32),
            pltpu.VMEM((1, lanes), f32),
            pltpu.VMEM((2, n_wide, 1, lanes), f32),
            pltpu.VMEM((2 * n_wide - 1, 1, lanes), f32),
            dma((3,)),
            dma((2, 2)),
            dma((2, 2)),
            dma((2,)),
            dma((2, 2)),
            dma,
            dma((2,)),
            dma,
            dma((2,)),
        ],
        compiler_params=pltpu.CompilerParams(
            collective_id=0, has_side_effects=True, vmem_limit_bytes=VERLET_VMEM
        ),
    )(
        jnp.transpose(offsets, (0, 1, 4, 2, 3)),
        jnp.transpose(velocities, (0, 1, 4, 2, 3)),
        occupied,
    )
    o, v, f, h = pl.pallas_call(
        functools.partial(unpack, (nx, ny, nz, slots)),
        name="unpack",
        out_shape=[plane, plane, plane, jax.ShapeDtypeStruct((2, STEPS), f32)],
        in_specs=[vmem],
        out_specs=[vmem] * 4,
        compiler_params=pltpu.CompilerParams(vmem_limit_bytes=UNPACK_VMEM),
    )(result)
    back = (0, 1, 3, 4, 2)
    return (jnp.transpose(o, back), jnp.transpose(v, back), jnp.transpose(f, back), h.T)


def solution(mesh):
    axes = tuple(mesh.shape[a] for a in ("gx", "gy", "gz"))
    in_specs = (
        P("gx", "gy", "gz", None, None),
        P("gx", "gy", "gz", None, None),
        P("gx", "gy", "gz", None),
    )
    out_specs = (
        P("gx", "gy", "gz", None, None),
        P("gx", "gy", "gz", None, None),
        P("gx", "gy", "gz", None, None),
        P(),
    )
    return jax.shard_map(
        functools.partial(shards, axes), mesh=mesh, in_specs=in_specs, out_specs=out_specs, check_vma=False
    )
```

```python
import functools
import itertools

import jax
import jax.numpy as jnp
from jax import lax
from jax.experimental import pallas as pl
from jax.experimental.pallas import tpu as pltpu
from jax.sharding import PartitionSpec as P

MESH = pl.DeviceIdType.MESH
STEPS = 4
CUTOFF = 2.5
CELL_SIDE = 2.6
TIME_STEP = 0.005
BATH_STRENGTH = 0.25
GOAL_WARMTH = 0.8
FORCE_EDGE = 24.0 * (2.0 * CUTOFF ** (-13) - CUTOFF ** (-7))
ENERGY_EDGE = 4.0 * (CUTOFF ** (-12) - CUTOFF ** (-6))
FAR = 32.0
VERLET_VMEM = 60 * 1024 * 1024
UNPACK_VMEM = 4 * 1024 * 1024


NEAR = ("z",)
WIDE = ("xl", "xh", "y")


def parts_of(axes):
    gx, gy, gz = axes
    return {"xl": gx // 4, "y": 4, "xh": gy // 2, "z": gz}


def chips_of(axes, group):
    sizes = parts_of(axes)

    def hops(d):
        return sum(min(o, sizes[a] - o) for a, o in d.items())

    every = itertools.product(*[range(sizes[a]) for a in group])
    return sorted((dict(zip(group, d)) for d in every), key=lambda d: -hops(d))


def offsets_of(size):
    return [0] if size == 1 else [0, 1] if size == 2 else [0, 1, -1]


def canonical(size, off):
    return 0 if size == 1 else off % 2 if size == 2 else off


def padded(size, n):
    return [(canonical(size, -1), n - 1)] + [(0, i) for i in range(n)] + [(canonical(size, 1), 0)]


def deep(size, n):
    low, high = canonical(size, -1), canonical(size, 1)
    return [(low, n - 2), (low, n - 1)] + [(0, i) for i in range(n)] + [(high, 0), (high, 1)]


def deep_places(axes, ny):
    flat, rows, found = 0, 0, {}
    for d in itertools.product(*[offsets_of(n) for n in axes]):
        if d == (0, 0, 0):
            continue
        if d[2] == 0:
            found[d] = flat
            flat += ny
        else:
            found[d] = rows
            rows += 2 * ny
    return found, flat, rows


def partners_of(axes, ny):
    every = itertools.product(*[offsets_of(n) for n in axes])
    flat, rows, found = 0, 0, {}
    for d in every:
        if d == (0, 0, 0):
            continue
        need = sorted({yl for off, yl in padded(axes[1], ny) if off == d[1]})
        if d[2] == 0:
            found[d] = need, flat
            flat += len(need)
        else:
            found[d] = need, rows
            rows += len(need)
    return found, flat, rows


def kernel(
    axes, shape, o_in, v_in, occ_in, result,
    planes_in, kept, ostate, vstate, held, near, around, first_near, first_force, osend, orecv, oedge, oedges, vsend, vrecv, vedge, vedges,
    occ_planes, fsend, frecv, fedge, fedges, tally, history, row_sum, near_sums, chip_sum, wide_sums, wide_out,
    in_sem, o_sem, v_sem, f_send_sem, f_recv_sem, near_send, near_recv, wide_send, wide_recv,
):
    gx, gy, gz = axes
    nx, ny, nz, slots = shape
    lanes = nz * slots
    tile = fsend.shape[2]
    slot_total = float(gx * gy * gz * nx * ny * lanes)
    me = [lax.axis_index(a) for a in ("gx", "gy", "gz")]
    sizes = parts_of(axes)
    place = {"xl": me[0] // 4, "y": lax.rem(me[0], 4), "xh": me[1] // 2, "z": me[2]}
    core = lax.rem(me[1], 2)
    leads = core == 1
    follows = core == 0
    near_chips, wide_chips = chips_of(axes, NEAR), chips_of(axes, WIDE)

    turned = [[lax.rem(me[i] + j, n) for j in range(n)] for i, n in enumerate(axes)]

    def device(d):
        return tuple(turned[i][d[i] % axes[i]] for i in range(3))

    def member(d, sign, which):
        at = dict(place)
        for a, o in d.items():
            if o:
                at[a] = lax.rem(at[a] + (o if sign > 0 else sizes[a] - o), sizes[a])
        return (at["xl"] * 4 + at["y"], at["xh"] * 2 + which, at["z"])

    def index_in(group):
        at = 0
        for a in group:
            at = at * sizes[a] + place[a]
        return at

    px_of, py_of = padded(gx, nx), padded(gy, ny)
    xs = offsets_of(gx)
    partners, flats, rows = partners_of(axes, ny)

    def remote(src, dst, send_sem, recv_sem, to):
        return pltpu.make_async_remote_copy(
            src_ref=src, dst_ref=dst, send_sem=send_sem, recv_sem=recv_sem, device_id=to, device_id_type=MESH
        )

    def copies_of(send, recv, edge, edges, send_sem, recv_sem):
        copies = []
        for d, (need, at) in reversed([*partners.items()]):
            where = pl.ds(need[0], len(need))
            to = device(tuple(-x for x in d))
            if d[2] == 0:
                copies.append(remote(send.at[where], recv.at[pl.ds(at, len(need))], send_sem.at[0], recv_sem.at[0], to))
            else:
                src = edge.at[0 if d[2] == 1 else 1, where]
                copies.append(remote(src, edges.at[pl.ds(at, len(need))], send_sem.at[1], recv_sem.at[1], to))
        return copies

    def await_all(ref, sem):
        pltpu.make_async_copy(ref, ref, sem).wait()

    def await_halo(recv, edges, sem):
        await_all(recv, sem.at[0])
        await_all(edges, sem.at[1])

    barrier = pltpu.get_barrier_semaphore()

    greeted = [device(d) for d in partners]
    greeted += [member(d, 1, which) for group in (near_chips, wide_chips) for d in group if any(d.values()) for which in (0, 1)]
    greeted.append(member({}, 1, 1 - core))
    for to in greeted:
        pl.semaphore_signal(barrier, inc=1, device_id=to, device_id_type=MESH)

    loads = [
        pltpu.make_async_copy(o_in, planes_in.at[0], in_sem.at[0]),
        pltpu.make_async_copy(occ_in, occ_planes, in_sem.at[1]),
        pltpu.make_async_copy(v_in, planes_in.at[1], in_sem.at[2]),
    ]
    for load in loads:
        load.start()

    lane = lax.broadcasted_iota(jnp.int32, (nz, lanes), 1)
    level = lax.broadcasted_iota(jnp.int32, (nz, lanes), 0)
    spread = (
        lax.rem(lax.broadcasted_iota(jnp.int32, (slots, lanes), 1), slots)
        == lax.broadcasted_iota(jnp.int32, (slots, lanes), 0)
    ).astype(jnp.float32)

    def rows_of(planes):
        flat = planes.reshape(-1, slots)
        wide = jnp.dot(flat, spread, precision=lax.Precision.HIGHEST, preferred_element_type=jnp.float32)
        wide = wide.reshape(-1, nz, lanes)
        return jnp.sum(jnp.where((lane // slots == level)[None], wide, 0.0), axis=1)

    for load in loads:
        load.wait()
    o_rows = rows_of(planes_in[0])
    v_rows = rows_of(planes_in[1])
    w_rows = rows_of(occ_planes[...].astype(jnp.float32))
    osend[...] = jnp.zeros_like(osend)
    kept[...] = jnp.zeros_like(kept)
    vsend[...] = jnp.zeros_like(vsend)
    fsend[...] = jnp.zeros_like(fsend)
    for x in range(nx):
        for y in range(ny):
            w = w_rows[x * ny + y : x * ny + y + 1]
            for c in range(3):
                i = (x * ny + y) * 3 + c
                r = c * nx + x
                kept[y, r : r + 1] = o_rows[i : i + 1]
                osend[y, r : r + 1] = jnp.where(w > 0.5, o_rows[i : i + 1], FAR)
                vsend[y, r : r + 1] = v_rows[i : i + 1] * w

    quarter = lanes // 4
    row_lane = lane[:1]

    def folded(row, times):
        for i in range(times):
            row = row + pltpu.roll(row, lanes >> (i + 1), 1)
        return row

    tally[...] = folded(jnp.sum(w_rows, axis=0, keepdims=True), 2)

    tile_lane = lax.broadcasted_iota(jnp.int32, (tile, lanes), 1)
    tile_row = lax.broadcasted_iota(jnp.int32, (tile, lanes), 0)
    slot_lane = lax.rem(tile_lane, slots)
    ends = [[slot_lane + (i if side == 0 else nz - 1 - i) * slots for i in range(2)] for side in range(2)]
    back = tile_row * slots + lax.rem(tile_lane, slots)

    def packed(block, side, depth=0):
        taken = jnp.take_along_axis(block, ends[side][depth], axis=1, mode="promise_in_bounds")
        return jnp.sum(jnp.where(tile_lane // slots == tile_row, taken, 0.0), axis=0, keepdims=True)

    def unpacked(row):
        wide = jnp.broadcast_to(row, (tile, lanes))
        return jnp.take_along_axis(wide, back, axis=1, mode="promise_in_bounds")

    for side in range(2):
        for y in range(ny):
            for depth in range(2):
                oedge[side, 2 * y + depth] = packed(osend[y], side, depth)
            vedge[side, y] = packed(vsend[y], side)

    pl.semaphore_wait(barrier, len(greeted))
    places, _, _ = deep_places(axes, ny)
    for d, at in reversed([*places.items()]):
        to = device(tuple(-x for x in d))
        if d[2] == 0:
            remote(osend, orecv.at[pl.ds(at, ny)], o_sem.at[0, 0], o_sem.at[1, 0], to).start()
        else:
            src = oedge.at[0 if d[2] == 1 else 1]
            remote(src, oedges.at[pl.ds(at, 2 * ny)], o_sem.at[0, 1], o_sem.at[1, 1], to).start()
    for copy in copies_of(vsend, vrecv, vedge, vedges, v_sem.at[0], v_sem.at[1]):
        copy.start()

    def columns(send, recv, edges):
        found = {}
        for xi, a in enumerate(xs):
            for py, (b, yl) in enumerate(py_of):
                if (a, b) == (0, 0):
                    mid = send[yl]
                else:
                    need, at = partners[a, b, 0]
                    mid = recv[at + need.index(yl)]
                ends_of = []
                for c in (-1, 1):
                    need, at = partners[a, b, c]
                    ends_of.append(unpacked(edges[at + need.index(yl)]))
                below, above = ends_of
                found[xi, py, 1] = mid
                low = jnp.where(tile_lane >= lanes - slots, below, mid)
                found[xi, py, 0] = pltpu.roll(low, slots, 1)
                high = jnp.where(tile_lane < slots, above, mid)
                found[xi, py, 2] = pltpu.roll(high, lanes - slots, 1)
        return found

    cell = tile_lane // slots
    deep_x, deep_y = deep(gx, nx), deep(gy, ny)
    pairs = ny + 2

    def neighbourhood():
        ends_of = {}
        for xi, a in enumerate(xs):
            for at, (b, yl) in enumerate(deep_y):
                mid = osend[yl] if (a, b) == (0, 0) else orecv[places[a, b, 0] + yl]
                below, above = (
                    [unpacked(oedges[places[a, b, c] + 2 * yl + depth]) for depth in range(2)] for c in (-1, 1)
                )
                low = jnp.where(tile_lane >= lanes - slots, below[0], mid)
                high = jnp.where(tile_lane < slots, above[0], mid)
                around[xi, at, 0] = pltpu.roll(low, slots, 1)
                around[xi, at, 1] = mid
                around[xi, at, 2] = pltpu.roll(high, lanes - slots, 1)
                bottom = jnp.where(cell == 0, below[1], jnp.where(cell == 1, below[0], pltpu.roll(mid, 2 * slots, 1)))
                top = jnp.where(cell == nz - 1, above[1], above[0])
                top = jnp.where(cell == nz - 3, pltpu.roll(mid, lanes - 2 * slots, 1), top)
                ends_of[xi, at] = jnp.where(cell < nz // 2, bottom, top)
        for xi in range(len(xs)):
            for dy in range(3):
                for dz in range(3):
                    centre = jnp.where(lax.rem(cell, 2) == 0, dz, nz - 3 + dz)
                    source = centre * slots + slot_lane
                    gathered = jnp.zeros((tile, lanes), jnp.float32)
                    for t in range(pairs):
                        taken = jnp.take_along_axis(ends_of[xi, t + dy], source, axis=1, mode="promise_in_bounds")
                        gathered = jnp.where(cell // 2 == t, taken, gathered)
                    around[xi, pairs + 2 + dy, dz] = gathered

    await_halo(orecv, oedges, o_sem.at[1])
    neighbourhood()
    for xi in range(len(xs)):
        for py in range(ny + 2):
            for dz in range(3):
                ostate[xi, py, dz] = around[xi, py + 1, dz]

    lane_id = lax.broadcasted_iota(jnp.int32, (slots, lanes), 1)
    slot_id = lax.broadcasted_iota(jnp.int32, (slots, lanes), 0)
    pick = (lane_id // slots) * slots + slot_id
    itself = lax.rem(lane_id, slots) == slot_id

    def nearby(py):
        for px, (a, xl) in enumerate(px_of):
            for dz in range(3):
                for c in range(3):
                    r = c * nx + xl
                    row = jnp.broadcast_to(ostate[xs.index(a), py, dz, r : r + 1], (slots, lanes))
                    near[px, py, dz, c] = jnp.take_along_axis(row, pick, axis=1, mode="promise_in_bounds")

    half = 0.5 * TIME_STEP
    reach2 = CUTOFF * CUTOFF

    def terms(squared):
        inv = lax.rsqrt(squared)
        inv2 = inv * inv
        inv6 = inv2 * inv2 * inv2
        inv12 = inv6 * inv6
        bond = inv12 - inv6
        return inv, bond, inv * (bond + inv12)

    _, _, edge = terms(jnp.full((slots, lanes), reach2, jnp.float32))
    pair_count = 27.0 * slots

    def pair_sums(mine, near_of):
        force = [jnp.zeros((slots, lanes), jnp.float32) for _ in range(3)]
        bonds, reach = (jnp.zeros((slots, lanes), jnp.float32) for _ in range(2))
        for shift in itertools.product((-1, 0, 1), repeat=3):
            apart = [near_of(shift, c) - (mine[c] - shift[c] * CELL_SIDE) for c in range(3)]
            squared = apart[0] * apart[0] + apart[1] * apart[1] + apart[2] * apart[2]
            if shift == (0, 0, 0):
                squared = jnp.where(itself, reach2, squared)
            squared = jnp.minimum(squared, reach2)
            inv, bond, push = terms(squared)
            pull = inv * (edge - push)
            for c in range(3):
                force[c] = force[c] + pull * apart[c]
            bonds = bonds + bond
            reach = reach + squared * inv
        return [24.0 * jnp.sum(f, axis=0, keepdims=True) for f in force], bonds, reach

    def first_row(i, _):
        centre = i + 1 + 2 * (i // pairs)
        for px, (a, xl) in enumerate(deep_x):
            for dy in range(3):
                for dz in range(3):
                    for c in range(3):
                        r = c * nx + xl
                        row = jnp.broadcast_to(around[xs.index(a), centre - 1 + dy, dz, r : r + 1], (slots, lanes))
                        first_near[px, dy, dz, c] = jnp.take_along_axis(row, pick, axis=1, mode="promise_in_bounds")
        for px, (a, xl) in enumerate(px_of):
            block = around[xs.index(a), centre, 1]
            mine = [block[c * nx + xl : c * nx + xl + 1] for c in range(3)]
            force, _, _ = pair_sums(
                mine, lambda shift, c: first_near[px + 1 + shift[0], 1 + shift[1], 1 + shift[2], c]
            )
            for c in range(3):
                r = c * nx + xl
                first_force[xs.index(a), i, r : r + 1] = jnp.where(mine[0] < 0.5 * FAR, force[c], 0.0)
        return 0

    first_force[...] = jnp.zeros_like(first_force)
    lax.fori_loop(0, pairs + 1, first_row, 0)

    await_halo(vrecv, vedges, v_sem.at[1])
    first_v = columns(vsend, vrecv, vedges)
    for xi in range(len(xs)):
        outer = first_force[xi, pairs]
        for py in range(pairs):
            mid = first_force[xi, py]
            low = jnp.where(tile_lane < slots, pltpu.roll(outer, (lanes - 2 * py * slots) % lanes, 1), pltpu.roll(mid, slots, 1))
            high = jnp.where(
                tile_lane >= lanes - slots,
                pltpu.roll(outer, lanes - 2 * (py + 1) * slots, 1),
                pltpu.roll(mid, lanes - slots, 1),
            )
            for dz, f in enumerate((low, mid, high)):
                v = first_v[xi, py, dz] + half * f
                vstate[xi, py, dz] = v
                ostate[xi, py, dz] = ostate[xi, py, dz] + TIME_STEP * v

    def step(k, _):
        p = lax.rem(k, 2)
        for py in range(ny + 2):
            nearby(py)

        energy_rows = jnp.zeros((1, lanes), jnp.float32)
        for x in range(nx):
            for y in range(ny):
                block = ostate[0, y + 1, 1]
                mine = [block[c * nx + x : c * nx + x + 1] for c in range(3)]
                occupied = mine[0] < 0.5 * FAR
                force, bonds, reach = pair_sums(
                    mine, lambda shift, c: near[x + 1 + shift[0], y + 1 + shift[1], 1 + shift[2], c]
                )
                for c in range(3):
                    r = c * nx + x
                    fsend[p, y, r : r + 1] = jnp.where(occupied, force[c], 0.0)
                energy = 4.0 * bonds + FORCE_EDGE * reach
                total = jnp.sum(energy, axis=0, keepdims=True)
                total = total - pair_count * (ENERGY_EDGE + CUTOFF * FORCE_EDGE)
                energy_rows = energy_rows + jnp.where(occupied, total, 0.0)

        kinetic = jnp.zeros((tile, lanes), jnp.float32)
        for y in range(ny):
            v = vstate[0, y + 1, 1] + half * fsend[p, y]
            kinetic = kinetic + v * v
        kinetic = folded(jnp.sum(kinetic, axis=0, keepdims=True), 1)
        potential = folded(energy_rows, 2)
        row = jnp.where(
            row_lane < 2 * quarter, 0.5 * kinetic, jnp.where(row_lane < 3 * quarter, 0.5 * potential, tally[...])
        )
        row_sum[...] = row
        at = index_in(NEAR) * 2 + core
        for d in near_chips:
            if any(d.values()):
                remote(row_sum, near_sums.at[p, at], near_send, near_recv.at[p], member(d, -1, 1)).start()

        @pl.when(follows)
        def _():
            remote(row_sum, near_sums.at[p, at], near_send, near_recv.at[p], member({}, 1, 1)).start()

        @pl.when(leads)
        def _():
            near_sums[p, at] = row

        @pl.when(k < STEPS)
        def _():
            for side in range(2):
                for y in range(ny):
                    fedge[p, side, y] = packed(fsend[p, y], side)
            for copy in copies_of(
                fsend.at[p], frecv.at[p], fedge.at[p], fedges.at[p], f_send_sem, f_recv_sem.at[p]
            ):
                copy.start()

        def total_of(ref, n):
            parts = [ref[p, i] for i in range(n)]
            while len(parts) > 1:
                parts = [sum(parts[i + 1 : i + 2], parts[i]) for i in range(0, len(parts), 2)]
            return parts[0]

        n_near, n_wide = len(near_chips), len(wide_chips)

        @pl.when(leads)
        def _():
            await_all(near_sums.at[p, pl.ds(0, 2 * n_near - 1)], near_recv.at[p])
            row = total_of(near_sums, 2 * n_near)
            chip_sum[...] = row
            at = index_in(WIDE)
            for d in wide_chips:
                for which in (0, 1):
                    if which == 0 or any(d.values()):
                        remote(
                            chip_sum, wide_sums.at[p, at], wide_send, wide_recv.at[p], member(d, -1, which)
                        ).start()
            wide_sums[p, at] = row

        @pl.when(k < STEPS)
        def _():
            await_halo(frecv.at[p], fedges.at[p], f_recv_sem.at[p])
            await_halo(frecv.at[p], fedges.at[p], f_send_sem)
            for (xi, py, dz), f in columns(fsend.at[p], frecv.at[p], fedges.at[p]).items():
                vstate[xi, py, dz] = vstate[xi, py, dz] + half * f
                held[xi, py, dz] = half * f

        @pl.when(leads)
        def _():
            await_all(near_sums.at[p, pl.ds(0, n_near - 1)], near_send)
            await_all(wide_sums.at[p, pl.ds(0, n_wide - 1)], wide_recv.at[p])

        @pl.when(follows)
        def _():
            await_all(near_sums.at[p, pl.ds(0, n_near)], near_send)
            await_all(wide_sums.at[p], wide_recv.at[p])

        row = total_of(wide_sums, n_wide)

        def across(low, high):
            picked = jnp.where((row_lane >= low * quarter) & (row_lane < high * quarter), row, 0.0)
            return jnp.broadcast_to(jnp.sum(picked, axis=1, keepdims=True), (1, lanes))

        vigor, potential, count = across(0, 2), across(2, 3), across(3, 4)
        square = (1.0 - BATH_STRENGTH) + (BATH_STRENGTH * GOAL_WARMTH * 1.5) * count / vigor
        which = lax.broadcasted_iota(jnp.int32, (2, lanes), 1)
        record = jnp.concatenate([potential, square * vigor], axis=0) / slot_total
        history[...] = jnp.where(which == k - 1, record, history[...])

        @pl.when(leads)
        def _():
            await_all(wide_out, wide_send)

        lam = jnp.sqrt(square)

        @pl.when(k < STEPS)
        def _():
            for xi in range(len(xs)):
                for py in range(ny + 2):
                    for dz in range(3):
                        v = vstate[xi, py, dz] * lam + held[xi, py, dz]
                        vstate[xi, py, dz] = v
                        ostate[xi, py, dz] = ostate[xi, py, dz] + TIME_STEP * v

        @pl.when(k == STEPS)
        def _():
            for y in range(ny):
                here = ostate[0, y + 1, 1]
                result[y] = jnp.where(here < 0.5 * FAR, here, kept[y])
                result[ny + y] = (vstate[0, y + 1, 1] + half * fsend[p, y]) * lam
                result[2 * ny + y] = fsend[p, y]
            result[3 * ny, 0:2] = history[...]

        return 0

    history[...] = jnp.zeros_like(history)
    lax.fori_loop(1, STEPS + 1, step, 0)
    await_halo(orecv, oedges, o_sem.at[0])
    await_halo(vrecv, vedges, v_sem.at[0])


def unpack(shape, result, o_out, v_out, f_out, h_out):
    nx, ny, nz, slots = shape
    lanes = nz * slots
    at = lax.broadcasted_iota(jnp.int32, (nz, lanes), 0) * slots + lax.rem(
        lax.broadcasted_iota(jnp.int32, (nz, lanes), 1), slots
    )
    for i, ref in enumerate((o_out, v_out, f_out)):
        for y in range(ny):
            for x in range(nx):
                for c in range(3):
                    r = c * nx + x
                    row = jnp.broadcast_to(result[i * ny + y, r : r + 1], (nz, lanes))
                    ref[x, y, c] = jnp.take_along_axis(row, at, axis=1, mode="promise_in_bounds")[:, :slots]
    h_out[...] = result[3 * ny, 0:2, :STEPS]


def shards(axes, offsets, velocities, occupied):
    nx, ny, nz, slots = occupied.shape
    lanes = nz * slots
    tile = lanes // slots
    assert axes[2] > 2 and tile >= 3 * nx and min(nx, ny) >= 2 and nz == 2 * (ny + 2)
    _, flats, rows = partners_of(axes, ny)
    _, deep_flats, deep_rows = deep_places(axes, ny)
    nxo = len(offsets_of(axes[0]))
    n_near, n_wide = (len(chips_of(axes, group)) for group in (NEAR, WIDE))
    f32 = jnp.float32
    plane = jax.ShapeDtypeStruct((nx, ny, 3, nz, slots), f32)
    vmem = pl.BlockSpec(memory_space=pltpu.VMEM)
    dma = pltpu.SemaphoreType.DMA
    state = pltpu.VMEM((nxo, ny + 2, 3, tile, lanes), f32)
    halo = [
        pltpu.VMEM((ny, tile, lanes), f32),
        pltpu.VMEM((flats, tile, lanes), f32),
        pltpu.VMEM((2, ny, 1, lanes), f32),
        pltpu.VMEM((rows, 1, lanes), f32),
    ]
    result = pl.pallas_call(
        functools.partial(kernel, axes, (nx, ny, nz, slots)),
        name="verlet",
        out_shape=pltpu.VMEM((3 * ny + 1, tile, lanes), f32),
        in_specs=[pl.BlockSpec(memory_space=pltpu.HBM)] * 3,
        out_specs=vmem,
        scratch_shapes=[
            pltpu.VMEM((2, nx, ny, 3, nz, slots), f32),
            pltpu.VMEM((ny, tile, lanes), f32),
            state,
            state,
            state,
            pltpu.VMEM((nx + 2, ny + 2, 3, 3, slots, lanes), f32),
            pltpu.VMEM((nxo, ny + 7, 3, tile, lanes), f32),
            pltpu.VMEM((nx + 4, 3, 3, 3, slots, lanes), f32),
            pltpu.VMEM((nxo, ny + 3, tile, lanes), f32),
            pltpu.VMEM((ny, tile, lanes), f32),
            pltpu.VMEM((deep_flats, tile, lanes), f32),
            pltpu.VMEM((2, 2 * ny, 1, lanes), f32),
            pltpu.VMEM((deep_rows, 1, lanes), f32),
            *halo,
            pltpu.VMEM((nx, ny, nz, slots), jnp.int32),
            pltpu.VMEM((2, ny, tile, lanes), f32),
            pltpu.VMEM((2, flats, tile, lanes), f32),
            pltpu.VMEM((2, 2, ny, 1, lanes), f32),
            pltpu.VMEM((2, rows, 1, lanes), f32),
            pltpu.VMEM((1, lanes), f32),
            pltpu.VMEM((2, lanes), f32),
            pltpu.VMEM((1, lanes), f32),
            pltpu.VMEM((2, 2 * n_near, 1, lanes), f32),
            pltpu.VMEM((1, lanes), f32),
            pltpu.VMEM((2, n_wide, 1, lanes), f32),
            pltpu.VMEM((2 * n_wide - 1, 1, lanes), f32),
            dma((3,)),
            dma((2, 2)),
            dma((2, 2)),
            dma((2,)),
            dma((2, 2)),
            dma,
            dma((2,)),
            dma,
            dma((2,)),
        ],
        compiler_params=pltpu.CompilerParams(
            collective_id=0, has_side_effects=True, vmem_limit_bytes=VERLET_VMEM
        ),
    )(
        jnp.transpose(offsets, (0, 1, 4, 2, 3)),
        jnp.transpose(velocities, (0, 1, 4, 2, 3)),
        occupied,
    )
    o, v, f, h = pl.pallas_call(
        functools.partial(unpack, (nx, ny, nz, slots)),
        name="unpack",
        out_shape=[plane, plane, plane, jax.ShapeDtypeStruct((2, STEPS), f32)],
        in_specs=[vmem],
        out_specs=[vmem] * 4,
        compiler_params=pltpu.CompilerParams(vmem_limit_bytes=UNPACK_VMEM),
    )(result)
    back = (0, 1, 3, 4, 2)
    return (jnp.transpose(o, back), jnp.transpose(v, back), jnp.transpose(f, back), h.T)


def solution(mesh):
    axes = tuple(mesh.shape[a] for a in ("gx", "gy", "gz"))
    in_specs = (
        P("gx", "gy", "gz", None, None),
        P("gx", "gy", "gz", None, None),
        P("gx", "gy", "gz", None),
    )
    out_specs = (
        P("gx", "gy", "gz", None, None),
        P("gx", "gy", "gz", None, None),
        P("gx", "gy", "gz", None, None),
        P(),
    )
    return jax.shard_map(
        functools.partial(shards, axes), mesh=mesh, in_specs=in_specs, out_specs=out_specs, check_vma=False
    )
```

```python
import functools
import itertools

import jax
import jax.numpy as jnp
from jax import lax
from jax.experimental import pallas as pl
from jax.experimental.pallas import tpu as pltpu
from jax.sharding import PartitionSpec as P

MESH = pl.DeviceIdType.MESH
STEPS = 4
CUTOFF = 2.5
CELL_SIDE = 2.6
TIME_STEP = 0.005
BATH_STRENGTH = 0.25
GOAL_WARMTH = 0.8
FORCE_EDGE = 24.0 * (2.0 * CUTOFF ** (-13) - CUTOFF ** (-7))
ENERGY_EDGE = 4.0 * (CUTOFF ** (-12) - CUTOFF ** (-6))
FAR = 32.0
VERLET_VMEM = 60 * 1024 * 1024
UNPACK_VMEM = 4 * 1024 * 1024


NEAR = ("z",)
WIDE = ("xl", "xh", "y")


def parts_of(axes):
    gx, gy, gz = axes
    return {"xl": gx // 4, "y": 4, "xh": gy // 2, "z": gz}


def chips_of(axes, group):
    sizes = parts_of(axes)

    def hops(d):
        return sum(min(o, sizes[a] - o) for a, o in d.items())

    every = itertools.product(*[range(sizes[a]) for a in group])
    return sorted((dict(zip(group, d)) for d in every), key=lambda d: -hops(d))


def offsets_of(size):
    return [0] if size == 1 else [0, 1] if size == 2 else [0, 1, -1]


def canonical(size, off):
    return 0 if size == 1 else off % 2 if size == 2 else off


def padded(size, n):
    return [(canonical(size, -1), n - 1)] + [(0, i) for i in range(n)] + [(canonical(size, 1), 0)]


def deep(size, n):
    low, high = canonical(size, -1), canonical(size, 1)
    return [(low, n - 2), (low, n - 1)] + [(0, i) for i in range(n)] + [(high, 0), (high, 1)]


def deep_places(axes, ny):
    flat, rows, found = 0, 0, {}
    for d in itertools.product(*[offsets_of(n) for n in axes]):
        if d == (0, 0, 0):
            continue
        if d[2] == 0:
            found[d] = flat
            flat += ny
        else:
            found[d] = rows
            rows += 2 * ny
    return found, flat, rows


def partners_of(axes, ny):
    every = itertools.product(*[offsets_of(n) for n in axes])
    flat, rows, found = 0, 0, {}
    for d in every:
        if d == (0, 0, 0):
            continue
        need = sorted({yl for off, yl in padded(axes[1], ny) if off == d[1]})
        if d[2] == 0:
            found[d] = need, flat
            flat += len(need)
        else:
            found[d] = need, rows
            rows += len(need)
    return found, flat, rows


def kernel(
    axes, shape, o_in, v_in, occ_in, result,
    planes_in, kept, ostate, vstate, held, near, around, ends_of, first_near, first_force, osend, orecv, oedge, oedges, vsend, vrecv, vedge, vedges,
    occ_planes, fsend, frecv, fedge, fedges, tally, history, row_sum, near_sums, chip_sum, wide_sums, wide_out,
    in_sem, o_sem, o_recv_sem, v_sem, f_send_sem, f_recv_sem, near_send, near_recv, wide_send, wide_recv,
):
    gx, gy, gz = axes
    nx, ny, nz, slots = shape
    lanes = nz * slots
    tile = fsend.shape[2]
    slot_total = float(gx * gy * gz * nx * ny * lanes)
    me = [lax.axis_index(a) for a in ("gx", "gy", "gz")]
    sizes = parts_of(axes)
    place = {"xl": me[0] // 4, "y": lax.rem(me[0], 4), "xh": me[1] // 2, "z": me[2]}
    core = lax.rem(me[1], 2)
    leads = core == 1
    follows = core == 0
    near_chips, wide_chips = chips_of(axes, NEAR), chips_of(axes, WIDE)

    turned = [[lax.rem(me[i] + j, n) for j in range(n)] for i, n in enumerate(axes)]

    def device(d):
        return tuple(turned[i][d[i] % axes[i]] for i in range(3))

    def member(d, sign, which):
        at = dict(place)
        for a, o in d.items():
            if o:
                at[a] = lax.rem(at[a] + (o if sign > 0 else sizes[a] - o), sizes[a])
        return (at["xl"] * 4 + at["y"], at["xh"] * 2 + which, at["z"])

    def index_in(group):
        at = 0
        for a in group:
            at = at * sizes[a] + place[a]
        return at

    px_of, py_of = padded(gx, nx), padded(gy, ny)
    xs = offsets_of(gx)
    partners, flats, rows = partners_of(axes, ny)

    def remote(src, dst, send_sem, recv_sem, to):
        return pltpu.make_async_remote_copy(
            src_ref=src, dst_ref=dst, send_sem=send_sem, recv_sem=recv_sem, device_id=to, device_id_type=MESH
        )

    def copies_of(send, recv, edge, edges, send_sem, recv_sem):
        copies = []
        for d, (need, at) in reversed([*partners.items()]):
            where = pl.ds(need[0], len(need))
            to = device(tuple(-x for x in d))
            if d[2] == 0:
                copies.append(remote(send.at[where], recv.at[pl.ds(at, len(need))], send_sem.at[0], recv_sem.at[0], to))
            else:
                src = edge.at[0 if d[2] == 1 else 1, where]
                copies.append(remote(src, edges.at[pl.ds(at, len(need))], send_sem.at[1], recv_sem.at[1], to))
        return copies

    def await_all(ref, sem):
        pltpu.make_async_copy(ref, ref, sem).wait()

    def await_halo(recv, edges, sem):
        await_all(recv, sem.at[0])
        await_all(edges, sem.at[1])

    barrier = pltpu.get_barrier_semaphore()

    greeted = [device(d) for d in reversed([*partners])]
    greeted += [member(d, 1, which) for group in (near_chips, wide_chips) for d in group if any(d.values()) for which in (0, 1)]
    greeted.append(member({}, 1, 1 - core))
    for to in greeted:
        pl.semaphore_signal(barrier, inc=1, device_id=to, device_id_type=MESH)

    loads = [
        pltpu.make_async_copy(o_in, planes_in.at[0], in_sem.at[0]),
        pltpu.make_async_copy(occ_in, occ_planes, in_sem.at[1]),
        pltpu.make_async_copy(v_in, planes_in.at[1], in_sem.at[2]),
    ]
    for load in loads:
        load.start()

    lane = lax.broadcasted_iota(jnp.int32, (nz, lanes), 1)
    level = lax.broadcasted_iota(jnp.int32, (nz, lanes), 0)
    spread = (
        lax.rem(lax.broadcasted_iota(jnp.int32, (slots, lanes), 1), slots)
        == lax.broadcasted_iota(jnp.int32, (slots, lanes), 0)
    ).astype(jnp.float32)

    def rows_of(planes):
        flat = planes.reshape(-1, slots)
        wide = jnp.dot(flat, spread, precision=lax.Precision.HIGHEST, preferred_element_type=jnp.float32)
        wide = wide.reshape(-1, nz, lanes)
        return jnp.sum(jnp.where((lane // slots == level)[None], wide, 0.0), axis=1)

    for load in loads:
        load.wait()
    o_rows = rows_of(planes_in[0])
    v_rows = rows_of(planes_in[1])
    w_rows = rows_of(occ_planes[...].astype(jnp.float32))
    osend[...] = jnp.zeros_like(osend)
    kept[...] = jnp.zeros_like(kept)
    vsend[...] = jnp.zeros_like(vsend)
    fsend[...] = jnp.zeros_like(fsend)
    for x in range(nx):
        for y in range(ny):
            w = w_rows[x * ny + y : x * ny + y + 1]
            for c in range(3):
                i = (x * ny + y) * 3 + c
                r = c * nx + x
                kept[y, r : r + 1] = o_rows[i : i + 1]
                osend[y, r : r + 1] = jnp.where(w > 0.5, o_rows[i : i + 1], FAR)
                vsend[y, r : r + 1] = v_rows[i : i + 1] * w

    quarter = lanes // 4
    row_lane = lane[:1]

    tally[...] = jnp.broadcast_to(jnp.sum(w_rows, keepdims=True), (1, lanes))

    tile_lane = lax.broadcasted_iota(jnp.int32, (tile, lanes), 1)
    tile_row = lax.broadcasted_iota(jnp.int32, (tile, lanes), 0)
    slot_lane = lax.rem(tile_lane, slots)
    ends = [[slot_lane + (i if side == 0 else nz - 1 - i) * slots for i in range(2)] for side in range(2)]
    back = tile_row * slots + lax.rem(tile_lane, slots)

    def packed(block, side, depth=0):
        taken = jnp.take_along_axis(block, ends[side][depth], axis=1, mode="promise_in_bounds")
        return jnp.sum(jnp.where(tile_lane // slots == tile_row, taken, 0.0), axis=0, keepdims=True)

    def unpacked(row):
        wide = jnp.broadcast_to(row, (tile, lanes))
        return jnp.take_along_axis(wide, back, axis=1, mode="promise_in_bounds")

    for side in range(2):
        for y in range(ny):
            for depth in range(2):
                oedge[side, 2 * y + depth] = packed(osend[y], side, depth)
            vedge[side, y] = packed(vsend[y], side)

    pl.semaphore_wait(barrier, len(greeted))
    places, _, _ = deep_places(axes, ny)
    for d, at in reversed([*places.items()]):
        to = device(tuple(-x for x in d))
        if d[2] == 0:
            remote(osend, orecv.at[pl.ds(at, ny)], o_sem.at[0], o_recv_sem.at[d[1] % 3, 0], to).start()
        else:
            src = oedge.at[0 if d[2] == 1 else 1]
            remote(src, oedges.at[pl.ds(at, 2 * ny)], o_sem.at[1], o_recv_sem.at[d[1] % 3, 1], to).start()
    for copy in copies_of(vsend, vrecv, vedge, vedges, v_sem.at[0], v_sem.at[1]):
        copy.start()

    def columns(send, recv, edges):
        found = {}
        for xi, a in enumerate(xs):
            for py, (b, yl) in enumerate(py_of):
                if (a, b) == (0, 0):
                    mid = send[yl]
                else:
                    need, at = partners[a, b, 0]
                    mid = recv[at + need.index(yl)]
                ends_of = []
                for c in (-1, 1):
                    need, at = partners[a, b, c]
                    ends_of.append(unpacked(edges[at + need.index(yl)]))
                below, above = ends_of
                found[xi, py, 1] = mid
                low = jnp.where(tile_lane >= lanes - slots, below, mid)
                found[xi, py, 0] = pltpu.roll(low, slots, 1)
                high = jnp.where(tile_lane < slots, above, mid)
                found[xi, py, 2] = pltpu.roll(high, lanes - slots, 1)
        return found

    cell = tile_lane // slots
    deep_x, deep_y = deep(gx, nx), deep(gy, ny)
    pairs = ny + 2

    def lay(xi, at, mid, below, above):
        below, above = ([unpacked(oedges[e + depth]) for depth in range(2)] for e in (below, above))
        low = jnp.where(tile_lane >= lanes - slots, below[0], mid)
        high = jnp.where(tile_lane < slots, above[0], mid)
        around[xi, at, 0] = pltpu.roll(low, slots, 1)
        around[xi, at, 1] = mid
        around[xi, at, 2] = pltpu.roll(high, lanes - slots, 1)
        bottom = jnp.where(cell == 0, below[1], jnp.where(cell == 1, below[0], pltpu.roll(mid, 2 * slots, 1)))
        top = jnp.where(cell == nz - 1, above[1], above[0])
        top = jnp.where(cell == nz - 3, pltpu.roll(mid, lanes - 2 * slots, 1), top)
        ends_of[xi, at] = jnp.where(cell < nz // 2, bottom, top)

    def await_row(b, level_tiles):
        await_all(orecv.at[pl.ds(0, level_tiles)], o_recv_sem.at[b, 0])
        await_all(oedges.at[pl.ds(0, 4 * ny * len(xs))], o_recv_sem.at[b, 1])

    def lay_beside(up):
        await_row(2 - up, ny * len(xs))
        for xi, a in enumerate(xs):
            above, below = ([places[a, canonical(gy, b), c] for c in (0, -1, 1)] for b in (1, -1))
            level_at, low_at, high_at = (m + up * (p - m) for p, m in zip(above, below))
            for yl in range(2):
                layer = (ny - 2) * (1 - up) + yl
                lay(
                    xi, yl + up * (ny + 2), orecv[level_at + layer], low_at + 2 * layer, high_at + 2 * layer
                )

    def lay_packed():
        for xi in range(len(xs)):
            for dy in range(3):
                for dz in range(3):
                    centre = jnp.where(lax.rem(cell, 2) == 0, dz, nz - 3 + dz)
                    source = centre * slots + slot_lane
                    gathered = jnp.zeros((tile, lanes), jnp.float32)
                    for t in range(pairs):
                        taken = jnp.take_along_axis(ends_of[xi, t + dy], source, axis=1, mode="promise_in_bounds")
                        gathered = jnp.where(cell // 2 == t, taken, gathered)
                    around[xi, pairs + 2 + dy, dz] = gathered

    lane_id = lax.broadcasted_iota(jnp.int32, (slots, lanes), 1)
    slot_id = lax.broadcasted_iota(jnp.int32, (slots, lanes), 0)
    pick = (lane_id // slots) * slots + slot_id
    itself = lax.rem(lane_id, slots) == slot_id

    def nearby(py):
        for px, (a, xl) in enumerate(px_of):
            for dz in range(3):
                for c in range(3):
                    r = c * nx + xl
                    row = jnp.broadcast_to(ostate[xs.index(a), py, dz, r : r + 1], (slots, lanes))
                    near[px, py, dz, c] = jnp.take_along_axis(row, pick, axis=1, mode="promise_in_bounds")

    half = 0.5 * TIME_STEP
    reach2 = CUTOFF * CUTOFF

    def terms(squared):
        inv = lax.rsqrt(squared)
        inv2 = inv * inv
        inv6 = inv2 * inv2 * inv2
        inv12 = inv6 * inv6
        bond = inv12 - inv6
        return inv, bond, inv * (bond + inv12)

    _, _, edge = terms(jnp.full((slots, lanes), reach2, jnp.float32))
    pair_count = 27.0 * slots

    def pair_sums(mine, near_of):
        force = [jnp.zeros((slots, lanes), jnp.float32) for _ in range(3)]
        bonds, reach = (jnp.zeros((slots, lanes), jnp.float32) for _ in range(2))
        for shift in itertools.product((-1, 0, 1), repeat=3):
            apart = [near_of(shift, c) - (mine[c] - shift[c] * CELL_SIDE) for c in range(3)]
            squared = apart[0] * apart[0] + apart[1] * apart[1] + apart[2] * apart[2]
            if shift == (0, 0, 0):
                squared = jnp.where(itself, reach2, squared)
            squared = jnp.minimum(squared, reach2)
            inv, bond, push = terms(squared)
            pull = inv * (edge - push)
            for c in range(3):
                force[c] = force[c] + pull * apart[c]
            bonds = bonds + bond
            reach = reach + squared * inv
        return [24.0 * jnp.sum(f, axis=0, keepdims=True) for f in force], bonds, reach

    def first_row(i, _):
        centre = i + 1 + 2 * (i // pairs)
        for px, (a, xl) in enumerate(deep_x):
            for dy in range(3):
                for dz in range(3):
                    for c in range(3):
                        r = c * nx + xl
                        row = jnp.broadcast_to(around[xs.index(a), centre - 1 + dy, dz, r : r + 1], (slots, lanes))
                        first_near[px, dy, dz, c] = jnp.take_along_axis(row, pick, axis=1, mode="promise_in_bounds")
        for px, (a, xl) in enumerate(px_of):
            block = around[xs.index(a), centre, 1]
            mine = [block[c * nx + xl : c * nx + xl + 1] for c in range(3)]
            force, _, _ = pair_sums(
                mine, lambda shift, c: first_near[px + 1 + shift[0], 1 + shift[1], 1 + shift[2], c]
            )
            for c in range(3):
                r = c * nx + xl
                first_force[xs.index(a), i, r : r + 1] = jnp.where(mine[0] < 0.5 * FAR, force[c], 0.0)
        return 0

    first_force[...] = jnp.zeros_like(first_force)
    await_row(0, ny * (len(xs) - 1))
    for xi, a in enumerate(xs):
        for yl in range(ny):
            mid = osend[yl] if a == 0 else orecv[places[a, 0, 0] + yl]
            lay(xi, yl + 2, mid, places[a, 0, -1] + 2 * yl, places[a, 0, 1] + 2 * yl)
    lay_beside(1 - core)
    near_rows = pairs // 2
    lax.fori_loop(0, near_rows, lambda t, _: first_row(t + near_rows * (1 - core), 0), 0)
    lay_beside(core)
    lay_packed()
    last = pairs - near_rows
    lax.fori_loop(
        0, last + 1, lambda t, _: first_row((t + near_rows * core) * (1 - t // last) + pairs * (t // last), 0), 0
    )

    await_halo(vrecv, vedges, v_sem.at[1])
    first_v = columns(vsend, vrecv, vedges)
    for xi in range(len(xs)):
        outer = first_force[xi, pairs]
        for py in range(pairs):
            mid = first_force[xi, py]
            low = jnp.where(tile_lane < slots, pltpu.roll(outer, (lanes - 2 * py * slots) % lanes, 1), pltpu.roll(mid, slots, 1))
            high = jnp.where(
                tile_lane >= lanes - slots,
                pltpu.roll(outer, lanes - 2 * (py + 1) * slots, 1),
                pltpu.roll(mid, lanes - slots, 1),
            )
            for dz, f in enumerate((low, mid, high)):
                v = first_v[xi, py, dz] + half * f
                vstate[xi, py, dz] = v
                ostate[xi, py, dz] = around[xi, py + 1, dz] + TIME_STEP * v

    def step(k, _):
        p = lax.rem(k, 2)
        for py in range(ny + 2):
            nearby(py)

        energy_rows = jnp.zeros((1, lanes), jnp.float32)
        for x in range(nx):
            for y in range(ny):
                block = ostate[0, y + 1, 1]
                mine = [block[c * nx + x : c * nx + x + 1] for c in range(3)]
                occupied = mine[0] < 0.5 * FAR
                force, bonds, reach = pair_sums(
                    mine, lambda shift, c: near[x + 1 + shift[0], y + 1 + shift[1], 1 + shift[2], c]
                )
                for c in range(3):
                    r = c * nx + x
                    fsend[p, y, r : r + 1] = jnp.where(occupied, force[c], 0.0)
                energy = 4.0 * bonds + FORCE_EDGE * reach
                total = jnp.sum(energy, axis=0, keepdims=True)
                total = total - pair_count * (ENERGY_EDGE + CUTOFF * FORCE_EDGE)
                energy_rows = energy_rows + jnp.where(occupied, total, 0.0)

        kinetic = jnp.zeros((tile, lanes), jnp.float32)
        for y in range(ny):
            v = vstate[0, y + 1, 1] + half * fsend[p, y]
            kinetic = kinetic + v * v
        kinetic = jnp.sum(jnp.sum(kinetic, axis=0, keepdims=True), axis=1, keepdims=True)
        potential = jnp.sum(energy_rows, axis=1, keepdims=True)
        row = jnp.where(
            row_lane < 2 * quarter, 0.5 * kinetic, jnp.where(row_lane < 3 * quarter, 0.5 * potential, tally[...])
        )
        row_sum[...] = row
        at = index_in(NEAR) * 2 + core
        for d in near_chips:
            if any(d.values()):
                remote(row_sum, near_sums.at[p, at], near_send, near_recv.at[p], member(d, -1, 1)).start()

        @pl.when(follows)
        def _():
            remote(row_sum, near_sums.at[p, at], near_send, near_recv.at[p], member({}, 1, 1)).start()

        @pl.when(leads)
        def _():
            near_sums[p, at] = row

        @pl.when(k < STEPS)
        def _():
            for side in range(2):
                for y in range(ny):
                    fedge[p, side, y] = packed(fsend[p, y], side)
            for copy in copies_of(
                fsend.at[p], frecv.at[p], fedge.at[p], fedges.at[p], f_send_sem, f_recv_sem.at[p]
            ):
                copy.start()

        def total_of(ref, n):
            parts = [ref[p, i] for i in range(n)]
            while len(parts) > 1:
                parts = [sum(parts[i + 1 : i + 2], parts[i]) for i in range(0, len(parts), 2)]
            return parts[0]

        n_near, n_wide = len(near_chips), len(wide_chips)

        @pl.when(leads)
        def _():
            await_all(near_sums.at[p, pl.ds(0, 2 * n_near - 1)], near_recv.at[p])
            row = total_of(near_sums, 2 * n_near)
            chip_sum[...] = row
            at = index_in(WIDE)
            for d in wide_chips:
                for which in (0, 1):
                    if which == 0 or any(d.values()):
                        remote(
                            chip_sum, wide_sums.at[p, at], wide_send, wide_recv.at[p], member(d, -1, which)
                        ).start()
            wide_sums[p, at] = row

        @pl.when(k < STEPS)
        def _():
            await_halo(frecv.at[p], fedges.at[p], f_recv_sem.at[p])
            await_halo(frecv.at[p], fedges.at[p], f_send_sem)
            for (xi, py, dz), f in columns(fsend.at[p], frecv.at[p], fedges.at[p]).items():
                vstate[xi, py, dz] = vstate[xi, py, dz] + half * f
                held[xi, py, dz] = half * f

        @pl.when(leads)
        def _():
            await_all(near_sums.at[p, pl.ds(0, n_near - 1)], near_send)
            await_all(wide_sums.at[p, pl.ds(0, n_wide - 1)], wide_recv.at[p])

        @pl.when(follows)
        def _():
            await_all(near_sums.at[p, pl.ds(0, n_near)], near_send)
            await_all(wide_sums.at[p], wide_recv.at[p])

        row = total_of(wide_sums, n_wide)

        def across(part):
            return jnp.full((1, lanes), row[0, part * quarter], jnp.float32)

        vigor, potential, count = across(0), across(2), across(3)
        square = (1.0 - BATH_STRENGTH) + (BATH_STRENGTH * GOAL_WARMTH * 1.5) * count / vigor
        which = lax.broadcasted_iota(jnp.int32, (2, lanes), 1)
        record = jnp.concatenate([potential, square * vigor], axis=0) / slot_total
        history[...] = jnp.where(which == k - 1, record, history[...])

        @pl.when(leads)
        def _():
            await_all(wide_out, wide_send)

        lam = jnp.sqrt(square)

        @pl.when(k < STEPS)
        def _():
            for xi in range(len(xs)):
                for py in range(ny + 2):
                    for dz in range(3):
                        v = vstate[xi, py, dz] * lam + held[xi, py, dz]
                        vstate[xi, py, dz] = v
                        ostate[xi, py, dz] = ostate[xi, py, dz] + TIME_STEP * v

        @pl.when(k == STEPS)
        def _():
            for y in range(ny):
                here = ostate[0, y + 1, 1]
                result[y] = jnp.where(here < 0.5 * FAR, here, kept[y])
                result[ny + y] = (vstate[0, y + 1, 1] + half * fsend[p, y]) * lam
                result[2 * ny + y] = fsend[p, y]
            result[3 * ny, 0:2] = history[...]

        return 0

    history[...] = jnp.zeros_like(history)
    lax.fori_loop(1, STEPS + 1, step, 0)
    await_halo(orecv, oedges, o_sem)
    await_halo(vrecv, vedges, v_sem.at[0])


def unpack(shape, result, o_out, v_out, f_out, h_out):
    nx, ny, nz, slots = shape
    lanes = nz * slots
    at = lax.broadcasted_iota(jnp.int32, (nz, lanes), 0) * slots + lax.rem(
        lax.broadcasted_iota(jnp.int32, (nz, lanes), 1), slots
    )
    for i, ref in enumerate((o_out, v_out, f_out)):
        for y in range(ny):
            for x in range(nx):
                for c in range(3):
                    r = c * nx + x
                    row = jnp.broadcast_to(result[i * ny + y, r : r + 1], (nz, lanes))
                    ref[x, y, c] = jnp.take_along_axis(row, at, axis=1, mode="promise_in_bounds")[:, :slots]
    h_out[...] = result[3 * ny, 0:2, :STEPS]


def shards(axes, offsets, velocities, occupied):
    nx, ny, nz, slots = occupied.shape
    lanes = nz * slots
    tile = lanes // slots
    assert axes[2] > 2 and tile >= 3 * nx and min(nx, ny) >= 2 and ny % 2 == 0 and nz == 2 * (ny + 2)
    _, flats, rows = partners_of(axes, ny)
    _, deep_flats, deep_rows = deep_places(axes, ny)
    nxo = len(offsets_of(axes[0]))
    n_near, n_wide = (len(chips_of(axes, group)) for group in (NEAR, WIDE))
    f32 = jnp.float32
    plane = jax.ShapeDtypeStruct((nx, ny, 3, nz, slots), f32)
    vmem = pl.BlockSpec(memory_space=pltpu.VMEM)
    dma = pltpu.SemaphoreType.DMA
    state = pltpu.VMEM((nxo, ny + 2, 3, tile, lanes), f32)
    halo = [
        pltpu.VMEM((ny, tile, lanes), f32),
        pltpu.VMEM((flats, tile, lanes), f32),
        pltpu.VMEM((2, ny, 1, lanes), f32),
        pltpu.VMEM((rows, 1, lanes), f32),
    ]
    result = pl.pallas_call(
        functools.partial(kernel, axes, (nx, ny, nz, slots)),
        name="verlet",
        out_shape=pltpu.VMEM((3 * ny + 1, tile, lanes), f32),
        in_specs=[pl.BlockSpec(memory_space=pltpu.HBM)] * 3,
        out_specs=vmem,
        scratch_shapes=[
            pltpu.VMEM((2, nx, ny, 3, nz, slots), f32),
            pltpu.VMEM((ny, tile, lanes), f32),
            state,
            state,
            state,
            pltpu.VMEM((nx + 2, ny + 2, 3, 3, slots, lanes), f32),
            pltpu.VMEM((nxo, ny + 7, 3, tile, lanes), f32),
            pltpu.VMEM((nxo, ny + 4, tile, lanes), f32),
            pltpu.VMEM((nx + 4, 3, 3, 3, slots, lanes), f32),
            pltpu.VMEM((nxo, ny + 3, tile, lanes), f32),
            pltpu.VMEM((ny, tile, lanes), f32),
            pltpu.VMEM((deep_flats, tile, lanes), f32),
            pltpu.VMEM((2, 2 * ny, 1, lanes), f32),
            pltpu.VMEM((deep_rows, 1, lanes), f32),
            *halo,
            pltpu.VMEM((nx, ny, nz, slots), jnp.int32),
            pltpu.VMEM((2, ny, tile, lanes), f32),
            pltpu.VMEM((2, flats, tile, lanes), f32),
            pltpu.VMEM((2, 2, ny, 1, lanes), f32),
            pltpu.VMEM((2, rows, 1, lanes), f32),
            pltpu.VMEM((1, lanes), f32),
            pltpu.VMEM((2, lanes), f32),
            pltpu.VMEM((1, lanes), f32),
            pltpu.VMEM((2, 2 * n_near, 1, lanes), f32),
            pltpu.VMEM((1, lanes), f32),
            pltpu.VMEM((2, n_wide, 1, lanes), f32),
            pltpu.VMEM((2 * n_wide - 1, 1, lanes), f32),
            dma((3,)),
            dma((2,)),
            dma((3, 2)),
            dma((2, 2)),
            dma((2,)),
            dma((2, 2)),
            dma,
            dma((2,)),
            dma,
            dma((2,)),
        ],
        compiler_params=pltpu.CompilerParams(
            collective_id=0, has_side_effects=True, vmem_limit_bytes=VERLET_VMEM
        ),
    )(
        jnp.transpose(offsets, (0, 1, 4, 2, 3)),
        jnp.transpose(velocities, (0, 1, 4, 2, 3)),
        occupied,
    )
    o, v, f, h = pl.pallas_call(
        functools.partial(unpack, (nx, ny, nz, slots)),
        name="unpack",
        out_shape=[plane, plane, plane, jax.ShapeDtypeStruct((2, STEPS), f32)],
        in_specs=[vmem],
        out_specs=[vmem] * 4,
        compiler_params=pltpu.CompilerParams(vmem_limit_bytes=UNPACK_VMEM),
    )(result)
    back = (0, 1, 3, 4, 2)
    return (jnp.transpose(o, back), jnp.transpose(v, back), jnp.transpose(f, back), h.T)


def solution(mesh):
    axes = tuple(mesh.shape[a] for a in ("gx", "gy", "gz"))
    in_specs = (
        P("gx", "gy", "gz", None, None),
        P("gx", "gy", "gz", None, None),
        P("gx", "gy", "gz", None),
    )
    out_specs = (
        P("gx", "gy", "gz", None, None),
        P("gx", "gy", "gz", None, None),
        P("gx", "gy", "gz", None, None),
        P(),
    )
    return jax.shard_map(
        functools.partial(shards, axes), mesh=mesh, in_specs=in_specs, out_specs=out_specs, check_vma=False
    )
```

```python
import functools
import itertools

import jax
import jax.numpy as jnp
from jax import lax
from jax.experimental import pallas as pl
from jax.experimental.pallas import tpu as pltpu
from jax.sharding import PartitionSpec as P

MESH = pl.DeviceIdType.MESH
STEPS = 4
CUTOFF = 2.5
CELL_SIDE = 2.6
TIME_STEP = 0.005
BATH_STRENGTH = 0.25
GOAL_WARMTH = 0.8
FORCE_EDGE = 24.0 * (2.0 * CUTOFF ** (-13) - CUTOFF ** (-7))
ENERGY_EDGE = 4.0 * (CUTOFF ** (-12) - CUTOFF ** (-6))
FAR = 32.0
VERLET_VMEM = 60 * 1024 * 1024
UNPACK_VMEM = 4 * 1024 * 1024


NEAR = ("z",)
WIDE = ("xl", "xh", "y")


def parts_of(axes):
    gx, gy, gz = axes
    return {"xl": gx // 4, "y": 4, "xh": gy // 2, "z": gz}


def chips_of(axes, group):
    sizes = parts_of(axes)

    def hops(d):
        return sum(min(o, sizes[a] - o) for a, o in d.items())

    every = itertools.product(*[range(sizes[a]) for a in group])
    return sorted((dict(zip(group, d)) for d in every), key=lambda d: -hops(d))


def offsets_of(size):
    return [0] if size == 1 else [0, 1] if size == 2 else [0, 1, -1]


def canonical(size, off):
    return 0 if size == 1 else off % 2 if size == 2 else off


def padded(size, n):
    return [(canonical(size, -1), n - 1)] + [(0, i) for i in range(n)] + [(canonical(size, 1), 0)]


def deep(size, n):
    low, high = canonical(size, -1), canonical(size, 1)
    return [(low, n - 2), (low, n - 1)] + [(0, i) for i in range(n)] + [(high, 0), (high, 1)]


def deep_places(axes, ny):
    flat, rows, found = 0, 0, {}
    for d in itertools.product(*[offsets_of(n) for n in axes]):
        if d == (0, 0, 0):
            continue
        if d[2] == 0:
            found[d] = flat
            flat += ny
        else:
            found[d] = rows
            rows += 2 * ny
    return found, flat, rows


def partners_of(axes, ny):
    every = itertools.product(*[offsets_of(n) for n in axes])
    flat, rows, found = 0, 0, {}
    for d in every:
        if d == (0, 0, 0):
            continue
        need = sorted({yl for off, yl in padded(axes[1], ny) if off == d[1]})
        if d[2] == 0:
            found[d] = need, flat
            flat += len(need)
        else:
            found[d] = need, rows
            rows += len(need)
    return found, flat, rows


def kernel(
    axes, shape, o_in, v_in, occ_in, result,
    planes_in, kept, ostate, vstate, held, near, around, ends_of, first_near, first_force, osend, orecv, oedge, oedges, vsend, vrecv, vedge, vedges,
    occ_planes, fsend, frecv, fedge, fedges, tally, history, row_sum, near_sums, chip_sum, wide_sums, measure,
    in_sem, first_sem, o_recv_sem, v_sem, f_send_sem, f_recv_sem, sum_send, near_recv, wide_recv,
):
    gx, gy, gz = axes
    nx, ny, nz, slots = shape
    lanes = nz * slots
    tile = fsend.shape[2]
    slot_total = float(gx * gy * gz * nx * ny * lanes)
    me = [lax.axis_index(a) for a in ("gx", "gy", "gz")]
    sizes = parts_of(axes)
    place = {"xl": me[0] // 4, "y": lax.rem(me[0], 4), "xh": me[1] // 2, "z": me[2]}
    core = lax.rem(me[1], 2)
    leads = core == 1
    follows = core == 0
    near_chips, wide_chips = chips_of(axes, NEAR), chips_of(axes, WIDE)

    turned = [[lax.rem(me[i] + j, n) for j in range(n)] for i, n in enumerate(axes)]

    def device(d):
        return tuple(turned[i][d[i] % axes[i]] for i in range(3))

    def member(d, sign, which):
        at = dict(place)
        for a, o in d.items():
            if o:
                at[a] = lax.rem(at[a] + (o if sign > 0 else sizes[a] - o), sizes[a])
        return (at["xl"] * 4 + at["y"], at["xh"] * 2 + which, at["z"])

    def index_in(group):
        at = 0
        for a in group:
            at = at * sizes[a] + place[a]
        return at

    px_of, py_of = padded(gx, nx), padded(gy, ny)
    xs = offsets_of(gx)
    partners, flats, rows = partners_of(axes, ny)

    def remote(src, dst, send_sem, recv_sem, to):
        return pltpu.make_async_remote_copy(
            src_ref=src, dst_ref=dst, send_sem=send_sem, recv_sem=recv_sem, device_id=to, device_id_type=MESH
        )

    def copies_of(send, recv, edge, edges, send_sem, recv_sem):
        copies = []
        for d, (need, at) in reversed([*partners.items()]):
            where = pl.ds(need[0], len(need))
            to = device(tuple(-x for x in d))
            if d[2] == 0:
                copies.append(remote(send.at[where], recv.at[pl.ds(at, len(need))], send_sem, recv_sem, to))
            else:
                src = edge.at[0 if d[2] == 1 else 1, where]
                copies.append(remote(src, edges.at[pl.ds(at, len(need))], send_sem, recv_sem, to))
        return copies

    def await_all(ref, sem):
        pltpu.make_async_copy(ref, ref, sem).wait()

    def await_rows(n, sem):
        await_all(measure.at[pl.ds(0, n)], sem)

    halo_rows = flats * tile + rows
    deep_rows = sum(ny * tile if d[2] == 0 else 2 * ny for d in deep_places(axes, ny)[0])

    barrier = pltpu.get_barrier_semaphore()

    greeted = [device(d) for d in reversed([*partners])]
    greeted += [member(d, 1, which) for group in (near_chips, wide_chips) for d in group if any(d.values()) for which in (0, 1)]
    greeted.append(member({}, 1, 1 - core))
    for to in greeted:
        pl.semaphore_signal(barrier, inc=1, device_id=to, device_id_type=MESH)

    loads = [
        pltpu.make_async_copy(o_in, planes_in.at[0], in_sem.at[0]),
        pltpu.make_async_copy(occ_in, occ_planes, in_sem.at[1]),
        pltpu.make_async_copy(v_in, planes_in.at[1], in_sem.at[0]),
    ]
    for load in loads:
        load.start()

    lane = lax.broadcasted_iota(jnp.int32, (nz, lanes), 1)
    level = lax.broadcasted_iota(jnp.int32, (nz, lanes), 0)
    spread = (
        lax.rem(lax.broadcasted_iota(jnp.int32, (slots, lanes), 1), slots)
        == lax.broadcasted_iota(jnp.int32, (slots, lanes), 0)
    ).astype(jnp.float32)

    def rows_of(planes):
        flat = planes.reshape(-1, slots)
        wide = jnp.dot(flat, spread, precision=lax.Precision.HIGHEST, preferred_element_type=jnp.float32)
        wide = wide.reshape(-1, nz, lanes)
        return jnp.sum(jnp.where((lane // slots == level)[None], wide, 0.0), axis=1)

    await_all(planes_in, in_sem.at[0])
    loads[1].wait()
    o_rows = rows_of(planes_in[0])
    v_rows = rows_of(planes_in[1])
    w_rows = rows_of(occ_planes[...].astype(jnp.float32))
    osend[...] = jnp.zeros_like(osend)
    kept[...] = jnp.zeros_like(kept)
    vsend[...] = jnp.zeros_like(vsend)
    fsend[...] = jnp.zeros_like(fsend)
    for x in range(nx):
        for y in range(ny):
            w = w_rows[x * ny + y : x * ny + y + 1]
            for c in range(3):
                i = (x * ny + y) * 3 + c
                r = c * nx + x
                kept[y, r : r + 1] = o_rows[i : i + 1]
                osend[y, r : r + 1] = jnp.where(w > 0.5, o_rows[i : i + 1], FAR)
                vsend[y, r : r + 1] = v_rows[i : i + 1] * w

    quarter = lanes // 4
    row_lane = lane[:1]

    tally[...] = jnp.broadcast_to(jnp.sum(w_rows, keepdims=True), (1, lanes))

    tile_lane = lax.broadcasted_iota(jnp.int32, (tile, lanes), 1)
    tile_row = lax.broadcasted_iota(jnp.int32, (tile, lanes), 0)
    slot_lane = lax.rem(tile_lane, slots)
    ends = [[slot_lane + (i if side == 0 else nz - 1 - i) * slots for i in range(2)] for side in range(2)]
    back = tile_row * slots + lax.rem(tile_lane, slots)

    def packed(block, side, depth=0):
        taken = jnp.take_along_axis(block, ends[side][depth], axis=1, mode="promise_in_bounds")
        return jnp.sum(jnp.where(tile_lane // slots == tile_row, taken, 0.0), axis=0, keepdims=True)

    def unpacked(row):
        wide = jnp.broadcast_to(row, (tile, lanes))
        return jnp.take_along_axis(wide, back, axis=1, mode="promise_in_bounds")

    for side in range(2):
        for y in range(ny):
            for depth in range(2):
                oedge[side, 2 * y + depth] = packed(osend[y], side, depth)
            vedge[side, y] = packed(vsend[y], side)

    pl.semaphore_wait(barrier, len(greeted))
    places, _, _ = deep_places(axes, ny)
    for d, at in reversed([*places.items()]):
        to = device(tuple(-x for x in d))
        if d[2] == 0:
            remote(osend, orecv.at[pl.ds(at, ny)], first_sem, o_recv_sem.at[d[1] % 3], to).start()
        else:
            src = oedge.at[0 if d[2] == 1 else 1]
            remote(src, oedges.at[pl.ds(at, 2 * ny)], first_sem, o_recv_sem.at[d[1] % 3], to).start()
    for copy in copies_of(vsend, vrecv, vedge, vedges, first_sem, v_sem):
        copy.start()

    def columns(send, recv, edges):
        found = {}
        for xi, a in enumerate(xs):
            for py, (b, yl) in enumerate(py_of):
                if (a, b) == (0, 0):
                    mid = send[yl]
                else:
                    need, at = partners[a, b, 0]
                    mid = recv[at + need.index(yl)]
                ends_of = []
                for c in (-1, 1):
                    need, at = partners[a, b, c]
                    ends_of.append(unpacked(edges[at + need.index(yl)]))
                below, above = ends_of
                found[xi, py, 1] = mid
                low = jnp.where(tile_lane >= lanes - slots, below, mid)
                found[xi, py, 0] = pltpu.roll(low, slots, 1)
                high = jnp.where(tile_lane < slots, above, mid)
                found[xi, py, 2] = pltpu.roll(high, lanes - slots, 1)
        return found

    cell = tile_lane // slots
    deep_x, deep_y = deep(gx, nx), deep(gy, ny)
    pairs = ny + 2

    def lay(xi, at, mid, below, above):
        below, above = ([unpacked(oedges[e + depth]) for depth in range(2)] for e in (below, above))
        low = jnp.where(tile_lane >= lanes - slots, below[0], mid)
        high = jnp.where(tile_lane < slots, above[0], mid)
        around[xi, at, 0] = pltpu.roll(low, slots, 1)
        around[xi, at, 1] = mid
        around[xi, at, 2] = pltpu.roll(high, lanes - slots, 1)
        bottom = jnp.where(cell == 0, below[1], jnp.where(cell == 1, below[0], pltpu.roll(mid, 2 * slots, 1)))
        top = jnp.where(cell == nz - 1, above[1], above[0])
        top = jnp.where(cell == nz - 3, pltpu.roll(mid, lanes - 2 * slots, 1), top)
        ends_of[xi, at] = jnp.where(cell < nz // 2, bottom, top)

    def await_row(b, level_tiles):
        await_rows(level_tiles * tile + 4 * ny * len(xs), o_recv_sem.at[b])

    def lay_beside(up):
        await_row(2 - up, ny * len(xs))
        for xi, a in enumerate(xs):
            above, below = ([places[a, canonical(gy, b), c] for c in (0, -1, 1)] for b in (1, -1))
            level_at, low_at, high_at = (m + up * (p - m) for p, m in zip(above, below))
            for yl in range(2):
                layer = (ny - 2) * (1 - up) + yl
                lay(
                    xi, yl + up * (ny + 2), orecv[level_at + layer], low_at + 2 * layer, high_at + 2 * layer
                )

    def lay_packed():
        for xi in range(len(xs)):
            for dy in range(3):
                for dz in range(3):
                    centre = jnp.where(lax.rem(cell, 2) == 0, dz, nz - 3 + dz)
                    source = centre * slots + slot_lane
                    gathered = jnp.zeros((tile, lanes), jnp.float32)
                    for t in range(pairs):
                        taken = jnp.take_along_axis(ends_of[xi, t + dy], source, axis=1, mode="promise_in_bounds")
                        gathered = jnp.where(cell // 2 == t, taken, gathered)
                    around[xi, pairs + 2 + dy, dz] = gathered

    lane_id = lax.broadcasted_iota(jnp.int32, (slots, lanes), 1)
    slot_id = lax.broadcasted_iota(jnp.int32, (slots, lanes), 0)
    pick = (lane_id // slots) * slots + slot_id
    itself = lax.rem(lane_id, slots) == slot_id

    def nearby(py):
        for px, (a, xl) in enumerate(px_of):
            for dz in range(3):
                for c in range(3):
                    r = c * nx + xl
                    row = jnp.broadcast_to(ostate[xs.index(a), py, dz, r : r + 1], (slots, lanes))
                    near[px, py, dz, c] = jnp.take_along_axis(row, pick, axis=1, mode="promise_in_bounds")

    half = 0.5 * TIME_STEP
    reach2 = CUTOFF * CUTOFF

    def terms(squared):
        inv = lax.rsqrt(squared)
        inv2 = inv * inv
        inv6 = inv2 * inv2 * inv2
        inv12 = inv6 * inv6
        bond = inv12 - inv6
        return inv, bond, inv * (bond + inv12)

    _, _, edge = terms(jnp.full((slots, lanes), reach2, jnp.float32))
    pair_count = 27.0 * slots

    def pair_sums(mine, near_of):
        force = [jnp.zeros((slots, lanes), jnp.float32) for _ in range(3)]
        bonds, reach = (jnp.zeros((slots, lanes), jnp.float32) for _ in range(2))
        for shift in itertools.product((-1, 0, 1), repeat=3):
            apart = [near_of(shift, c) - (mine[c] - shift[c] * CELL_SIDE) for c in range(3)]
            squared = apart[0] * apart[0] + apart[1] * apart[1] + apart[2] * apart[2]
            if shift == (0, 0, 0):
                squared = jnp.where(itself, reach2, squared)
            squared = jnp.minimum(squared, reach2)
            inv, bond, push = terms(squared)
            pull = inv * (edge - push)
            for c in range(3):
                force[c] = force[c] + pull * apart[c]
            bonds = bonds + bond
            reach = reach + squared * inv
        return [24.0 * jnp.sum(f, axis=0, keepdims=True) for f in force], bonds, reach

    def first_row(i, _):
        centre = i + 1 + 2 * (i // pairs)
        for px, (a, xl) in enumerate(deep_x):
            for dy in range(3):
                for dz in range(3):
                    for c in range(3):
                        r = c * nx + xl
                        row = jnp.broadcast_to(around[xs.index(a), centre - 1 + dy, dz, r : r + 1], (slots, lanes))
                        first_near[px, dy, dz, c] = jnp.take_along_axis(row, pick, axis=1, mode="promise_in_bounds")
        for px, (a, xl) in enumerate(px_of):
            block = around[xs.index(a), centre, 1]
            mine = [block[c * nx + xl : c * nx + xl + 1] for c in range(3)]
            force, _, _ = pair_sums(
                mine, lambda shift, c: first_near[px + 1 + shift[0], 1 + shift[1], 1 + shift[2], c]
            )
            for c in range(3):
                r = c * nx + xl
                first_force[xs.index(a), i, r : r + 1] = jnp.where(mine[0] < 0.5 * FAR, force[c], 0.0)
        return 0

    first_force[...] = jnp.zeros_like(first_force)
    await_row(0, ny * (len(xs) - 1))
    for xi, a in enumerate(xs):
        for yl in range(ny):
            mid = osend[yl] if a == 0 else orecv[places[a, 0, 0] + yl]
            lay(xi, yl + 2, mid, places[a, 0, -1] + 2 * yl, places[a, 0, 1] + 2 * yl)
    lay_beside(1 - core)
    near_rows = pairs // 2
    lax.fori_loop(0, near_rows, lambda t, _: first_row(t + near_rows * (1 - core), 0), 0)
    lay_beside(core)
    lay_packed()
    last = pairs - near_rows
    lax.fori_loop(
        0, last + 1, lambda t, _: first_row((t + near_rows * core) * (1 - t // last) + pairs * (t // last), 0), 0
    )

    await_rows(halo_rows, v_sem)
    first_v = columns(vsend, vrecv, vedges)
    for xi in range(len(xs)):
        outer = first_force[xi, pairs]
        for py in range(pairs):
            mid = first_force[xi, py]
            low = jnp.where(tile_lane < slots, pltpu.roll(outer, (lanes - 2 * py * slots) % lanes, 1), pltpu.roll(mid, slots, 1))
            high = jnp.where(
                tile_lane >= lanes - slots,
                pltpu.roll(outer, lanes - 2 * (py + 1) * slots, 1),
                pltpu.roll(mid, lanes - slots, 1),
            )
            for dz, f in enumerate((low, mid, high)):
                v = first_v[xi, py, dz] + half * f
                vstate[xi, py, dz] = v
                ostate[xi, py, dz] = around[xi, py + 1, dz] + TIME_STEP * v

    def step(k, _):
        p = lax.rem(k, 2)
        for py in range(ny + 2):
            nearby(py)

        energy_rows = jnp.zeros((1, lanes), jnp.float32)
        for x in range(nx):
            for y in range(ny):
                block = ostate[0, y + 1, 1]
                mine = [block[c * nx + x : c * nx + x + 1] for c in range(3)]
                occupied = mine[0] < 0.5 * FAR
                force, bonds, reach = pair_sums(
                    mine, lambda shift, c: near[x + 1 + shift[0], y + 1 + shift[1], 1 + shift[2], c]
                )
                for c in range(3):
                    r = c * nx + x
                    fsend[p, y, r : r + 1] = jnp.where(occupied, force[c], 0.0)
                energy = 4.0 * bonds + FORCE_EDGE * reach
                total = jnp.sum(energy, axis=0, keepdims=True)
                total = total - pair_count * (ENERGY_EDGE + CUTOFF * FORCE_EDGE)
                energy_rows = energy_rows + jnp.where(occupied, total, 0.0)

        kinetic = jnp.zeros((tile, lanes), jnp.float32)
        for y in range(ny):
            v = vstate[0, y + 1, 1] + half * fsend[p, y]
            kinetic = kinetic + v * v
        kinetic = jnp.sum(jnp.sum(kinetic, axis=0, keepdims=True), axis=1, keepdims=True)
        potential = jnp.sum(energy_rows, axis=1, keepdims=True)
        row = jnp.where(
            row_lane < 2 * quarter, 0.5 * kinetic, jnp.where(row_lane < 3 * quarter, 0.5 * potential, tally[...])
        )
        row_sum[...] = row
        at = index_in(NEAR) * 2 + core
        for d in near_chips:
            if any(d.values()):
                remote(row_sum, near_sums.at[p, at], sum_send, near_recv.at[p], member(d, -1, 1)).start()

        @pl.when(follows)
        def _():
            remote(row_sum, near_sums.at[p, at], sum_send, near_recv.at[p], member({}, 1, 1)).start()

        @pl.when(leads)
        def _():
            near_sums[p, at] = row

        @pl.when(k < STEPS)
        def _():
            for side in range(2):
                for y in range(ny):
                    fedge[p, side, y] = packed(fsend[p, y], side)
            for copy in copies_of(
                fsend.at[p], frecv.at[p], fedge.at[p], fedges.at[p], f_send_sem, f_recv_sem.at[p]
            ):
                copy.start()

        def total_of(ref, n):
            parts = [ref[p, i] for i in range(n)]
            while len(parts) > 1:
                parts = [sum(parts[i + 1 : i + 2], parts[i]) for i in range(0, len(parts), 2)]
            return parts[0]

        n_near, n_wide = len(near_chips), len(wide_chips)

        @pl.when(leads)
        def _():
            await_all(near_sums.at[p, pl.ds(0, 2 * n_near - 1)], near_recv.at[p])
            row = total_of(near_sums, 2 * n_near)
            chip_sum[...] = row
            at = index_in(WIDE)
            for d in wide_chips:
                for which in (0, 1):
                    if which == 0 or any(d.values()):
                        remote(
                            chip_sum, wide_sums.at[p, at], sum_send, wide_recv.at[p], member(d, -1, which)
                        ).start()
            wide_sums[p, at] = row

        @pl.when(k < STEPS)
        def _():
            await_rows(halo_rows, f_recv_sem.at[p])
            await_rows(halo_rows, f_send_sem)
            for (xi, py, dz), f in columns(fsend.at[p], frecv.at[p], fedges.at[p]).items():
                vstate[xi, py, dz] = vstate[xi, py, dz] + half * f
                held[xi, py, dz] = half * f

        @pl.when(leads)
        def _():
            await_all(wide_sums.at[p, pl.ds(0, n_wide - 1)], wide_recv.at[p])

        @pl.when(follows)
        def _():
            await_rows(n_near, sum_send)
            await_all(wide_sums.at[p], wide_recv.at[p])

        row = total_of(wide_sums, n_wide)

        def across(part):
            return jnp.full((1, lanes), row[0, part * quarter], jnp.float32)

        vigor, potential, count = across(0), across(2), across(3)
        square = (1.0 - BATH_STRENGTH) + (BATH_STRENGTH * GOAL_WARMTH * 1.5) * count / vigor
        which = lax.broadcasted_iota(jnp.int32, (2, lanes), 1)
        record = jnp.concatenate([potential, square * vigor], axis=0) / slot_total
        history[...] = jnp.where(which == k - 1, record, history[...])

        @pl.when(leads)
        def _():
            await_rows(n_near + 2 * n_wide - 2, sum_send)

        lam = jnp.sqrt(square)

        @pl.when(k < STEPS)
        def _():
            for xi in range(len(xs)):
                for py in range(ny + 2):
                    for dz in range(3):
                        v = vstate[xi, py, dz] * lam + held[xi, py, dz]
                        vstate[xi, py, dz] = v
                        ostate[xi, py, dz] = ostate[xi, py, dz] + TIME_STEP * v

        @pl.when(k == STEPS)
        def _():
            for y in range(ny):
                here = ostate[0, y + 1, 1]
                result[y] = jnp.where(here < 0.5 * FAR, here, kept[y])
                result[ny + y] = (vstate[0, y + 1, 1] + half * fsend[p, y]) * lam
                result[2 * ny + y] = fsend[p, y]
            result[3 * ny, 0:2] = history[...]

        return 0

    history[...] = jnp.zeros_like(history)
    lax.fori_loop(1, STEPS + 1, step, 0)
    await_rows(deep_rows + halo_rows, first_sem)


def unpack(shape, result, o_out, v_out, f_out, h_out):
    nx, ny, nz, slots = shape
    lanes = nz * slots
    at = lax.broadcasted_iota(jnp.int32, (nz, lanes), 0) * slots + lax.rem(
        lax.broadcasted_iota(jnp.int32, (nz, lanes), 1), slots
    )
    for i, ref in enumerate((o_out, v_out, f_out)):
        for y in range(ny):
            for x in range(nx):
                for c in range(3):
                    r = c * nx + x
                    row = jnp.broadcast_to(result[i * ny + y, r : r + 1], (nz, lanes))
                    ref[x, y, c] = jnp.take_along_axis(row, at, axis=1, mode="promise_in_bounds")[:, :slots]
    h_out[...] = result[3 * ny, 0:2, :STEPS]


def shards(axes, offsets, velocities, occupied):
    nx, ny, nz, slots = occupied.shape
    lanes = nz * slots
    tile = lanes // slots
    assert axes[2] > 2 and tile >= 3 * nx and min(nx, ny) >= 2 and ny % 2 == 0 and nz == 2 * (ny + 2)
    _, flats, rows = partners_of(axes, ny)
    _, deep_flats, deep_rows = deep_places(axes, ny)
    nxo = len(offsets_of(axes[0]))
    n_near, n_wide = (len(chips_of(axes, group)) for group in (NEAR, WIDE))
    f32 = jnp.float32
    plane = jax.ShapeDtypeStruct((nx, ny, 3, nz, slots), f32)
    vmem = pl.BlockSpec(memory_space=pltpu.VMEM)
    dma = pltpu.SemaphoreType.DMA
    state = pltpu.VMEM((nxo, ny + 2, 3, tile, lanes), f32)
    halo = [
        pltpu.VMEM((ny, tile, lanes), f32),
        pltpu.VMEM((flats, tile, lanes), f32),
        pltpu.VMEM((2, ny, 1, lanes), f32),
        pltpu.VMEM((rows, 1, lanes), f32),
    ]
    result = pl.pallas_call(
        functools.partial(kernel, axes, (nx, ny, nz, slots)),
        name="verlet",
        out_shape=pltpu.VMEM((3 * ny + 1, tile, lanes), f32),
        in_specs=[pl.BlockSpec(memory_space=pltpu.HBM)] * 3,
        out_specs=vmem,
        scratch_shapes=[
            pltpu.VMEM((2, nx, ny, 3, nz, slots), f32),
            pltpu.VMEM((ny, tile, lanes), f32),
            state,
            state,
            state,
            pltpu.VMEM((nx + 2, ny + 2, 3, 3, slots, lanes), f32),
            pltpu.VMEM((nxo, ny + 7, 3, tile, lanes), f32),
            pltpu.VMEM((nxo, ny + 4, tile, lanes), f32),
            pltpu.VMEM((nx + 4, 3, 3, 3, slots, lanes), f32),
            pltpu.VMEM((nxo, ny + 3, tile, lanes), f32),
            pltpu.VMEM((ny, tile, lanes), f32),
            pltpu.VMEM((deep_flats, tile, lanes), f32),
            pltpu.VMEM((2, 2 * ny, 1, lanes), f32),
            pltpu.VMEM((deep_rows, 1, lanes), f32),
            *halo,
            pltpu.VMEM((nx, ny, nz, slots), jnp.int32),
            pltpu.VMEM((2, ny, tile, lanes), f32),
            pltpu.VMEM((2, flats, tile, lanes), f32),
            pltpu.VMEM((2, 2, ny, 1, lanes), f32),
            pltpu.VMEM((2, rows, 1, lanes), f32),
            pltpu.VMEM((1, lanes), f32),
            pltpu.VMEM((2, lanes), f32),
            pltpu.VMEM((1, lanes), f32),
            pltpu.VMEM((2, 2 * n_near, 1, lanes), f32),
            pltpu.VMEM((1, lanes), f32),
            pltpu.VMEM((2, n_wide, 1, lanes), f32),
            pltpu.VMEM((deep_flats * tile + deep_rows + flats * tile + rows, 1, lanes), f32),
            dma((2,)),
            dma,
            dma((3,)),
            dma,
            dma,
            dma((2,)),
            dma,
            dma((2,)),
            dma((2,)),
        ],
        compiler_params=pltpu.CompilerParams(
            collective_id=0, has_side_effects=True, vmem_limit_bytes=VERLET_VMEM
        ),
    )(
        jnp.transpose(offsets, (0, 1, 4, 2, 3)),
        jnp.transpose(velocities, (0, 1, 4, 2, 3)),
        occupied,
    )
    o, v, f, h = pl.pallas_call(
        functools.partial(unpack, (nx, ny, nz, slots)),
        name="unpack",
        out_shape=[plane, plane, plane, jax.ShapeDtypeStruct((2, STEPS), f32)],
        in_specs=[vmem],
        out_specs=[vmem] * 4,
        compiler_params=pltpu.CompilerParams(vmem_limit_bytes=UNPACK_VMEM),
    )(result)
    back = (0, 1, 3, 4, 2)
    return (jnp.transpose(o, back), jnp.transpose(v, back), jnp.transpose(f, back), h.T)


def solution(mesh):
    axes = tuple(mesh.shape[a] for a in ("gx", "gy", "gz"))
    in_specs = (
        P("gx", "gy", "gz", None, None),
        P("gx", "gy", "gz", None, None),
        P("gx", "gy", "gz", None),
    )
    out_specs = (
        P("gx", "gy", "gz", None, None),
        P("gx", "gy", "gz", None, None),
        P("gx", "gy", "gz", None, None),
        P(),
    )
    return jax.shard_map(
        functools.partial(shards, axes), mesh=mesh, in_specs=in_specs, out_specs=out_specs, check_vma=False
    )
```

```python
import functools
import itertools

import jax
import jax.numpy as jnp
from jax import lax
from jax.experimental import pallas as pl
from jax.experimental.pallas import tpu as pltpu
from jax.sharding import PartitionSpec as P

MESH = pl.DeviceIdType.MESH
STEPS = 4
CUTOFF = 2.5
CELL_SIDE = 2.6
TIME_STEP = 0.005
BATH_STRENGTH = 0.25
GOAL_WARMTH = 0.8
FORCE_EDGE = 24.0 * (2.0 * CUTOFF ** (-13) - CUTOFF ** (-7))
ENERGY_EDGE = 4.0 * (CUTOFF ** (-12) - CUTOFF ** (-6))
FAR = 32.0
VERLET_VMEM = 60 * 1024 * 1024
UNPACK_VMEM = 4 * 1024 * 1024


NEAR = ("xl", "xh", "y")
WIDE = ("z",)


def parts_of(axes):
    gx, gy, gz = axes
    return {"xl": gx // 4, "y": 4, "xh": gy // 2, "z": gz}


def chips_of(axes, group):
    sizes = parts_of(axes)

    def hops(d):
        return sum(min(o, sizes[a] - o) for a, o in d.items())

    every = itertools.product(*[range(sizes[a]) for a in group])
    return sorted((dict(zip(group, d)) for d in every), key=lambda d: -hops(d))


def offsets_of(size):
    return [0] if size == 1 else [0, 1] if size == 2 else [0, 1, -1]


def canonical(size, off):
    return 0 if size == 1 else off % 2 if size == 2 else off


def padded(size, n):
    return [(canonical(size, -1), n - 1)] + [(0, i) for i in range(n)] + [(canonical(size, 1), 0)]


def deep(size, n):
    low, high = canonical(size, -1), canonical(size, 1)
    return [(low, n - 2), (low, n - 1)] + [(0, i) for i in range(n)] + [(high, 0), (high, 1)]


def deep_places(axes, ny):
    flat, rows, found = 0, 0, {}
    for d in itertools.product(*[offsets_of(n) for n in axes]):
        if d == (0, 0, 0):
            continue
        if d[2] == 0:
            found[d] = flat
            flat += ny
        else:
            found[d] = rows
            rows += 2 * ny
    return found, flat, rows


def partners_of(axes, ny):
    every = itertools.product(*[offsets_of(n) for n in axes])
    flat, rows, found = 0, 0, {}
    for d in every:
        if d == (0, 0, 0):
            continue
        need = sorted({yl for off, yl in padded(axes[1], ny) if off == d[1]})
        if d[2] == 0:
            found[d] = need, flat
            flat += len(need)
        else:
            found[d] = need, rows
            rows += len(need)
    return found, flat, rows


def kernel(
    axes, shape, o_in, v_in, occ_in, result,
    planes_in, kept, ostate, vstate, held, near, around, ends_of, first_near, first_force, osend, orecv, oedge, oedges, vsend, vrecv, vedge, vedges,
    occ_planes, fsend, frecv, fedge, fedges, tally, history, row_sum, near_sums, chip_sum, wide_sums, measure,
    in_sem, first_sem, o_recv_sem, v_sem, f_send_sem, f_recv_sem, sum_send, near_recv, wide_recv,
):
    gx, gy, gz = axes
    nx, ny, nz, slots = shape
    lanes = nz * slots
    tile = fsend.shape[2]
    slot_total = float(gx * gy * gz * nx * ny * lanes)
    me = [lax.axis_index(a) for a in ("gx", "gy", "gz")]
    sizes = parts_of(axes)
    place = {"xl": me[0] // 4, "y": lax.rem(me[0], 4), "xh": me[1] // 2, "z": me[2]}
    core = lax.rem(me[1], 2)
    leads = core == 1
    follows = core == 0
    near_chips, wide_chips = chips_of(axes, NEAR), chips_of(axes, WIDE)

    turned = [[lax.rem(me[i] + j, n) for j in range(n)] for i, n in enumerate(axes)]

    def device(d):
        return tuple(turned[i][d[i] % axes[i]] for i in range(3))

    def member(d, sign, which):
        at = dict(place)
        for a, o in d.items():
            if o:
                at[a] = lax.rem(at[a] + (o if sign > 0 else sizes[a] - o), sizes[a])
        return (at["xl"] * 4 + at["y"], at["xh"] * 2 + which, at["z"])

    def index_in(group):
        at = 0
        for a in group:
            at = at * sizes[a] + place[a]
        return at

    px_of, py_of = padded(gx, nx), padded(gy, ny)
    xs = offsets_of(gx)
    partners, flats, rows = partners_of(axes, ny)

    def remote(src, dst, send_sem, recv_sem, to):
        return pltpu.make_async_remote_copy(
            src_ref=src, dst_ref=dst, send_sem=send_sem, recv_sem=recv_sem, device_id=to, device_id_type=MESH
        )

    def copies_of(send, recv, edge, edges, send_sem, recv_sem):
        copies = []
        for d, (need, at) in reversed([*partners.items()]):
            where = pl.ds(need[0], len(need))
            to = device(tuple(-x for x in d))
            if d[2] == 0:
                copies.append(remote(send.at[where], recv.at[pl.ds(at, len(need))], send_sem, recv_sem, to))
            else:
                src = edge.at[0 if d[2] == 1 else 1, where]
                copies.append(remote(src, edges.at[pl.ds(at, len(need))], send_sem, recv_sem, to))
        return copies

    def await_all(ref, sem):
        pltpu.make_async_copy(ref, ref, sem).wait()

    def await_rows(n, sem):
        await_all(measure.at[pl.ds(0, n)], sem)

    halo_rows = flats * tile + rows
    deep_rows = sum(ny * tile if d[2] == 0 else 2 * ny for d in deep_places(axes, ny)[0])

    barrier = pltpu.get_barrier_semaphore()

    greeted = [device(d) for d in reversed([*partners])]
    greeted += [member(d, 1, which) for group in (near_chips, wide_chips) for d in group if any(d.values()) for which in (0, 1)]
    greeted.append(member({}, 1, 1 - core))
    for to in greeted:
        pl.semaphore_signal(barrier, inc=1, device_id=to, device_id_type=MESH)

    loads = [
        pltpu.make_async_copy(o_in, planes_in.at[0], in_sem.at[0]),
        pltpu.make_async_copy(occ_in, occ_planes, in_sem.at[1]),
        pltpu.make_async_copy(v_in, planes_in.at[1], in_sem.at[0]),
    ]
    for load in loads:
        load.start()

    lane = lax.broadcasted_iota(jnp.int32, (nz, lanes), 1)
    level = lax.broadcasted_iota(jnp.int32, (nz, lanes), 0)
    spread = (
        lax.rem(lax.broadcasted_iota(jnp.int32, (slots, lanes), 1), slots)
        == lax.broadcasted_iota(jnp.int32, (slots, lanes), 0)
    ).astype(jnp.float32)

    def rows_of(planes):
        flat = planes.reshape(-1, slots)
        wide = jnp.dot(flat, spread, precision=lax.Precision.HIGHEST, preferred_element_type=jnp.float32)
        wide = wide.reshape(-1, nz, lanes)
        return jnp.sum(jnp.where((lane // slots == level)[None], wide, 0.0), axis=1)

    await_all(planes_in, in_sem.at[0])
    loads[1].wait()
    o_rows = rows_of(planes_in[0])
    v_rows = rows_of(planes_in[1])
    w_rows = rows_of(occ_planes[...].astype(jnp.float32))
    osend[...] = jnp.zeros_like(osend)
    kept[...] = jnp.zeros_like(kept)
    vsend[...] = jnp.zeros_like(vsend)
    fsend[...] = jnp.zeros_like(fsend)
    for x in range(nx):
        for y in range(ny):
            w = w_rows[x * ny + y : x * ny + y + 1]
            for c in range(3):
                i = (x * ny + y) * 3 + c
                r = c * nx + x
                kept[y, r : r + 1] = o_rows[i : i + 1]
                osend[y, r : r + 1] = jnp.where(w > 0.5, o_rows[i : i + 1], FAR)
                vsend[y, r : r + 1] = v_rows[i : i + 1] * w

    quarter = lanes // 4
    row_lane = lane[:1]

    tally[...] = jnp.broadcast_to(jnp.sum(w_rows, keepdims=True), (1, lanes))

    tile_lane = lax.broadcasted_iota(jnp.int32, (tile, lanes), 1)
    tile_row = lax.broadcasted_iota(jnp.int32, (tile, lanes), 0)
    slot_lane = lax.rem(tile_lane, slots)
    ends = [[slot_lane + (i if side == 0 else nz - 1 - i) * slots for i in range(2)] for side in range(2)]
    back = tile_row * slots + lax.rem(tile_lane, slots)

    def packed(block, side, depth=0):
        taken = jnp.take_along_axis(block, ends[side][depth], axis=1, mode="promise_in_bounds")
        return jnp.sum(jnp.where(tile_lane // slots == tile_row, taken, 0.0), axis=0, keepdims=True)

    def unpacked(row):
        wide = jnp.broadcast_to(row, (tile, lanes))
        return jnp.take_along_axis(wide, back, axis=1, mode="promise_in_bounds")

    for side in range(2):
        for y in range(ny):
            for depth in range(2):
                oedge[side, 2 * y + depth] = packed(osend[y], side, depth)
            vedge[side, y] = packed(vsend[y], side)

    pl.semaphore_wait(barrier, len(greeted))
    places, _, _ = deep_places(axes, ny)
    for d, at in reversed([*places.items()]):
        to = device(tuple(-x for x in d))
        if d[2] == 0:
            remote(osend, orecv.at[pl.ds(at, ny)], first_sem, o_recv_sem.at[d[1] % 3], to).start()
        else:
            src = oedge.at[0 if d[2] == 1 else 1]
            remote(src, oedges.at[pl.ds(at, 2 * ny)], first_sem, o_recv_sem.at[d[1] % 3], to).start()
    for copy in copies_of(vsend, vrecv, vedge, vedges, first_sem, v_sem):
        copy.start()

    def columns(send, recv, edges):
        found = {}
        for xi, a in enumerate(xs):
            for py, (b, yl) in enumerate(py_of):
                if (a, b) == (0, 0):
                    mid = send[yl]
                else:
                    need, at = partners[a, b, 0]
                    mid = recv[at + need.index(yl)]
                ends_of = []
                for c in (-1, 1):
                    need, at = partners[a, b, c]
                    ends_of.append(unpacked(edges[at + need.index(yl)]))
                below, above = ends_of
                found[xi, py, 1] = mid
                low = jnp.where(tile_lane >= lanes - slots, below, mid)
                found[xi, py, 0] = pltpu.roll(low, slots, 1)
                high = jnp.where(tile_lane < slots, above, mid)
                found[xi, py, 2] = pltpu.roll(high, lanes - slots, 1)
        return found

    cell = tile_lane // slots
    deep_x, deep_y = deep(gx, nx), deep(gy, ny)
    pairs = ny + 2

    def lay(xi, at, mid, below, above):
        below, above = ([unpacked(oedges[e + depth]) for depth in range(2)] for e in (below, above))
        low = jnp.where(tile_lane >= lanes - slots, below[0], mid)
        high = jnp.where(tile_lane < slots, above[0], mid)
        around[xi, at, 0] = pltpu.roll(low, slots, 1)
        around[xi, at, 1] = mid
        around[xi, at, 2] = pltpu.roll(high, lanes - slots, 1)
        bottom = jnp.where(cell == 0, below[1], jnp.where(cell == 1, below[0], pltpu.roll(mid, 2 * slots, 1)))
        top = jnp.where(cell == nz - 1, above[1], above[0])
        top = jnp.where(cell == nz - 3, pltpu.roll(mid, lanes - 2 * slots, 1), top)
        ends_of[xi, at] = jnp.where(cell < nz // 2, bottom, top)

    def await_row(b, level_tiles):
        await_rows(level_tiles * tile + 4 * ny * len(xs), o_recv_sem.at[b])

    def lay_beside(up):
        await_row(2 - up, ny * len(xs))
        for xi, a in enumerate(xs):
            above, below = ([places[a, canonical(gy, b), c] for c in (0, -1, 1)] for b in (1, -1))
            level_at, low_at, high_at = (m + up * (p - m) for p, m in zip(above, below))
            for yl in range(2):
                layer = (ny - 2) * (1 - up) + yl
                lay(
                    xi, yl + up * (ny + 2), orecv[level_at + layer], low_at + 2 * layer, high_at + 2 * layer
                )

    def lay_packed():
        for xi in range(len(xs)):
            for dy in range(3):
                for dz in range(3):
                    centre = jnp.where(lax.rem(cell, 2) == 0, dz, nz - 3 + dz)
                    source = centre * slots + slot_lane
                    gathered = jnp.zeros((tile, lanes), jnp.float32)
                    for t in range(pairs):
                        taken = jnp.take_along_axis(ends_of[xi, t + dy], source, axis=1, mode="promise_in_bounds")
                        gathered = jnp.where(cell // 2 == t, taken, gathered)
                    around[xi, pairs + 2 + dy, dz] = gathered

    lane_id = lax.broadcasted_iota(jnp.int32, (slots, lanes), 1)
    slot_id = lax.broadcasted_iota(jnp.int32, (slots, lanes), 0)
    pick = (lane_id // slots) * slots + slot_id
    itself = lax.rem(lane_id, slots) == slot_id

    def nearby(py):
        for px, (a, xl) in enumerate(px_of):
            for dz in range(3):
                for c in range(3):
                    r = c * nx + xl
                    row = jnp.broadcast_to(ostate[xs.index(a), py, dz, r : r + 1], (slots, lanes))
                    near[px, py, dz, c] = jnp.take_along_axis(row, pick, axis=1, mode="promise_in_bounds")

    half = 0.5 * TIME_STEP
    reach2 = CUTOFF * CUTOFF

    def terms(squared):
        inv = lax.rsqrt(squared)
        inv2 = inv * inv
        inv6 = inv2 * inv2 * inv2
        inv12 = inv6 * inv6
        bond = inv12 - inv6
        return inv, bond, inv * (bond + inv12)

    _, _, edge = terms(jnp.full((slots, lanes), reach2, jnp.float32))
    pair_count = 27.0 * slots

    def pair_sums(mine, near_of):
        force = [jnp.zeros((slots, lanes), jnp.float32) for _ in range(3)]
        bonds, reach = (jnp.zeros((slots, lanes), jnp.float32) for _ in range(2))
        for shift in itertools.product((-1, 0, 1), repeat=3):
            apart = [near_of(shift, c) - (mine[c] - shift[c] * CELL_SIDE) for c in range(3)]
            squared = apart[0] * apart[0] + apart[1] * apart[1] + apart[2] * apart[2]
            if shift == (0, 0, 0):
                squared = jnp.where(itself, reach2, squared)
            squared = jnp.minimum(squared, reach2)
            inv, bond, push = terms(squared)
            pull = inv * (edge - push)
            for c in range(3):
                force[c] = force[c] + pull * apart[c]
            bonds = bonds + bond
            reach = reach + squared * inv
        return [24.0 * jnp.sum(f, axis=0, keepdims=True) for f in force], bonds, reach

    def first_row(i, _):
        centre = i + 1 + 2 * (i // pairs)
        for px, (a, xl) in enumerate(deep_x):
            for dy in range(3):
                for dz in range(3):
                    for c in range(3):
                        r = c * nx + xl
                        row = jnp.broadcast_to(around[xs.index(a), centre - 1 + dy, dz, r : r + 1], (slots, lanes))
                        first_near[px, dy, dz, c] = jnp.take_along_axis(row, pick, axis=1, mode="promise_in_bounds")
        for px, (a, xl) in enumerate(px_of):
            block = around[xs.index(a), centre, 1]
            mine = [block[c * nx + xl : c * nx + xl + 1] for c in range(3)]
            force, _, _ = pair_sums(
                mine, lambda shift, c: first_near[px + 1 + shift[0], 1 + shift[1], 1 + shift[2], c]
            )
            for c in range(3):
                r = c * nx + xl
                first_force[xs.index(a), i, r : r + 1] = jnp.where(mine[0] < 0.5 * FAR, force[c], 0.0)
        return 0

    first_force[...] = jnp.zeros_like(first_force)
    await_row(0, ny * (len(xs) - 1))
    for xi, a in enumerate(xs):
        for yl in range(ny):
            mid = osend[yl] if a == 0 else orecv[places[a, 0, 0] + yl]
            lay(xi, yl + 2, mid, places[a, 0, -1] + 2 * yl, places[a, 0, 1] + 2 * yl)
    lay_beside(1 - core)
    near_rows = pairs // 2
    lax.fori_loop(0, near_rows, lambda t, _: first_row(t + near_rows * (1 - core), 0), 0)
    lay_beside(core)
    lay_packed()
    last = pairs - near_rows
    lax.fori_loop(
        0, last + 1, lambda t, _: first_row((t + near_rows * core) * (1 - t // last) + pairs * (t // last), 0), 0
    )

    await_rows(halo_rows, v_sem)
    first_v = columns(vsend, vrecv, vedges)
    for xi in range(len(xs)):
        outer = first_force[xi, pairs]
        for py in range(pairs):
            mid = first_force[xi, py]
            low = jnp.where(tile_lane < slots, pltpu.roll(outer, (lanes - 2 * py * slots) % lanes, 1), pltpu.roll(mid, slots, 1))
            high = jnp.where(
                tile_lane >= lanes - slots,
                pltpu.roll(outer, lanes - 2 * (py + 1) * slots, 1),
                pltpu.roll(mid, lanes - slots, 1),
            )
            for dz, f in enumerate((low, mid, high)):
                v = first_v[xi, py, dz] + half * f
                vstate[xi, py, dz] = v
                ostate[xi, py, dz] = around[xi, py + 1, dz] + TIME_STEP * v

    def step(k, _):
        p = lax.rem(k, 2)
        for py in range(ny + 2):
            nearby(py)

        energy_rows = jnp.zeros((1, lanes), jnp.float32)
        for x in range(nx):
            for y in range(ny):
                block = ostate[0, y + 1, 1]
                mine = [block[c * nx + x : c * nx + x + 1] for c in range(3)]
                occupied = mine[0] < 0.5 * FAR
                force, bonds, reach = pair_sums(
                    mine, lambda shift, c: near[x + 1 + shift[0], y + 1 + shift[1], 1 + shift[2], c]
                )
                for c in range(3):
                    r = c * nx + x
                    fsend[p, y, r : r + 1] = jnp.where(occupied, force[c], 0.0)
                energy = 4.0 * bonds + FORCE_EDGE * reach
                total = jnp.sum(energy, axis=0, keepdims=True)
                total = total - pair_count * (ENERGY_EDGE + CUTOFF * FORCE_EDGE)
                energy_rows = energy_rows + jnp.where(occupied, total, 0.0)

        kinetic = jnp.zeros((tile, lanes), jnp.float32)
        for y in range(ny):
            v = vstate[0, y + 1, 1] + half * fsend[p, y]
            kinetic = kinetic + v * v
        kinetic = jnp.sum(jnp.sum(kinetic, axis=0, keepdims=True), axis=1, keepdims=True)
        potential = jnp.sum(energy_rows, axis=1, keepdims=True)
        row = jnp.where(
            row_lane < 2 * quarter, 0.5 * kinetic, jnp.where(row_lane < 3 * quarter, 0.5 * potential, tally[...])
        )
        row_sum[...] = row
        at = index_in(NEAR) * 2 + core
        for d in near_chips:
            if any(d.values()):
                remote(row_sum, near_sums.at[p, at], sum_send, near_recv.at[p], member(d, -1, 1)).start()

        @pl.when(follows)
        def _():
            remote(row_sum, near_sums.at[p, at], sum_send, near_recv.at[p], member({}, 1, 1)).start()

        @pl.when(leads)
        def _():
            near_sums[p, at] = row

        @pl.when(k < STEPS)
        def _():
            for side in range(2):
                for y in range(ny):
                    fedge[p, side, y] = packed(fsend[p, y], side)
            for copy in copies_of(
                fsend.at[p], frecv.at[p], fedge.at[p], fedges.at[p], f_send_sem, f_recv_sem.at[p]
            ):
                copy.start()

        def total_of(ref, n):
            parts = [ref[p, i] for i in range(n)]
            while len(parts) > 1:
                parts = [sum(parts[i + 1 : i + 2], parts[i]) for i in range(0, len(parts), 2)]
            return parts[0]

        n_near, n_wide = len(near_chips), len(wide_chips)

        @pl.when(leads)
        def _():
            await_all(near_sums.at[p, pl.ds(0, 2 * n_near - 1)], near_recv.at[p])
            row = total_of(near_sums, 2 * n_near)
            chip_sum[...] = row
            at = index_in(WIDE)
            for d in wide_chips:
                for which in (0, 1):
                    if which == 0 or any(d.values()):
                        remote(
                            chip_sum, wide_sums.at[p, at], sum_send, wide_recv.at[p], member(d, -1, which)
                        ).start()
            wide_sums[p, at] = row

        @pl.when(k < STEPS)
        def _():
            await_rows(halo_rows, f_recv_sem.at[p])
            await_rows(halo_rows, f_send_sem)
            for (xi, py, dz), f in columns(fsend.at[p], frecv.at[p], fedges.at[p]).items():
                vstate[xi, py, dz] = vstate[xi, py, dz] + half * f
                held[xi, py, dz] = half * f

        @pl.when(leads)
        def _():
            await_all(wide_sums.at[p, pl.ds(0, n_wide - 1)], wide_recv.at[p])

        @pl.when(follows)
        def _():
            await_rows(n_near, sum_send)
            await_all(wide_sums.at[p], wide_recv.at[p])

        row = total_of(wide_sums, n_wide)

        def across(part):
            return jnp.full((1, lanes), row[0, part * quarter], jnp.float32)

        vigor, potential, count = across(0), across(2), across(3)
        square = (1.0 - BATH_STRENGTH) + (BATH_STRENGTH * GOAL_WARMTH * 1.5) * count / vigor
        which = lax.broadcasted_iota(jnp.int32, (2, lanes), 1)
        record = jnp.concatenate([potential, square * vigor], axis=0) / slot_total
        history[...] = jnp.where(which == k - 1, record, history[...])

        @pl.when(leads)
        def _():
            await_rows(n_near + 2 * n_wide - 2, sum_send)

        lam = jnp.sqrt(square)

        @pl.when(k < STEPS)
        def _():
            for xi in range(len(xs)):
                for py in range(ny + 2):
                    for dz in range(3):
                        v = vstate[xi, py, dz] * lam + held[xi, py, dz]
                        vstate[xi, py, dz] = v
                        ostate[xi, py, dz] = ostate[xi, py, dz] + TIME_STEP * v

        @pl.when(k == STEPS)
        def _():
            for y in range(ny):
                here = ostate[0, y + 1, 1]
                result[y] = jnp.where(here < 0.5 * FAR, here, kept[y])
                result[ny + y] = (vstate[0, y + 1, 1] + half * fsend[p, y]) * lam
                result[2 * ny + y] = fsend[p, y]
            result[3 * ny, 0:2] = history[...]

        return 0

    history[...] = jnp.zeros_like(history)
    lax.fori_loop(1, STEPS + 1, step, 0)
    await_rows(deep_rows + halo_rows, first_sem)


def unpack(shape, result, o_out, v_out, f_out, h_out):
    nx, ny, nz, slots = shape
    lanes = nz * slots
    at = lax.broadcasted_iota(jnp.int32, (nz, lanes), 0) * slots + lax.rem(
        lax.broadcasted_iota(jnp.int32, (nz, lanes), 1), slots
    )
    for i, ref in enumerate((o_out, v_out, f_out)):
        for y in range(ny):
            for x in range(nx):
                for c in range(3):
                    r = c * nx + x
                    row = jnp.broadcast_to(result[i * ny + y, r : r + 1], (nz, lanes))
                    ref[x, y, c] = jnp.take_along_axis(row, at, axis=1, mode="promise_in_bounds")[:, :slots]
    h_out[...] = result[3 * ny, 0:2, :STEPS]


def shards(axes, offsets, velocities, occupied):
    nx, ny, nz, slots = occupied.shape
    lanes = nz * slots
    tile = lanes // slots
    assert axes[2] > 2 and tile >= 3 * nx and min(nx, ny) >= 2 and ny % 2 == 0 and nz == 2 * (ny + 2)
    _, flats, rows = partners_of(axes, ny)
    _, deep_flats, deep_rows = deep_places(axes, ny)
    nxo = len(offsets_of(axes[0]))
    n_near, n_wide = (len(chips_of(axes, group)) for group in (NEAR, WIDE))
    f32 = jnp.float32
    plane = jax.ShapeDtypeStruct((nx, ny, 3, nz, slots), f32)
    vmem = pl.BlockSpec(memory_space=pltpu.VMEM)
    dma = pltpu.SemaphoreType.DMA
    state = pltpu.VMEM((nxo, ny + 2, 3, tile, lanes), f32)
    halo = [
        pltpu.VMEM((ny, tile, lanes), f32),
        pltpu.VMEM((flats, tile, lanes), f32),
        pltpu.VMEM((2, ny, 1, lanes), f32),
        pltpu.VMEM((rows, 1, lanes), f32),
    ]
    result = pl.pallas_call(
        functools.partial(kernel, axes, (nx, ny, nz, slots)),
        name="verlet",
        out_shape=pltpu.VMEM((3 * ny + 1, tile, lanes), f32),
        in_specs=[pl.BlockSpec(memory_space=pltpu.HBM)] * 3,
        out_specs=vmem,
        scratch_shapes=[
            pltpu.VMEM((2, nx, ny, 3, nz, slots), f32),
            pltpu.VMEM((ny, tile, lanes), f32),
            state,
            state,
            state,
            pltpu.VMEM((nx + 2, ny + 2, 3, 3, slots, lanes), f32),
            pltpu.VMEM((nxo, ny + 7, 3, tile, lanes), f32),
            pltpu.VMEM((nxo, ny + 4, tile, lanes), f32),
            pltpu.VMEM((nx + 4, 3, 3, 3, slots, lanes), f32),
            pltpu.VMEM((nxo, ny + 3, tile, lanes), f32),
            pltpu.VMEM((ny, tile, lanes), f32),
            pltpu.VMEM((deep_flats, tile, lanes), f32),
            pltpu.VMEM((2, 2 * ny, 1, lanes), f32),
            pltpu.VMEM((deep_rows, 1, lanes), f32),
            *halo,
            pltpu.VMEM((nx, ny, nz, slots), jnp.int32),
            pltpu.VMEM((2, ny, tile, lanes), f32),
            pltpu.VMEM((2, flats, tile, lanes), f32),
            pltpu.VMEM((2, 2, ny, 1, lanes), f32),
            pltpu.VMEM((2, rows, 1, lanes), f32),
            pltpu.VMEM((1, lanes), f32),
            pltpu.VMEM((2, lanes), f32),
            pltpu.VMEM((1, lanes), f32),
            pltpu.VMEM((2, 2 * n_near, 1, lanes), f32),
            pltpu.VMEM((1, lanes), f32),
            pltpu.VMEM((2, n_wide, 1, lanes), f32),
            pltpu.VMEM((deep_flats * tile + deep_rows + flats * tile + rows, 1, lanes), f32),
            dma((2,)),
            dma,
            dma((3,)),
            dma,
            dma,
            dma((2,)),
            dma,
            dma((2,)),
            dma((2,)),
        ],
        compiler_params=pltpu.CompilerParams(
            collective_id=0, has_side_effects=True, vmem_limit_bytes=VERLET_VMEM
        ),
    )(
        jnp.transpose(offsets, (0, 1, 4, 2, 3)),
        jnp.transpose(velocities, (0, 1, 4, 2, 3)),
        occupied,
    )
    o, v, f, h = pl.pallas_call(
        functools.partial(unpack, (nx, ny, nz, slots)),
        name="unpack",
        out_shape=[plane, plane, plane, jax.ShapeDtypeStruct((2, STEPS), f32)],
        in_specs=[vmem],
        out_specs=[vmem] * 4,
        compiler_params=pltpu.CompilerParams(vmem_limit_bytes=UNPACK_VMEM),
    )(result)
    back = (0, 1, 3, 4, 2)
    return (jnp.transpose(o, back), jnp.transpose(v, back), jnp.transpose(f, back), h.T)


def solution(mesh):
    axes = tuple(mesh.shape[a] for a in ("gx", "gy", "gz"))
    in_specs = (
        P("gx", "gy", "gz", None, None),
        P("gx", "gy", "gz", None, None),
        P("gx", "gy", "gz", None),
    )
    out_specs = (
        P("gx", "gy", "gz", None, None),
        P("gx", "gy", "gz", None, None),
        P("gx", "gy", "gz", None, None),
        P(),
    )
    return jax.shard_map(
        functools.partial(shards, axes), mesh=mesh, in_specs=in_specs, out_specs=out_specs, check_vma=False
    )
```

```python
import functools
import itertools

import jax
import jax.numpy as jnp
from jax import lax
from jax.experimental import pallas as pl
from jax.experimental.pallas import tpu as pltpu
from jax.sharding import PartitionSpec as P

MESH = pl.DeviceIdType.MESH
STEPS = 4
CUTOFF = 2.5
CELL_SIDE = 2.6
TIME_STEP = 0.005
BATH_STRENGTH = 0.25
GOAL_WARMTH = 0.8
FORCE_EDGE = 24.0 * (2.0 * CUTOFF ** (-13) - CUTOFF ** (-7))
ENERGY_EDGE = 4.0 * (CUTOFF ** (-12) - CUTOFF ** (-6))
FAR = 32.0
VERLET_VMEM = 60 * 1024 * 1024
UNPACK_VMEM = 4 * 1024 * 1024


NEAR = ("xl", "xh", "y")
WIDE = ("z",)


def parts_of(axes):
    gx, gy, gz = axes
    return {"xl": gx // 4, "y": 4, "xh": gy // 2, "z": gz}


def chips_of(axes, group):
    sizes = parts_of(axes)

    def hops(d):
        return sum(min(o, sizes[a] - o) for a, o in d.items())

    every = itertools.product(*[range(sizes[a]) for a in group])
    return sorted((dict(zip(group, d)) for d in every), key=lambda d: -hops(d))


def offsets_of(size):
    return [0] if size == 1 else [0, 1] if size == 2 else [0, 1, -1]


def canonical(size, off):
    return 0 if size == 1 else off % 2 if size == 2 else off


def padded(size, n):
    return [(canonical(size, -1), n - 1)] + [(0, i) for i in range(n)] + [(canonical(size, 1), 0)]


def deep(size, n):
    low, high = canonical(size, -1), canonical(size, 1)
    return [(low, n - 2), (low, n - 1)] + [(0, i) for i in range(n)] + [(high, 0), (high, 1)]


def deep_places(axes, ny):
    flat, rows, found = 0, 0, {}
    for d in itertools.product(*[offsets_of(n) for n in axes]):
        if d == (0, 0, 0):
            continue
        if d[2] == 0:
            found[d] = flat
            flat += ny
        else:
            found[d] = rows
            rows += 2 * ny
    return found, flat, rows


def partners_of(axes, ny):
    every = itertools.product(*[offsets_of(n) for n in axes])
    flat, rows, found = 0, 0, {}
    for d in every:
        if d == (0, 0, 0):
            continue
        need = sorted({yl for off, yl in padded(axes[1], ny) if off == d[1]})
        if d[2] == 0:
            found[d] = need, flat
            flat += len(need)
        else:
            found[d] = need, rows
            rows += len(need)
    return found, flat, rows


def kernel(
    axes, shape, o_in, v_in, occ_in, result,
    planes_in, kept, ostate, vstate, held, near, around, ends_of, first_near, first_force, osend, orecv, oedge, oedges, vsend, vrecv, vedge, vedges,
    occ_planes, fsend, frecv, fedge, fedges, tally, history, scale, row_sum, near_sums, chip_sum, wide_sums, measure,
    in_sem, first_sem, o_recv_sem, v_sem, f_send_sem, f_recv_sem, sum_send, near_recv, wide_recv,
):
    gx, gy, gz = axes
    nx, ny, nz, slots = shape
    lanes = nz * slots
    tile = fsend.shape[2]
    slot_total = float(gx * gy * gz * nx * ny * lanes)
    me = [lax.axis_index(a) for a in ("gx", "gy", "gz")]
    sizes = parts_of(axes)
    place = {"xl": me[0] // 4, "y": lax.rem(me[0], 4), "xh": me[1] // 2, "z": me[2]}
    core = lax.rem(me[1], 2)
    leads = core == 1
    follows = core == 0
    near_chips, wide_chips = chips_of(axes, NEAR), chips_of(axes, WIDE)

    turned = [[lax.rem(me[i] + j, n) for j in range(n)] for i, n in enumerate(axes)]

    def device(d):
        return tuple(turned[i][d[i] % axes[i]] for i in range(3))

    def member(d, sign, which):
        at = dict(place)
        for a, o in d.items():
            if o:
                at[a] = lax.rem(at[a] + (o if sign > 0 else sizes[a] - o), sizes[a])
        return (at["xl"] * 4 + at["y"], at["xh"] * 2 + which, at["z"])

    def index_in(group):
        at = 0
        for a in group:
            at = at * sizes[a] + place[a]
        return at

    px_of, py_of = padded(gx, nx), padded(gy, ny)
    xs = offsets_of(gx)
    partners, flats, rows = partners_of(axes, ny)

    def remote(src, dst, send_sem, recv_sem, to):
        return pltpu.make_async_remote_copy(
            src_ref=src, dst_ref=dst, send_sem=send_sem, recv_sem=recv_sem, device_id=to, device_id_type=MESH
        )

    def copies_of(send, recv, edge, edges, send_sem, recv_sem):
        copies = []
        for d, (need, at) in reversed([*partners.items()]):
            where = pl.ds(need[0], len(need))
            to = device(tuple(-x for x in d))
            if d[2] == 0:
                copies.append(remote(send.at[where], recv.at[pl.ds(at, len(need))], send_sem, recv_sem, to))
            else:
                src = edge.at[0 if d[2] == 1 else 1, where]
                copies.append(remote(src, edges.at[pl.ds(at, len(need))], send_sem, recv_sem, to))
        return copies

    def await_all(ref, sem):
        pltpu.make_async_copy(ref, ref, sem).wait()

    def await_rows(n, sem):
        await_all(measure.at[pl.ds(0, n)], sem)

    halo_rows = flats * tile + rows
    deep_rows = sum(ny * tile if d[2] == 0 else 2 * ny for d in deep_places(axes, ny)[0])

    barrier = pltpu.get_barrier_semaphore()

    greeted = [device(d) for d in reversed([*partners])]
    greeted += [member(d, 1, which) for group in (near_chips, wide_chips) for d in group if any(d.values()) for which in (0, 1)]
    greeted.append(member({}, 1, 1 - core))
    for to in greeted:
        pl.semaphore_signal(barrier, inc=1, device_id=to, device_id_type=MESH)

    loads = [
        pltpu.make_async_copy(o_in, planes_in.at[0], in_sem.at[0]),
        pltpu.make_async_copy(occ_in, occ_planes, in_sem.at[1]),
        pltpu.make_async_copy(v_in, planes_in.at[1], in_sem.at[0]),
    ]
    for load in loads:
        load.start()

    lane = lax.broadcasted_iota(jnp.int32, (nz, lanes), 1)
    level = lax.broadcasted_iota(jnp.int32, (nz, lanes), 0)
    spread = (
        lax.rem(lax.broadcasted_iota(jnp.int32, (slots, lanes), 1), slots)
        == lax.broadcasted_iota(jnp.int32, (slots, lanes), 0)
    ).astype(jnp.float32)

    def rows_of(planes):
        flat = planes.reshape(-1, slots)
        wide = jnp.dot(flat, spread, precision=lax.Precision.HIGHEST, preferred_element_type=jnp.float32)
        wide = wide.reshape(-1, nz, lanes)
        return jnp.sum(jnp.where((lane // slots == level)[None], wide, 0.0), axis=1)

    await_all(planes_in, in_sem.at[0])
    loads[1].wait()
    o_rows = rows_of(planes_in[0])
    v_rows = rows_of(planes_in[1])
    w_rows = rows_of(occ_planes[...].astype(jnp.float32))
    osend[...] = jnp.zeros_like(osend)
    kept[...] = jnp.zeros_like(kept)
    vsend[...] = jnp.zeros_like(vsend)
    fsend[...] = jnp.zeros_like(fsend)
    for x in range(nx):
        for y in range(ny):
            w = w_rows[x * ny + y : x * ny + y + 1]
            for c in range(3):
                i = (x * ny + y) * 3 + c
                r = c * nx + x
                kept[y, r : r + 1] = o_rows[i : i + 1]
                osend[y, r : r + 1] = jnp.where(w > 0.5, o_rows[i : i + 1], FAR)
                vsend[y, r : r + 1] = v_rows[i : i + 1] * w

    quarter = lanes // 4
    row_lane = lane[:1]

    tally[...] = jnp.broadcast_to(jnp.sum(w_rows, keepdims=True), (1, lanes))

    tile_lane = lax.broadcasted_iota(jnp.int32, (tile, lanes), 1)
    tile_row = lax.broadcasted_iota(jnp.int32, (tile, lanes), 0)
    slot_lane = lax.rem(tile_lane, slots)
    ends = [[slot_lane + (i if side == 0 else nz - 1 - i) * slots for i in range(2)] for side in range(2)]
    back = tile_row * slots + lax.rem(tile_lane, slots)

    def packed(block, side, depth=0):
        taken = jnp.take_along_axis(block, ends[side][depth], axis=1, mode="promise_in_bounds")
        return jnp.sum(jnp.where(tile_lane // slots == tile_row, taken, 0.0), axis=0, keepdims=True)

    def unpacked(row):
        wide = jnp.broadcast_to(row, (tile, lanes))
        return jnp.take_along_axis(wide, back, axis=1, mode="promise_in_bounds")

    for side in range(2):
        for y in range(ny):
            for depth in range(2):
                oedge[side, 2 * y + depth] = packed(osend[y], side, depth)
            vedge[side, y] = packed(vsend[y], side)

    pl.semaphore_wait(barrier, len(greeted))
    places, _, _ = deep_places(axes, ny)
    for d, at in reversed([*places.items()]):
        to = device(tuple(-x for x in d))
        if d[2] == 0:
            remote(osend, orecv.at[pl.ds(at, ny)], first_sem, o_recv_sem.at[d[1] % 3], to).start()
        else:
            src = oedge.at[0 if d[2] == 1 else 1]
            remote(src, oedges.at[pl.ds(at, 2 * ny)], first_sem, o_recv_sem.at[d[1] % 3], to).start()
    for copy in copies_of(vsend, vrecv, vedge, vedges, first_sem, v_sem):
        copy.start()

    def columns(send, recv, edges):
        found = {}
        for xi, a in enumerate(xs):
            for py, (b, yl) in enumerate(py_of):
                if (a, b) == (0, 0):
                    mid = send[yl]
                else:
                    need, at = partners[a, b, 0]
                    mid = recv[at + need.index(yl)]
                ends_of = []
                for c in (-1, 1):
                    need, at = partners[a, b, c]
                    ends_of.append(unpacked(edges[at + need.index(yl)]))
                below, above = ends_of
                found[xi, py, 1] = mid
                low = jnp.where(tile_lane >= lanes - slots, below, mid)
                found[xi, py, 0] = pltpu.roll(low, slots, 1)
                high = jnp.where(tile_lane < slots, above, mid)
                found[xi, py, 2] = pltpu.roll(high, lanes - slots, 1)
        return found

    cell = tile_lane // slots
    deep_x, deep_y = deep(gx, nx), deep(gy, ny)
    pairs = ny + 2

    def lay(xi, at, mid, below, above):
        below, above = ([unpacked(oedges[e + depth]) for depth in range(2)] for e in (below, above))
        low = jnp.where(tile_lane >= lanes - slots, below[0], mid)
        high = jnp.where(tile_lane < slots, above[0], mid)
        around[xi, at, 0] = pltpu.roll(low, slots, 1)
        around[xi, at, 1] = mid
        around[xi, at, 2] = pltpu.roll(high, lanes - slots, 1)
        bottom = jnp.where(cell == 0, below[1], jnp.where(cell == 1, below[0], pltpu.roll(mid, 2 * slots, 1)))
        top = jnp.where(cell == nz - 1, above[1], above[0])
        top = jnp.where(cell == nz - 3, pltpu.roll(mid, lanes - 2 * slots, 1), top)
        ends_of[xi, at] = jnp.where(cell < nz // 2, bottom, top)

    def await_row(b, level_tiles):
        await_rows(level_tiles * tile + 4 * ny * len(xs), o_recv_sem.at[b])

    def lay_beside(up):
        await_row(2 - up, ny * len(xs))
        for xi, a in enumerate(xs):
            above, below = ([places[a, canonical(gy, b), c] for c in (0, -1, 1)] for b in (1, -1))
            level_at, low_at, high_at = (m + up * (p - m) for p, m in zip(above, below))
            for yl in range(2):
                layer = (ny - 2) * (1 - up) + yl
                lay(
                    xi, yl + up * (ny + 2), orecv[level_at + layer], low_at + 2 * layer, high_at + 2 * layer
                )

    def lay_packed():
        for xi in range(len(xs)):
            for dy in range(3):
                for dz in range(3):
                    centre = jnp.where(lax.rem(cell, 2) == 0, dz, nz - 3 + dz)
                    source = centre * slots + slot_lane
                    gathered = jnp.zeros((tile, lanes), jnp.float32)
                    for t in range(pairs):
                        taken = jnp.take_along_axis(ends_of[xi, t + dy], source, axis=1, mode="promise_in_bounds")
                        gathered = jnp.where(cell // 2 == t, taken, gathered)
                    around[xi, pairs + 2 + dy, dz] = gathered

    lane_id = lax.broadcasted_iota(jnp.int32, (slots, lanes), 1)
    slot_id = lax.broadcasted_iota(jnp.int32, (slots, lanes), 0)
    pick = (lane_id // slots) * slots + slot_id
    itself = lax.rem(lane_id, slots) == slot_id

    def nearby(py):
        for px, (a, xl) in enumerate(px_of):
            for dz in range(3):
                for c in range(3):
                    r = c * nx + xl
                    row = jnp.broadcast_to(ostate[xs.index(a), py, dz, r : r + 1], (slots, lanes))
                    near[px, py, dz, c] = jnp.take_along_axis(row, pick, axis=1, mode="promise_in_bounds")

    half = 0.5 * TIME_STEP
    reach2 = CUTOFF * CUTOFF

    def terms(squared):
        inv = lax.rsqrt(squared)
        inv2 = inv * inv
        inv6 = inv2 * inv2 * inv2
        inv12 = inv6 * inv6
        bond = inv12 - inv6
        return inv, bond, inv * (bond + inv12)

    _, _, edge = terms(jnp.full((slots, lanes), reach2, jnp.float32))
    pair_count = 27.0 * slots

    def pair_sums(mine, near_of):
        force = [jnp.zeros((slots, lanes), jnp.float32) for _ in range(3)]
        bonds, reach = (jnp.zeros((slots, lanes), jnp.float32) for _ in range(2))
        for shift in itertools.product((-1, 0, 1), repeat=3):
            apart = [near_of(shift, c) - (mine[c] - shift[c] * CELL_SIDE) for c in range(3)]
            squared = apart[0] * apart[0] + apart[1] * apart[1] + apart[2] * apart[2]
            if shift == (0, 0, 0):
                squared = jnp.where(itself, reach2, squared)
            squared = jnp.minimum(squared, reach2)
            inv, bond, push = terms(squared)
            pull = inv * (edge - push)
            for c in range(3):
                force[c] = force[c] + pull * apart[c]
            bonds = bonds + bond
            reach = reach + squared * inv
        return [24.0 * jnp.sum(f, axis=0, keepdims=True) for f in force], bonds, reach

    def first_row(i, _):
        centre = i + 1 + 2 * (i // pairs)
        for px, (a, xl) in enumerate(deep_x):
            for dy in range(3):
                for dz in range(3):
                    for c in range(3):
                        r = c * nx + xl
                        row = jnp.broadcast_to(around[xs.index(a), centre - 1 + dy, dz, r : r + 1], (slots, lanes))
                        first_near[px, dy, dz, c] = jnp.take_along_axis(row, pick, axis=1, mode="promise_in_bounds")
        for px, (a, xl) in enumerate(px_of):
            block = around[xs.index(a), centre, 1]
            mine = [block[c * nx + xl : c * nx + xl + 1] for c in range(3)]
            force, _, _ = pair_sums(
                mine, lambda shift, c: first_near[px + 1 + shift[0], 1 + shift[1], 1 + shift[2], c]
            )
            for c in range(3):
                r = c * nx + xl
                first_force[xs.index(a), i, r : r + 1] = jnp.where(mine[0] < 0.5 * FAR, force[c], 0.0)
        return 0

    first_force[...] = jnp.zeros_like(first_force)
    await_row(0, ny * (len(xs) - 1))
    for xi, a in enumerate(xs):
        for yl in range(ny):
            mid = osend[yl] if a == 0 else orecv[places[a, 0, 0] + yl]
            lay(xi, yl + 2, mid, places[a, 0, -1] + 2 * yl, places[a, 0, 1] + 2 * yl)
    lay_beside(1 - core)
    near_rows = pairs // 2
    lax.fori_loop(0, near_rows, lambda t, _: first_row(t + near_rows * (1 - core), 0), 0)
    lay_beside(core)
    lay_packed()
    last = pairs - near_rows
    lax.fori_loop(
        0, last + 1, lambda t, _: first_row((t + near_rows * core) * (1 - t // last) + pairs * (t // last), 0), 0
    )

    await_rows(halo_rows, v_sem)
    first_v = columns(vsend, vrecv, vedges)
    for xi in range(len(xs)):
        outer = first_force[xi, pairs]
        for py in range(pairs):
            mid = first_force[xi, py]
            low = jnp.where(tile_lane < slots, pltpu.roll(outer, (lanes - 2 * py * slots) % lanes, 1), pltpu.roll(mid, slots, 1))
            high = jnp.where(
                tile_lane >= lanes - slots,
                pltpu.roll(outer, lanes - 2 * (py + 1) * slots, 1),
                pltpu.roll(mid, lanes - slots, 1),
            )
            for dz, f in enumerate((low, mid, high)):
                vstate[xi, py, dz] = first_v[xi, py, dz]
                held[xi, py, dz] = half * f
                ostate[xi, py, dz] = around[xi, py + 1, dz]

    def step(k, _):
        p = lax.rem(k, 2)
        lam = scale[...]
        for xi in range(len(xs)):
            for py in range(ny + 2):
                for dz in range(3):
                    v = vstate[xi, py, dz] * lam + held[xi, py, dz]
                    vstate[xi, py, dz] = v
                    ostate[xi, py, dz] = ostate[xi, py, dz] + TIME_STEP * v
        for py in range(ny + 2):
            nearby(py)

        energy_rows = jnp.zeros((1, lanes), jnp.float32)
        for x in range(nx):
            for y in range(ny):
                block = ostate[0, y + 1, 1]
                mine = [block[c * nx + x : c * nx + x + 1] for c in range(3)]
                occupied = mine[0] < 0.5 * FAR
                force, bonds, reach = pair_sums(
                    mine, lambda shift, c: near[x + 1 + shift[0], y + 1 + shift[1], 1 + shift[2], c]
                )
                for c in range(3):
                    r = c * nx + x
                    fsend[p, y, r : r + 1] = jnp.where(occupied, force[c], 0.0)
                energy = 4.0 * bonds + FORCE_EDGE * reach
                total = jnp.sum(energy, axis=0, keepdims=True)
                total = total - pair_count * (ENERGY_EDGE + CUTOFF * FORCE_EDGE)
                energy_rows = energy_rows + jnp.where(occupied, total, 0.0)

        kinetic = jnp.zeros((tile, lanes), jnp.float32)
        for y in range(ny):
            v = vstate[0, y + 1, 1] + half * fsend[p, y]
            kinetic = kinetic + v * v
        kinetic = jnp.sum(jnp.sum(kinetic, axis=0, keepdims=True), axis=1, keepdims=True)
        potential = jnp.sum(energy_rows, axis=1, keepdims=True)
        row = jnp.where(
            row_lane < 2 * quarter, 0.5 * kinetic, jnp.where(row_lane < 3 * quarter, 0.5 * potential, tally[...])
        )
        row_sum[...] = row
        at = index_in(NEAR) * 2 + core
        for d in near_chips:
            if any(d.values()):
                remote(row_sum, near_sums.at[p, at], sum_send, near_recv.at[p], member(d, -1, 1)).start()

        @pl.when(follows)
        def _():
            remote(row_sum, near_sums.at[p, at], sum_send, near_recv.at[p], member({}, 1, 1)).start()

        @pl.when(leads)
        def _():
            near_sums[p, at] = row

        @pl.when(k < STEPS)
        def _():
            for side in range(2):
                for y in range(ny):
                    fedge[p, side, y] = packed(fsend[p, y], side)
            for copy in copies_of(
                fsend.at[p], frecv.at[p], fedge.at[p], fedges.at[p], f_send_sem, f_recv_sem.at[p]
            ):
                copy.start()

        def total_of(ref, n):
            parts = [ref[p, i] for i in range(n)]
            while len(parts) > 1:
                parts = [sum(parts[i + 1 : i + 2], parts[i]) for i in range(0, len(parts), 2)]
            return parts[0]

        n_near, n_wide = len(near_chips), len(wide_chips)

        @pl.when(leads)
        def _():
            await_all(near_sums.at[p, pl.ds(0, 2 * n_near - 1)], near_recv.at[p])
            row = total_of(near_sums, 2 * n_near)
            chip_sum[...] = row
            at = index_in(WIDE)
            for d in wide_chips:
                for which in (0, 1):
                    if which == 0 or any(d.values()):
                        remote(
                            chip_sum, wide_sums.at[p, at], sum_send, wide_recv.at[p], member(d, -1, which)
                        ).start()
            wide_sums[p, at] = row

        @pl.when(k < STEPS)
        def _():
            await_rows(halo_rows, f_recv_sem.at[p])
            await_rows(halo_rows, f_send_sem)
            for (xi, py, dz), f in columns(fsend.at[p], frecv.at[p], fedges.at[p]).items():
                vstate[xi, py, dz] = vstate[xi, py, dz] + half * f
                held[xi, py, dz] = half * f

        @pl.when(leads)
        def _():
            await_all(wide_sums.at[p, pl.ds(0, n_wide - 1)], wide_recv.at[p])

        @pl.when(follows)
        def _():
            await_rows(n_near, sum_send)
            await_all(wide_sums.at[p], wide_recv.at[p])

        row = total_of(wide_sums, n_wide)

        def across(part):
            return jnp.full((1, lanes), row[0, part * quarter], jnp.float32)

        vigor, potential, count = across(0), across(2), across(3)
        square = (1.0 - BATH_STRENGTH) + (BATH_STRENGTH * GOAL_WARMTH * 1.5) * count / vigor
        which = lax.broadcasted_iota(jnp.int32, (2, lanes), 1)
        record = jnp.concatenate([potential, square * vigor], axis=0) / slot_total
        history[...] = jnp.where(which == k - 1, record, history[...])

        @pl.when(leads)
        def _():
            await_rows(n_near + 2 * n_wide - 2, sum_send)

        scale[...] = jnp.sqrt(square)
        return 0

    history[...] = jnp.zeros_like(history)
    scale[...] = jnp.ones_like(scale)
    lax.fori_loop(1, STEPS + 1, step, 0)
    for y in range(ny):
        here = ostate[0, y + 1, 1]
        result[y] = jnp.where(here < 0.5 * FAR, here, kept[y])
        result[ny + y] = (vstate[0, y + 1, 1] + half * fsend[STEPS % 2, y]) * scale[...]
        result[2 * ny + y] = fsend[STEPS % 2, y]
    result[3 * ny, 0:2] = history[...]
    await_rows(deep_rows + halo_rows, first_sem)


def unpack(shape, result, o_out, v_out, f_out, h_out):
    nx, ny, nz, slots = shape
    lanes = nz * slots
    at = lax.broadcasted_iota(jnp.int32, (nz, lanes), 0) * slots + lax.rem(
        lax.broadcasted_iota(jnp.int32, (nz, lanes), 1), slots
    )
    for i, ref in enumerate((o_out, v_out, f_out)):
        for y in range(ny):
            for x in range(nx):
                for c in range(3):
                    r = c * nx + x
                    row = jnp.broadcast_to(result[i * ny + y, r : r + 1], (nz, lanes))
                    ref[x, y, c] = jnp.take_along_axis(row, at, axis=1, mode="promise_in_bounds")[:, :slots]
    h_out[...] = result[3 * ny, 0:2, :STEPS]


def shards(axes, offsets, velocities, occupied):
    nx, ny, nz, slots = occupied.shape
    lanes = nz * slots
    tile = lanes // slots
    assert axes[2] > 2 and tile >= 3 * nx and min(nx, ny) >= 2 and ny % 2 == 0 and nz == 2 * (ny + 2)
    _, flats, rows = partners_of(axes, ny)
    _, deep_flats, deep_rows = deep_places(axes, ny)
    nxo = len(offsets_of(axes[0]))
    n_near, n_wide = (len(chips_of(axes, group)) for group in (NEAR, WIDE))
    f32 = jnp.float32
    plane = jax.ShapeDtypeStruct((nx, ny, 3, nz, slots), f32)
    vmem = pl.BlockSpec(memory_space=pltpu.VMEM)
    dma = pltpu.SemaphoreType.DMA
    state = pltpu.VMEM((nxo, ny + 2, 3, tile, lanes), f32)
    halo = [
        pltpu.VMEM((ny, tile, lanes), f32),
        pltpu.VMEM((flats, tile, lanes), f32),
        pltpu.VMEM((2, ny, 1, lanes), f32),
        pltpu.VMEM((rows, 1, lanes), f32),
    ]
    result = pl.pallas_call(
        functools.partial(kernel, axes, (nx, ny, nz, slots)),
        name="verlet",
        out_shape=pltpu.VMEM((3 * ny + 1, tile, lanes), f32),
        in_specs=[pl.BlockSpec(memory_space=pltpu.HBM)] * 3,
        out_specs=vmem,
        scratch_shapes=[
            pltpu.VMEM((2, nx, ny, 3, nz, slots), f32),
            pltpu.VMEM((ny, tile, lanes), f32),
            state,
            state,
            state,
            pltpu.VMEM((nx + 2, ny + 2, 3, 3, slots, lanes), f32),
            pltpu.VMEM((nxo, ny + 7, 3, tile, lanes), f32),
            pltpu.VMEM((nxo, ny + 4, tile, lanes), f32),
            pltpu.VMEM((nx + 4, 3, 3, 3, slots, lanes), f32),
            pltpu.VMEM((nxo, ny + 3, tile, lanes), f32),
            pltpu.VMEM((ny, tile, lanes), f32),
            pltpu.VMEM((deep_flats, tile, lanes), f32),
            pltpu.VMEM((2, 2 * ny, 1, lanes), f32),
            pltpu.VMEM((deep_rows, 1, lanes), f32),
            *halo,
            pltpu.VMEM((nx, ny, nz, slots), jnp.int32),
            pltpu.VMEM((2, ny, tile, lanes), f32),
            pltpu.VMEM((2, flats, tile, lanes), f32),
            pltpu.VMEM((2, 2, ny, 1, lanes), f32),
            pltpu.VMEM((2, rows, 1, lanes), f32),
            pltpu.VMEM((1, lanes), f32),
            pltpu.VMEM((2, lanes), f32),
            pltpu.VMEM((1, lanes), f32),
            pltpu.VMEM((1, lanes), f32),
            pltpu.VMEM((2, 2 * n_near, 1, lanes), f32),
            pltpu.VMEM((1, lanes), f32),
            pltpu.VMEM((2, n_wide, 1, lanes), f32),
            pltpu.VMEM((deep_flats * tile + deep_rows + flats * tile + rows, 1, lanes), f32),
            dma((2,)),
            dma,
            dma((3,)),
            dma,
            dma,
            dma((2,)),
            dma,
            dma((2,)),
            dma((2,)),
        ],
        compiler_params=pltpu.CompilerParams(
            collective_id=0, has_side_effects=True, vmem_limit_bytes=VERLET_VMEM
        ),
    )(
        jnp.transpose(offsets, (0, 1, 4, 2, 3)),
        jnp.transpose(velocities, (0, 1, 4, 2, 3)),
        occupied,
    )
    o, v, f, h = pl.pallas_call(
        functools.partial(unpack, (nx, ny, nz, slots)),
        name="unpack",
        out_shape=[plane, plane, plane, jax.ShapeDtypeStruct((2, STEPS), f32)],
        in_specs=[vmem],
        out_specs=[vmem] * 4,
        compiler_params=pltpu.CompilerParams(vmem_limit_bytes=UNPACK_VMEM),
    )(result)
    back = (0, 1, 3, 4, 2)
    return (jnp.transpose(o, back), jnp.transpose(v, back), jnp.transpose(f, back), h.T)


def solution(mesh):
    axes = tuple(mesh.shape[a] for a in ("gx", "gy", "gz"))
    in_specs = (
        P("gx", "gy", "gz", None, None),
        P("gx", "gy", "gz", None, None),
        P("gx", "gy", "gz", None),
    )
    out_specs = (
        P("gx", "gy", "gz", None, None),
        P("gx", "gy", "gz", None, None),
        P("gx", "gy", "gz", None, None),
        P(),
    )
    return jax.shard_map(
        functools.partial(shards, axes), mesh=mesh, in_specs=in_specs, out_specs=out_specs, check_vma=False
    )
```

```python
import functools
import itertools

import jax
import jax.numpy as jnp
from jax import lax
from jax.experimental import pallas as pl
from jax.experimental.pallas import tpu as pltpu
from jax.sharding import PartitionSpec as P

MESH = pl.DeviceIdType.MESH
STEPS = 4
CUTOFF = 2.5
CELL_SIDE = 2.6
TIME_STEP = 0.005
BATH_STRENGTH = 0.25
GOAL_WARMTH = 0.8
FORCE_EDGE = 24.0 * (2.0 * CUTOFF ** (-13) - CUTOFF ** (-7))
ENERGY_EDGE = 4.0 * (CUTOFF ** (-12) - CUTOFF ** (-6))
FAR = 32.0
VERLET_VMEM = 60 * 1024 * 1024
UNPACK_VMEM = 4 * 1024 * 1024


NEAR = ("xl", "xh", "y")
WIDE = ("z",)


def parts_of(axes):
    gx, gy, gz = axes
    return {"xl": gx // 4, "y": 4, "xh": gy // 2, "z": gz}


def chips_of(axes, group):
    sizes = parts_of(axes)

    def hops(d):
        return sum(min(o, sizes[a] - o) for a, o in d.items())

    every = itertools.product(*[range(sizes[a]) for a in group])
    return sorted((dict(zip(group, d)) for d in every), key=lambda d: -hops(d))


def offsets_of(size):
    return [0] if size == 1 else [0, 1] if size == 2 else [0, 1, -1]


def canonical(size, off):
    return 0 if size == 1 else off % 2 if size == 2 else off


def padded(size, n):
    return [(canonical(size, -1), n - 1)] + [(0, i) for i in range(n)] + [(canonical(size, 1), 0)]


def deep(size, n):
    low, high = canonical(size, -1), canonical(size, 1)
    return [(low, n - 2), (low, n - 1)] + [(0, i) for i in range(n)] + [(high, 0), (high, 1)]


def deep_places(axes, ny):
    flat, rows, found = 0, 0, {}
    for d in itertools.product(*[offsets_of(n) for n in axes]):
        if d == (0, 0, 0):
            continue
        if d[2] == 0:
            found[d] = flat
            flat += ny
        else:
            found[d] = rows
            rows += 2 * ny
    return found, flat, rows


def partners_of(axes, ny):
    every = itertools.product(*[offsets_of(n) for n in axes])
    flat, rows, found = 0, 0, {}
    for d in every:
        if d == (0, 0, 0):
            continue
        need = sorted({yl for off, yl in padded(axes[1], ny) if off == d[1]})
        if d[2] == 0:
            found[d] = need, flat
            flat += len(need)
        else:
            found[d] = need, rows
            rows += len(need)
    return found, flat, rows


def kernel(
    axes, shape, o_in, v_in, occ_in, result,
    planes_in, kept, ostate, vstate, held, near, around, ends_of, first_near, first_force, osend, orecv, oedge, oedges, vsend, vrecv, vedge, vedges,
    occ_planes, fsend, frecv, fedge, fedges, tally, history, row_sum, near_sums, chip_sum, wide_sums, measure,
    in_sem, first_sem, o_recv_sem, v_sem, f_send_sem, f_recv_sem, sum_send, near_recv, wide_recv,
):
    gx, gy, gz = axes
    nx, ny, nz, slots = shape
    lanes = nz * slots
    tile = fsend.shape[2]
    slot_total = float(gx * gy * gz * nx * ny * lanes)
    me = [lax.axis_index(a) for a in ("gx", "gy", "gz")]
    sizes = parts_of(axes)
    place = {"xl": me[0] // 4, "y": lax.rem(me[0], 4), "xh": me[1] // 2, "z": me[2]}
    core = lax.rem(me[1], 2)
    leads = core == 1
    follows = core == 0
    near_chips, wide_chips = chips_of(axes, NEAR), chips_of(axes, WIDE)

    turned = [[lax.rem(me[i] + j, n) for j in range(n)] for i, n in enumerate(axes)]

    def device(d):
        return tuple(turned[i][d[i] % axes[i]] for i in range(3))

    def member(d, sign, which):
        at = dict(place)
        for a, o in d.items():
            if o:
                at[a] = lax.rem(at[a] + (o if sign > 0 else sizes[a] - o), sizes[a])
        return (at["xl"] * 4 + at["y"], at["xh"] * 2 + which, at["z"])

    def index_in(group):
        at = 0
        for a in group:
            at = at * sizes[a] + place[a]
        return at

    px_of, py_of = padded(gx, nx), padded(gy, ny)
    xs = offsets_of(gx)
    partners, flats, rows = partners_of(axes, ny)

    def remote(src, dst, send_sem, recv_sem, to):
        return pltpu.make_async_remote_copy(
            src_ref=src, dst_ref=dst, send_sem=send_sem, recv_sem=recv_sem, device_id=to, device_id_type=MESH
        )

    def copies_of(send, recv, edge, edges, send_sem, recv_sem):
        copies = []
        for d, (need, at) in reversed([*partners.items()]):
            where = pl.ds(need[0], len(need))
            to = device(tuple(-x for x in d))
            if d[2] == 0:
                copies.append(remote(send.at[where], recv.at[pl.ds(at, len(need))], send_sem, recv_sem, to))
            else:
                src = edge.at[0 if d[2] == 1 else 1, where]
                copies.append(remote(src, edges.at[pl.ds(at, len(need))], send_sem, recv_sem, to))
        return copies

    def await_all(ref, sem):
        pltpu.make_async_copy(ref, ref, sem).wait()

    def await_rows(n, sem):
        await_all(measure.at[pl.ds(0, n)], sem)

    halo_rows = flats * tile + rows
    deep_rows = sum(ny * tile if d[2] == 0 else 2 * ny for d in deep_places(axes, ny)[0])

    barrier = pltpu.get_barrier_semaphore()

    greeted = [device(d) for d in reversed([*partners])]
    others = [d for group in (near_chips, wide_chips) for d in group if any(d.values())]
    greeted += [member(d, 1, 1) for d in others]
    greeted.append(member({}, 1, 1 - core))
    for to in greeted:
        pl.semaphore_signal(barrier, inc=1, device_id=to, device_id_type=MESH)

    @pl.when(leads)
    def _():
        for d in others:
            pl.semaphore_signal(barrier, inc=1, device_id=member(d, 1, 0), device_id_type=MESH)

    loads = [
        pltpu.make_async_copy(o_in, planes_in.at[0], in_sem.at[0]),
        pltpu.make_async_copy(occ_in, occ_planes, in_sem.at[1]),
        pltpu.make_async_copy(v_in, planes_in.at[1], in_sem.at[0]),
    ]
    for load in loads:
        load.start()

    lane = lax.broadcasted_iota(jnp.int32, (nz, lanes), 1)
    level = lax.broadcasted_iota(jnp.int32, (nz, lanes), 0)
    spread = (
        lax.rem(lax.broadcasted_iota(jnp.int32, (slots, lanes), 1), slots)
        == lax.broadcasted_iota(jnp.int32, (slots, lanes), 0)
    ).astype(jnp.float32)

    def rows_of(planes):
        flat = planes.reshape(-1, slots)
        wide = jnp.dot(flat, spread, precision=lax.Precision.HIGHEST, preferred_element_type=jnp.float32)
        wide = wide.reshape(-1, nz, lanes)
        return jnp.sum(jnp.where((lane // slots == level)[None], wide, 0.0), axis=1)

    await_all(planes_in, in_sem.at[0])
    loads[1].wait()
    o_rows = rows_of(planes_in[0])
    v_rows = rows_of(planes_in[1])
    w_rows = rows_of(occ_planes[...].astype(jnp.float32))
    osend[...] = jnp.zeros_like(osend)
    kept[...] = jnp.zeros_like(kept)
    vsend[...] = jnp.zeros_like(vsend)
    fsend[...] = jnp.zeros_like(fsend)
    for x in range(nx):
        for y in range(ny):
            w = w_rows[x * ny + y : x * ny + y + 1]
            for c in range(3):
                i = (x * ny + y) * 3 + c
                r = c * nx + x
                kept[y, r : r + 1] = o_rows[i : i + 1]
                osend[y, r : r + 1] = jnp.where(w > 0.5, o_rows[i : i + 1], FAR)
                vsend[y, r : r + 1] = v_rows[i : i + 1] * w

    quarter = lanes // 4
    row_lane = lane[:1]

    tally[...] = jnp.broadcast_to(jnp.sum(w_rows, keepdims=True), (1, lanes))

    tile_lane = lax.broadcasted_iota(jnp.int32, (tile, lanes), 1)
    tile_row = lax.broadcasted_iota(jnp.int32, (tile, lanes), 0)
    slot_lane = lax.rem(tile_lane, slots)
    ends = [[slot_lane + (i if side == 0 else nz - 1 - i) * slots for i in range(2)] for side in range(2)]
    back = tile_row * slots + lax.rem(tile_lane, slots)

    def packed(block, side, depth=0):
        taken = jnp.take_along_axis(block, ends[side][depth], axis=1, mode="promise_in_bounds")
        return jnp.sum(jnp.where(tile_lane // slots == tile_row, taken, 0.0), axis=0, keepdims=True)

    def unpacked(row):
        wide = jnp.broadcast_to(row, (tile, lanes))
        return jnp.take_along_axis(wide, back, axis=1, mode="promise_in_bounds")

    for side in range(2):
        for y in range(ny):
            for depth in range(2):
                oedge[side, 2 * y + depth] = packed(osend[y], side, depth)
            vedge[side, y] = packed(vsend[y], side)

    pl.semaphore_wait(barrier, len(greeted) + len(others) * core)
    places, _, _ = deep_places(axes, ny)
    for d, at in reversed([*places.items()]):
        to = device(tuple(-x for x in d))
        if d[2] == 0:
            remote(osend, orecv.at[pl.ds(at, ny)], first_sem, o_recv_sem.at[d[1] % 3], to).start()
        else:
            src = oedge.at[0 if d[2] == 1 else 1]
            remote(src, oedges.at[pl.ds(at, 2 * ny)], first_sem, o_recv_sem.at[d[1] % 3], to).start()
    for copy in copies_of(vsend, vrecv, vedge, vedges, first_sem, v_sem):
        copy.start()

    def columns(send, recv, edges):
        found = {}
        for xi, a in enumerate(xs):
            for py, (b, yl) in enumerate(py_of):
                if (a, b) == (0, 0):
                    mid = send[yl]
                else:
                    need, at = partners[a, b, 0]
                    mid = recv[at + need.index(yl)]
                ends_of = []
                for c in (-1, 1):
                    need, at = partners[a, b, c]
                    ends_of.append(unpacked(edges[at + need.index(yl)]))
                below, above = ends_of
                found[xi, py, 1] = mid
                low = jnp.where(tile_lane >= lanes - slots, below, mid)
                found[xi, py, 0] = pltpu.roll(low, slots, 1)
                high = jnp.where(tile_lane < slots, above, mid)
                found[xi, py, 2] = pltpu.roll(high, lanes - slots, 1)
        return found

    cell = tile_lane // slots
    deep_x, deep_y = deep(gx, nx), deep(gy, ny)
    pairs = ny + 2

    def lay(xi, at, mid, below, above):
        below, above = ([unpacked(oedges[e + depth]) for depth in range(2)] for e in (below, above))
        low = jnp.where(tile_lane >= lanes - slots, below[0], mid)
        high = jnp.where(tile_lane < slots, above[0], mid)
        around[xi, at, 0] = pltpu.roll(low, slots, 1)
        around[xi, at, 1] = mid
        around[xi, at, 2] = pltpu.roll(high, lanes - slots, 1)
        bottom = jnp.where(cell == 0, below[1], jnp.where(cell == 1, below[0], pltpu.roll(mid, 2 * slots, 1)))
        top = jnp.where(cell == nz - 1, above[1], above[0])
        top = jnp.where(cell == nz - 3, pltpu.roll(mid, lanes - 2 * slots, 1), top)
        ends_of[xi, at] = jnp.where(cell < nz // 2, bottom, top)

    def await_row(b, level_tiles):
        await_rows(level_tiles * tile + 4 * ny * len(xs), o_recv_sem.at[b])

    def lay_beside(up):
        await_row(2 - up, ny * len(xs))
        for xi, a in enumerate(xs):
            above, below = ([places[a, canonical(gy, b), c] for c in (0, -1, 1)] for b in (1, -1))
            level_at, low_at, high_at = (m + up * (p - m) for p, m in zip(above, below))
            for yl in range(2):
                layer = (ny - 2) * (1 - up) + yl
                lay(
                    xi, yl + up * (ny + 2), orecv[level_at + layer], low_at + 2 * layer, high_at + 2 * layer
                )

    def lay_packed():
        for xi in range(len(xs)):
            for dy in range(3):
                for dz in range(3):
                    centre = jnp.where(lax.rem(cell, 2) == 0, dz, nz - 3 + dz)
                    source = centre * slots + slot_lane
                    gathered = jnp.zeros((tile, lanes), jnp.float32)
                    for t in range(pairs):
                        taken = jnp.take_along_axis(ends_of[xi, t + dy], source, axis=1, mode="promise_in_bounds")
                        gathered = jnp.where(cell // 2 == t, taken, gathered)
                    around[xi, pairs + 2 + dy, dz] = gathered

    lane_id = lax.broadcasted_iota(jnp.int32, (slots, lanes), 1)
    slot_id = lax.broadcasted_iota(jnp.int32, (slots, lanes), 0)
    pick = (lane_id // slots) * slots + slot_id
    itself = lax.rem(lane_id, slots) == slot_id

    def nearby(py):
        for px, (a, xl) in enumerate(px_of):
            for dz in range(3):
                for c in range(3):
                    r = c * nx + xl
                    row = jnp.broadcast_to(ostate[xs.index(a), py, dz, r : r + 1], (slots, lanes))
                    near[px, py, dz, c] = jnp.take_along_axis(row, pick, axis=1, mode="promise_in_bounds")

    half = 0.5 * TIME_STEP
    reach2 = CUTOFF * CUTOFF

    def terms(squared):
        inv = lax.rsqrt(squared)
        inv2 = inv * inv
        inv6 = inv2 * inv2 * inv2
        inv12 = inv6 * inv6
        bond = inv12 - inv6
        return inv, bond, inv * (bond + inv12)

    _, _, edge = terms(jnp.full((slots, lanes), reach2, jnp.float32))
    pair_count = 27.0 * slots

    def pair_sums(mine, near_of):
        force = [jnp.zeros((slots, lanes), jnp.float32) for _ in range(3)]
        bonds, reach = (jnp.zeros((slots, lanes), jnp.float32) for _ in range(2))
        for shift in itertools.product((-1, 0, 1), repeat=3):
            apart = [near_of(shift, c) - (mine[c] - shift[c] * CELL_SIDE) for c in range(3)]
            squared = apart[0] * apart[0] + apart[1] * apart[1] + apart[2] * apart[2]
            if shift == (0, 0, 0):
                squared = jnp.where(itself, reach2, squared)
            squared = jnp.minimum(squared, reach2)
            inv, bond, push = terms(squared)
            pull = inv * (edge - push)
            for c in range(3):
                force[c] = force[c] + pull * apart[c]
            bonds = bonds + bond
            reach = reach + squared * inv
        return [24.0 * jnp.sum(f, axis=0, keepdims=True) for f in force], bonds, reach

    def first_row(i, _):
        centre = i + 1 + 2 * (i // pairs)
        for px, (a, xl) in enumerate(deep_x):
            for dy in range(3):
                for dz in range(3):
                    for c in range(3):
                        r = c * nx + xl
                        row = jnp.broadcast_to(around[xs.index(a), centre - 1 + dy, dz, r : r + 1], (slots, lanes))
                        first_near[px, dy, dz, c] = jnp.take_along_axis(row, pick, axis=1, mode="promise_in_bounds")
        for px, (a, xl) in enumerate(px_of):
            block = around[xs.index(a), centre, 1]
            mine = [block[c * nx + xl : c * nx + xl + 1] for c in range(3)]
            force, _, _ = pair_sums(
                mine, lambda shift, c: first_near[px + 1 + shift[0], 1 + shift[1], 1 + shift[2], c]
            )
            for c in range(3):
                r = c * nx + xl
                first_force[xs.index(a), i, r : r + 1] = jnp.where(mine[0] < 0.5 * FAR, force[c], 0.0)
        return 0

    first_force[...] = jnp.zeros_like(first_force)
    await_row(0, ny * (len(xs) - 1))
    for xi, a in enumerate(xs):
        for yl in range(ny):
            mid = osend[yl] if a == 0 else orecv[places[a, 0, 0] + yl]
            lay(xi, yl + 2, mid, places[a, 0, -1] + 2 * yl, places[a, 0, 1] + 2 * yl)
    lay_beside(1 - core)
    near_rows = pairs // 2
    lax.fori_loop(0, near_rows, lambda t, _: first_row(t + near_rows * (1 - core), 0), 0)
    lay_beside(core)
    lay_packed()
    last = pairs - near_rows
    lax.fori_loop(
        0, last + 1, lambda t, _: first_row((t + near_rows * core) * (1 - t // last) + pairs * (t // last), 0), 0
    )

    await_rows(halo_rows, v_sem)
    first_v = columns(vsend, vrecv, vedges)
    for xi in range(len(xs)):
        outer = first_force[xi, pairs]
        for py in range(pairs):
            mid = first_force[xi, py]
            low = jnp.where(tile_lane < slots, pltpu.roll(outer, (lanes - 2 * py * slots) % lanes, 1), pltpu.roll(mid, slots, 1))
            high = jnp.where(
                tile_lane >= lanes - slots,
                pltpu.roll(outer, lanes - 2 * (py + 1) * slots, 1),
                pltpu.roll(mid, lanes - slots, 1),
            )
            for dz, f in enumerate((low, mid, high)):
                v = first_v[xi, py, dz] + half * f
                vstate[xi, py, dz] = v
                ostate[xi, py, dz] = around[xi, py + 1, dz] + TIME_STEP * v

    def step(k, _):
        p = lax.rem(k, 2)
        for py in range(ny + 2):
            nearby(py)

        energy_rows = jnp.zeros((1, lanes), jnp.float32)
        for x in range(nx):
            for y in range(ny):
                block = ostate[0, y + 1, 1]
                mine = [block[c * nx + x : c * nx + x + 1] for c in range(3)]
                occupied = mine[0] < 0.5 * FAR
                force, bonds, reach = pair_sums(
                    mine, lambda shift, c: near[x + 1 + shift[0], y + 1 + shift[1], 1 + shift[2], c]
                )
                for c in range(3):
                    r = c * nx + x
                    fsend[p, y, r : r + 1] = jnp.where(occupied, force[c], 0.0)
                energy = 4.0 * bonds + FORCE_EDGE * reach
                total = jnp.sum(energy, axis=0, keepdims=True)
                total = total - pair_count * (ENERGY_EDGE + CUTOFF * FORCE_EDGE)
                energy_rows = energy_rows + jnp.where(occupied, total, 0.0)

        kinetic = jnp.zeros((tile, lanes), jnp.float32)
        for y in range(ny):
            v = vstate[0, y + 1, 1] + half * fsend[p, y]
            kinetic = kinetic + v * v
        kinetic = jnp.sum(jnp.sum(kinetic, axis=0, keepdims=True), axis=1, keepdims=True)
        potential = jnp.sum(energy_rows, axis=1, keepdims=True)
        row = jnp.where(
            row_lane < 2 * quarter, 0.5 * kinetic, jnp.where(row_lane < 3 * quarter, 0.5 * potential, tally[...])
        )
        row_sum[...] = row
        at = index_in(NEAR) * 2 + core
        for d in near_chips:
            if any(d.values()):
                remote(row_sum, near_sums.at[p, at], sum_send, near_recv.at[p], member(d, -1, 1)).start()

        @pl.when(follows)
        def _():
            remote(row_sum, near_sums.at[p, at], sum_send, near_recv.at[p], member({}, 1, 1)).start()

        @pl.when(leads)
        def _():
            near_sums[p, at] = row

        @pl.when(k < STEPS)
        def _():
            for side in range(2):
                for y in range(ny):
                    fedge[p, side, y] = packed(fsend[p, y], side)
            for copy in copies_of(
                fsend.at[p], frecv.at[p], fedge.at[p], fedges.at[p], f_send_sem, f_recv_sem.at[p]
            ):
                copy.start()

        def total_of(ref, n):
            parts = [ref[p, i] for i in range(n)]
            while len(parts) > 1:
                parts = [sum(parts[i + 1 : i + 2], parts[i]) for i in range(0, len(parts), 2)]
            return parts[0]

        n_near, n_wide = len(near_chips), len(wide_chips)

        @pl.when(leads)
        def _():
            await_all(near_sums.at[p, pl.ds(0, 2 * n_near - 1)], near_recv.at[p])
            row = total_of(near_sums, 2 * n_near)
            chip_sum[...] = row
            at = index_in(WIDE)
            for d in wide_chips:
                for which in (0, 1):
                    if which == 0 or any(d.values()):
                        remote(
                            chip_sum, wide_sums.at[p, at], sum_send, wide_recv.at[p], member(d, -1, which)
                        ).start()
            wide_sums[p, at] = row

        @pl.when(k < STEPS)
        def _():
            await_rows(halo_rows, f_recv_sem.at[p])
            await_rows(halo_rows, f_send_sem)
            for (xi, py, dz), f in columns(fsend.at[p], frecv.at[p], fedges.at[p]).items():
                vstate[xi, py, dz] = vstate[xi, py, dz] + half * f
                held[xi, py, dz] = half * f

        @pl.when(leads)
        def _():
            await_all(wide_sums.at[p, pl.ds(0, n_wide - 1)], wide_recv.at[p])

        @pl.when(follows)
        def _():
            await_rows(n_near, sum_send)
            await_all(wide_sums.at[p], wide_recv.at[p])

        row = total_of(wide_sums, n_wide)

        def across(part):
            return jnp.full((1, lanes), row[0, part * quarter], jnp.float32)

        vigor, potential, count = across(0), across(2), across(3)
        square = (1.0 - BATH_STRENGTH) + (BATH_STRENGTH * GOAL_WARMTH * 1.5) * count / vigor
        which = lax.broadcasted_iota(jnp.int32, (2, lanes), 1)
        record = jnp.concatenate([potential, square * vigor], axis=0) / slot_total
        history[...] = jnp.where(which == k - 1, record, history[...])

        @pl.when(leads)
        def _():
            await_rows(n_near + 2 * n_wide - 2, sum_send)

        lam = jnp.sqrt(square)

        @pl.when(k < STEPS)
        def _():
            for xi in range(len(xs)):
                for py in range(ny + 2):
                    for dz in range(3):
                        v = vstate[xi, py, dz] * lam + held[xi, py, dz]
                        vstate[xi, py, dz] = v
                        ostate[xi, py, dz] = ostate[xi, py, dz] + TIME_STEP * v

        @pl.when(k == STEPS)
        def _():
            for y in range(ny):
                here = ostate[0, y + 1, 1]
                result[y] = jnp.where(here < 0.5 * FAR, here, kept[y])
                result[ny + y] = (vstate[0, y + 1, 1] + half * fsend[p, y]) * lam
                result[2 * ny + y] = fsend[p, y]
            result[3 * ny, 0:2] = history[...]

        return 0

    history[...] = jnp.zeros_like(history)
    lax.fori_loop(1, STEPS + 1, step, 0)
    await_rows(deep_rows + halo_rows, first_sem)


def unpack(shape, result, o_out, v_out, f_out, h_out):
    nx, ny, nz, slots = shape
    lanes = nz * slots
    at = lax.broadcasted_iota(jnp.int32, (nz, lanes), 0) * slots + lax.rem(
        lax.broadcasted_iota(jnp.int32, (nz, lanes), 1), slots
    )
    for i, ref in enumerate((o_out, v_out, f_out)):
        for y in range(ny):
            for x in range(nx):
                for c in range(3):
                    r = c * nx + x
                    row = jnp.broadcast_to(result[i * ny + y, r : r + 1], (nz, lanes))
                    ref[x, y, c] = jnp.take_along_axis(row, at, axis=1, mode="promise_in_bounds")[:, :slots]
    h_out[...] = result[3 * ny, 0:2, :STEPS]


def shards(axes, offsets, velocities, occupied):
    nx, ny, nz, slots = occupied.shape
    lanes = nz * slots
    tile = lanes // slots
    assert axes[2] > 2 and tile >= 3 * nx and min(nx, ny) >= 2 and ny % 2 == 0 and nz == 2 * (ny + 2)
    _, flats, rows = partners_of(axes, ny)
    _, deep_flats, deep_rows = deep_places(axes, ny)
    nxo = len(offsets_of(axes[0]))
    n_near, n_wide = (len(chips_of(axes, group)) for group in (NEAR, WIDE))
    f32 = jnp.float32
    plane = jax.ShapeDtypeStruct((nx, ny, 3, nz, slots), f32)
    vmem = pl.BlockSpec(memory_space=pltpu.VMEM)
    dma = pltpu.SemaphoreType.DMA
    state = pltpu.VMEM((nxo, ny + 2, 3, tile, lanes), f32)
    halo = [
        pltpu.VMEM((ny, tile, lanes), f32),
        pltpu.VMEM((flats, tile, lanes), f32),
        pltpu.VMEM((2, ny, 1, lanes), f32),
        pltpu.VMEM((rows, 1, lanes), f32),
    ]
    result = pl.pallas_call(
        functools.partial(kernel, axes, (nx, ny, nz, slots)),
        name="verlet",
        out_shape=pltpu.VMEM((3 * ny + 1, tile, lanes), f32),
        in_specs=[pl.BlockSpec(memory_space=pltpu.HBM)] * 3,
        out_specs=vmem,
        scratch_shapes=[
            pltpu.VMEM((2, nx, ny, 3, nz, slots), f32),
            pltpu.VMEM((ny, tile, lanes), f32),
            state,
            state,
            state,
            pltpu.VMEM((nx + 2, ny + 2, 3, 3, slots, lanes), f32),
            pltpu.VMEM((nxo, ny + 7, 3, tile, lanes), f32),
            pltpu.VMEM((nxo, ny + 4, tile, lanes), f32),
            pltpu.VMEM((nx + 4, 3, 3, 3, slots, lanes), f32),
            pltpu.VMEM((nxo, ny + 3, tile, lanes), f32),
            pltpu.VMEM((ny, tile, lanes), f32),
            pltpu.VMEM((deep_flats, tile, lanes), f32),
            pltpu.VMEM((2, 2 * ny, 1, lanes), f32),
            pltpu.VMEM((deep_rows, 1, lanes), f32),
            *halo,
            pltpu.VMEM((nx, ny, nz, slots), jnp.int32),
            pltpu.VMEM((2, ny, tile, lanes), f32),
            pltpu.VMEM((2, flats, tile, lanes), f32),
            pltpu.VMEM((2, 2, ny, 1, lanes), f32),
            pltpu.VMEM((2, rows, 1, lanes), f32),
            pltpu.VMEM((1, lanes), f32),
            pltpu.VMEM((2, lanes), f32),
            pltpu.VMEM((1, lanes), f32),
            pltpu.VMEM((2, 2 * n_near, 1, lanes), f32),
            pltpu.VMEM((1, lanes), f32),
            pltpu.VMEM((2, n_wide, 1, lanes), f32),
            pltpu.VMEM((deep_flats * tile + deep_rows + flats * tile + rows, 1, lanes), f32),
            dma((2,)),
            dma,
            dma((3,)),
            dma,
            dma,
            dma((2,)),
            dma,
            dma((2,)),
            dma((2,)),
        ],
        compiler_params=pltpu.CompilerParams(
            collective_id=0, has_side_effects=True, vmem_limit_bytes=VERLET_VMEM
        ),
    )(
        jnp.transpose(offsets, (0, 1, 4, 2, 3)),
        jnp.transpose(velocities, (0, 1, 4, 2, 3)),
        occupied,
    )
    o, v, f, h = pl.pallas_call(
        functools.partial(unpack, (nx, ny, nz, slots)),
        name="unpack",
        out_shape=[plane, plane, plane, jax.ShapeDtypeStruct((2, STEPS), f32)],
        in_specs=[vmem],
        out_specs=[vmem] * 4,
        compiler_params=pltpu.CompilerParams(vmem_limit_bytes=UNPACK_VMEM),
    )(result)
    back = (0, 1, 3, 4, 2)
    return (jnp.transpose(o, back), jnp.transpose(v, back), jnp.transpose(f, back), h.T)


def solution(mesh):
    axes = tuple(mesh.shape[a] for a in ("gx", "gy", "gz"))
    in_specs = (
        P("gx", "gy", "gz", None, None),
        P("gx", "gy", "gz", None, None),
        P("gx", "gy", "gz", None),
    )
    out_specs = (
        P("gx", "gy", "gz", None, None),
        P("gx", "gy", "gz", None, None),
        P("gx", "gy", "gz", None, None),
        P(),
    )
    return jax.shard_map(
        functools.partial(shards, axes), mesh=mesh, in_specs=in_specs, out_specs=out_specs, check_vma=False
    )
```
